256 devices in a mesh: samp: 8 (over x, core), state: 32 (over z, y).
Axes of the slice: x: 4, y: 4, z: 8, core: 2. Of those that a mesh axis runs over, the one named last changes fastest.
Arguments:
- components: bfloat16 [64, 262144], P(None, 'samp'), may hold values from -96 to 96
- coefficients: bfloat16 [64, 4096], P(None, 'state'), may hold values from -1.5 to 1.5
- block_window: int32 [2048], P('samp'), may hold values from 0 to 4095
- block_fill: int32 [2048], P('samp'), may hold values from 1 to 128
Outputs:
- free_energy: float32 [4096], P('state')
- log_denom: float32 [262144], P('samp')
The draws below stay inside these ranges and needn't reach their ends.
Inputs may be any that keep to these rules, and one draw needn't show every extreme that they name: `block_window`: blocks of one generating state may stand anywhere; some states generate no block.
All inputs are finite; a program needn't handle non-finite values.
Results may differ from the reference program's by a relative error of at most 0.0003.
Values may be sent and summed in bfloat16 or wider, within the bound.
No kernel may reach another device: no remote copies, remote signals or barrier semaphores. Data moves between devices by JAX's collectives and lax.ppermute only.
A program may use at most 128 MiB of HBM per device.

```python
import math
import jax
import jax.numpy as jnp
import numpy as np
from jax import lax

COMP = 64
BLOCK = 128
ITERS = 2
STATES = 4096
SAMPLES = 262144
BLOCKS = 2048


def draw_components(key, part):
    values = jnp.clip(jax.random.normal(key, (COMP, SAMPLES), jnp.float32), -6.0, 6.0)
    marked = jax.random.randint(jax.random.fold_in(key, 23), (1, SAMPLES), 0, 8) == 0
    strength = 30.0 * jnp.exp(jax.random.uniform(jax.random.fold_in(key, 29), (1, SAMPLES), jnp.float32) * math.log(1.6))
    strong = jnp.clip(jax.random.normal(jax.random.fold_in(key, 31), (COMP, SAMPLES), jnp.float32), -2.0, 2.0) * strength
    values = jnp.where(marked, strong, values)
    return values.astype(jnp.bfloat16)


def plant(values, stream_key, smallest, largest):
    spot = [jax.random.randint(jax.random.fold_in(stream_key, axis), (), 0, length) for axis, length in enumerate(values.shape)]
    longest = values.shape.index(max(values.shape))
    beside = spot[:longest] + [(spot[longest] + 1) % values.shape[longest]] + spot[longest + 1:]
    return values.at[tuple(spot)].set(smallest).at[tuple(beside)].set(largest)


def levels(stream_key, dims, split, least, high):
    def one(axis_at, blocks):
        draws = jax.random.uniform(jax.random.fold_in(jax.random.fold_in(stream_key, 6), axis_at), (blocks,), jnp.float32, least / len(split), high / len(split))
        return jnp.repeat(jnp.exp(draws), dims[axis_at] // blocks).reshape((-1,) + (1,) * (len(dims) - axis_at - 1))

    loudness = one(*split[0])
    for cut in split[1:]:
        loudness = loudness * one(*cut)
    return loudness


def cumulative_ranks(number_of, lean):
    loads = [(1 << 20) // math.isqrt(rank ** lean) + 1 for rank in range(1, number_of + 1)]
    spread = 1 + sum(loads) // (1 << 30)
    return np.cumsum(np.array([max(1, weight // spread) for weight in loads]))


def ranked_ids(stream_key, dims, number_of, slope):
    grid = cumulative_ranks(number_of, slope)
    lot = jax.random.randint(jax.random.fold_in(stream_key, 1), dims, 0, int(grid[number_of - 1]))
    rank = jnp.searchsorted(jnp.asarray(grid, jnp.int32), lot, side="right")
    return jax.random.permutation(jax.random.fold_in(stream_key, 2), number_of)[rank].astype(jnp.int32)


def bell_draw(key, shape, deviation, limit, split=(), kind=jnp.bfloat16):
    drawn = jax.random.normal(key, shape, jnp.float32) * deviation
    if len(split) > 0:
        drawn = levels(key, shape, split, -0.22, 0.18) * drawn
    return jnp.clip(drawn, min=-limit, max=limit).astype(kind)


def setup_inputs(seed: int = 0) -> dict:
    key_of = jax.random.split(jax.random.key(seed), 5)
    return {
        "components": draw_components(jax.random.fold_in(key_of[4], 71), 0),
        "coefficients": bell_draw(key_of[1], (COMP, STATES), 0.25, 1.5, ((1, 32),)),
        "block_window": plant(ranked_ids(key_of[2], (BLOCKS,), STATES, 2), jax.random.fold_in(key_of[2], 3), 0, STATES - 1).astype(jnp.int32),
        "block_fill": plant(jax.random.randint(key_of[3], (BLOCKS,), 1, BLOCK + 1), jax.random.fold_in(key_of[3], 1), 1, BLOCK).astype(jnp.int32),
    }


NEGATIVE = -1.0e30


def reference(components, coefficients, block_window, block_fill):
    counts = jax.ops.segment_sum(block_fill.astype(jnp.float32), block_window, num_segments=STATES)
    log_count = jnp.where(counts > 0, jnp.log(jnp.maximum(counts, 1.0)), NEGATIVE)
    alive = (jnp.arange(BLOCK, dtype=jnp.int32)[None, :] < block_fill[:, None]).reshape(SAMPLES)
    width = min(4096, SAMPLES)
    parts = SAMPLES // width
    comp_blocks = jnp.transpose(components.reshape(COMP, parts, width), (1, 0, 2))
    alive_blocks = alive.reshape(parts, width)

    def block_energy(comp_block):
        return jnp.dot(coefficients.T, comp_block, preferred_element_type=jnp.float32)

    def denominators(energy, free):
        exponents = (log_count + free)[:, None] - energy
        highest = jnp.max(exponents, axis=0)
        return highest + jnp.log(jnp.sum(jnp.exp(exponents - highest[None, :]), axis=0))

    def iterate(free):
        def visit(carry, items):
            highest, totals = carry
            comp_block, alive_block = items
            energy = block_energy(comp_block)
            logden = denominators(energy, free)
            exponents = jnp.where(alive_block[None, :], -energy - logden[None, :], NEGATIVE)
            newest = jnp.maximum(highest, jnp.max(exponents, axis=1))
            totals = totals * jnp.exp(highest - newest) + jnp.sum(jnp.exp(exponents - newest[:, None]), axis=1)
            return (newest, totals), None

        start = (jnp.full((STATES,), NEGATIVE, jnp.float32), jnp.zeros((STATES,), jnp.float32))
        (highest, totals), unused = lax.scan(visit, start, (comp_blocks, alive_blocks))
        result = -(highest + jnp.log(totals))
        return result - result[0]

    free = jnp.zeros((STATES,), jnp.float32)
    for sweep in range(ITERS):
        free = iterate(free)
    logden = lax.map(lambda comp_block: denominators(block_energy(comp_block), free), comp_blocks)
    return free, logden.reshape(SAMPLES)
```

```python
import jax
import jax.numpy as jnp
from jax import lax
from jax.sharding import Mesh
from jax.sharding import PartitionSpec as P

BLOCK = 128
ITERS = 2
STATE = ("state_0", "state_1")
SAMP = ("samp_0", "samp_1")
NEGATIVE = -1e30


def copies_of_each(x, axes):
    copies = jnp.broadcast_to(x, (lax.axis_size(axes), *x.shape))
    return lax.all_to_all(copies, axes, split_axis=0, concat_axis=0, tiled=True)


def laid_out(pieces, dim):
    dims = list(pieces.shape[1:])
    dims[dim] *= pieces.shape[0]
    return jnp.moveaxis(pieces, 0, dim).reshape(dims)


def log_sum(logs):
    highest = jnp.max(logs, axis=0)
    return highest + jnp.log(jnp.sum(jnp.exp(logs - highest[None]), axis=0))


def shards(components, coefficients, block_window, block_fill):
    state_count = lax.axis_size(STATE)
    position = lax.axis_index(STATE)
    own_states = coefficients.shape[1]
    row_count = components.shape[1] // state_count
    block_count = row_count // BLOCK
    component_rows = lax.dynamic_slice_in_dim(components, position * row_count, row_count, 1)
    fill_rows = lax.dynamic_slice_in_dim(block_fill, position * block_count, block_count, 0)
    gathered = copies_of_each(coefficients, STATE)
    blocks = copies_of_each(jnp.stack([block_window, block_fill]), SAMP)
    windows, fills = blocks[:, 0].reshape(-1), blocks[:, 1].reshape(-1)
    energy = lax.dot_general(
        laid_out(gathered, 1), component_rows, (((0,), (0,)), ((), ())), preferred_element_type=jnp.float32
    )
    total_states = energy.shape[0]
    low = 128
    fills_high = jnp.where(
        windows[None, :] // low == jnp.arange(total_states // low, dtype=jnp.int32)[:, None], fills[None, :], 0
    ).astype(jnp.bfloat16)
    is_low = (windows[None, :] % low == jnp.arange(low, dtype=jnp.int32)[:, None]).astype(jnp.bfloat16)
    counts = lax.dot_general(
        fills_high, is_low, (((1,), (1,)), ((), ())), preferred_element_type=jnp.float32
    ).reshape(-1)
    log_count = jnp.where(counts > 0, jnp.log(jnp.maximum(counts, 1.0)), NEGATIVE)
    alive = (jnp.arange(BLOCK, dtype=jnp.int32)[None, :] < fill_rows[:, None]).reshape(-1)

    def local_denominator(free):
        exponents = (log_count + free)[:, None] - energy
        highest = jnp.max(exponents, axis=0)
        return highest + jnp.log(jnp.sum(jnp.exp(exponents - highest[None, :]), axis=0))

    free = jnp.zeros((total_states,), jnp.float32)
    for sweep in range(ITERS):
        logden = local_denominator(free)
        exponents = jnp.where(alive[None, :], -energy - logden[None, :], NEGATIVE)
        highest = jnp.max(exponents, axis=1)
        logs = highest + jnp.log(jnp.sum(jnp.exp(exponents - highest[:, None]), axis=1))
        for axes in (SAMP, STATE):
            logs = log_sum(copies_of_each(logs, axes))
        free = -logs
        free = free - free[0]
    logden = local_denominator(free)
    log_denom = laid_out(copies_of_each(logden, STATE), 0)
    free_energy = lax.dynamic_slice_in_dim(free, position * own_states, own_states, 0)
    return (free_energy, log_denom)


def solution(mesh):
    torus = Mesh(mesh.devices.reshape(4, 2, 8, 4), ("samp_0", "samp_1", "state_0", "state_1"))
    placed = (P(None, SAMP), P(None, STATE), P(SAMP), P(SAMP))
    return jax.shard_map(
        shards, mesh=torus, in_specs=placed, out_specs=(P(STATE), P(SAMP)), check_vma=False
    )
```

```python
import jax
import jax.numpy as jnp
from jax import lax
from jax.experimental import pallas as pl
from jax.experimental.pallas import tpu as pltpu
from jax.sharding import Mesh
from jax.sharding import PartitionSpec as P

BLOCK = 128
LANES = 128
COMP = 64
TILE = 256
DEPTH = 128
CHUNK = 256
STATE = ("state_0", "state_1")
SAMP = ("samp_0", "samp_1")
NEGATIVE = -1e30
BF16 = jnp.bfloat16
F32 = jnp.float32


def exchanged(copies, axes):
    return lax.all_to_all(copies, axes, split_axis=0, concat_axis=0, tiled=True)


def copies_of_each(x, axes):
    return exchanged(jnp.broadcast_to(x, (lax.axis_size(axes), *x.shape)), axes)


def iota(shape, dim):
    return lax.broadcasted_iota(jnp.int32, shape, dim)


def dot_nt(a, b):
    return lax.dot_general(a, b, (((1,), (1,)), ((), ())), preferred_element_type=F32)


def dot(a, b):
    return jnp.dot(a, b, preferred_element_type=F32)


def three_parts(x):
    high = x.astype(BF16).astype(F32)
    rest = x - high
    middle = rest.astype(BF16).astype(F32)
    return high, middle, rest - middle


def log_sum_rows(logs):
    highest = jnp.max(logs, axis=0, keepdims=True)
    return highest + jnp.log(jnp.sum(jnp.exp(logs - highest), axis=0, keepdims=True))


def count_kernel(blocks_ref, place_ref, meta_ref, log_count_ref):
    groups = place_ref.shape[0]
    slots = log_count_ref.shape[0]
    width = blocks_ref.shape[2]
    counts = jnp.zeros((groups, LANES), F32)
    for s in range(blocks_ref.shape[0]):
        window = blocks_ref[s, 0:1, :]
        fill = blocks_ref[s, 1:2, :]
        of_group = jnp.where(iota((groups, width), 0) == window >> 7, fill, 0).astype(F32).astype(BF16)
        of_lane = jnp.where(iota((LANES, width), 0) == (window & 127), 1.0, 0.0).astype(BF16)
        counts = counts + dot_nt(of_group, of_lane)
    flag = jnp.where(counts > 0, 1.0, 0.0)
    packed = flag.astype(BF16)
    before = jnp.where(iota((LANES, LANES), 0) < iota((LANES, LANES), 1), 1.0, 0.0).astype(BF16)
    within = dot(packed, before)
    total = dot(packed, jnp.ones((LANES, LANES), BF16))
    earlier = jnp.where(iota((groups, groups), 1) < iota((groups, groups), 0), 1.0, 0.0).astype(BF16)
    offset = dot(earlier, total.astype(BF16))
    offset_int = offset.astype(jnp.int32)
    within_int = within.astype(jnp.int32)
    counted = counts > 0
    place_ref[...] = jnp.where(counted, (offset_int & 127) + within_int, -1)
    meta_ref[0:groups, :] = offset_int >> 7
    everything = jnp.sum(total, axis=0, keepdims=True).astype(jnp.int32)
    meta_ref[groups : groups + 8, :] = jnp.broadcast_to(everything, (8, LANES))
    whole = jnp.where(counted, offset_int + within_int, -1)
    counts_int = counts.astype(jnp.int32)
    digits = (counts_int >> 14, (counts_int >> 7) & 127, counts_int & 127)
    gathered = jnp.zeros((3 * slots, LANES), F32)
    for t in range(groups):
        row = whole[t : t + 1, :]
        slot = iota((slots, LANES), 0) == row >> 7
        parts = [jnp.where(slot, d[t : t + 1, :], 0).astype(F32) for d in digits]
        of_lane = jnp.where(iota((LANES, LANES), 0) == (row & 127), 1.0, 0.0).astype(BF16)
        gathered = gathered + dot_nt(jnp.concatenate(parts, 0).astype(BF16), of_lane)
    compact = gathered[0:slots] * 16384.0 + gathered[slots : 2 * slots] * 128.0 + gathered[2 * slots :]
    log_count_ref[...] = jnp.where(compact > 0, jnp.log(jnp.maximum(compact, 1.0)), NEGATIVE)


def tail_rows(log_weight):
    row = iota((DEPTH - COMP, TILE), 0)
    rows = jnp.where(row < 3, 1.0, 0.0)
    if log_weight is not None:
        for k, part in enumerate(three_parts(log_weight)):
            rows = jnp.where(row == 3 + k, part, rows)
    return rows.astype(BF16)


def denominator_chunk(c, points_ref, tiles_ref, tiles, energy_ref):
    points = points_ref[pl.ds(c * CHUNK, CHUNK), :]

    def find(j, highest):
        exponents = dot(points, tiles_ref[j])
        energy_ref[j] = exponents
        return jnp.maximum(highest, jnp.maximum(exponents[:, :LANES], exponents[:, LANES:]))

    highest = lax.fori_loop(0, tiles, find, jnp.full((CHUNK, LANES), 4 * NEGATIVE, F32))
    highest = jnp.max(highest, axis=1, keepdims=True)

    def add(j, totals):
        grown = jnp.exp(energy_ref[j] - highest)
        return totals + (grown[:, :LANES] + grown[:, LANES:])

    totals = lax.fori_loop(0, tiles, add, jnp.zeros((CHUNK, LANES), F32))
    return highest + jnp.log(jnp.sum(totals, axis=1, keepdims=True))


def live_points(c, logden, points_ref, live_ref, fill_ref, first_block):
    row = iota((BLOCK, 1), 0)
    alive = [row < fill_ref[first_block + c * (CHUNK // BLOCK) + b] for b in range(CHUNK // BLOCK)]
    shift = [
        jnp.where(a, -logden[b * BLOCK : (b + 1) * BLOCK, :], NEGATIVE) for b, a in enumerate(alive)
    ]
    shift = jnp.concatenate(shift, 0)
    lane = iota((CHUNK, DEPTH), 1)
    points = jnp.where(lane < COMP, points_ref[pl.ds(c * CHUNK, CHUNK), :].astype(F32), 0.0)
    for k, part in enumerate(three_parts(shift)):
        points = jnp.where(lane == COMP + k, part, points)
    live_ref[pl.ds(c * CHUNK, CHUNK), :] = points.astype(BF16)


def state_log_sum(tile, live_ref, exponent_ref):
    rows = live_ref.shape[0]
    highest = None
    for c in range(rows // CHUNK):
        exponents = dot(live_ref[c * CHUNK : (c + 1) * CHUNK, :], tile)
        exponent_ref[c * CHUNK : (c + 1) * CHUNK, :] = exponents
        top = jnp.max(exponents.reshape(CHUNK // 8, 8, TILE), axis=0)
        highest = top if highest is None else jnp.maximum(highest, top)
    highest = jnp.max(highest, axis=0, keepdims=True)
    totals = jnp.zeros((8, TILE), F32)
    for c in range(rows // CHUNK):
        grown = jnp.exp(exponent_ref[c * CHUNK : (c + 1) * CHUNK, :] - highest)
        totals = totals + jnp.sum(grown.reshape(CHUNK // 8, 8, TILE), axis=0)
    return highest + jnp.log(jnp.sum(totals, axis=0, keepdims=True))


def first_kernel(
    meta_ref, fill_ref, gathered_ref, components_ref, place_ref, log_count_ref,
    logs_ref, tiles_ref, points_ref,
    packed_ref, energy_ref, live_ref, exponent_ref,
):
    groups = gathered_ref.shape[0]
    rows = points_ref.shape[0]
    tiles = (meta_ref[groups] + TILE - 1) // TILE
    packed_ref[...] = jnp.zeros(packed_ref.shape, F32)
    for t in range(groups):
        chosen = jnp.where(iota((2 * LANES, LANES), 0) == place_ref[t : t + 1, :], 1.0, 0.0).astype(BF16)
        moved = dot_nt(gathered_ref[t], chosen)
        at = meta_ref[t]
        packed_ref[at] += moved[:, :LANES]
        packed_ref[at + 1] += moved[:, LANES:]
    for j in range(tiles_ref.shape[0]):
        tiles_ref[j, 0:COMP, :] = jnp.concatenate([packed_ref[2 * j], packed_ref[2 * j + 1]], 1).astype(BF16)
        weight = jnp.concatenate([log_count_ref[2 * j : 2 * j + 1, :], log_count_ref[2 * j + 1 : 2 * j + 2, :]], 1)
        tiles_ref[j, COMP:DEPTH, :] = tail_rows(weight)
    lane = iota((LANES, DEPTH - COMP), 1)
    ones = jnp.where((lane >= 3) & (lane < 6), 1.0, 0.0)
    for b in range(rows // LANES):
        turned = -components_ref[:, b * LANES : (b + 1) * LANES].astype(F32).T
        points_ref[b * LANES : (b + 1) * LANES, :] = jnp.concatenate([turned, ones], 1).astype(BF16)
    first_block = meta_ref[groups + 1] * (rows // BLOCK)
    for c in range(rows // CHUNK):
        logden = denominator_chunk(c, points_ref, tiles_ref, tiles, energy_ref)
        live_points(c, logden, points_ref, live_ref, fill_ref, first_block)
    logs_ref[...] = jnp.zeros(logs_ref.shape, F32)

    def one(j, carry):
        logs = state_log_sum(tiles_ref[j], live_ref, exponent_ref)
        logs_ref[:, pl.ds(pl.multiple_of(j * TILE, TILE), TILE)] = jnp.broadcast_to(logs, (8, TILE))
        return carry

    lax.fori_loop(0, tiles, one, 0)


def second_kernel(
    meta_ref, fill_ref, logs_in_ref, gathered_ref, tiles_in_ref, points_ref, log_count_ref,
    logs_ref,
    tiles_ref, energy_ref, live_ref, exponent_ref,
):
    groups = gathered_ref.shape[0]
    rows = points_ref.shape[0]
    tiles = (meta_ref[groups] + TILE - 1) // TILE
    slots = tiles_ref.shape[0] * TILE
    weighted_tiles(logs_in_ref, tiles_in_ref, log_count_ref, tiles_ref, None)
    first_block = meta_ref[groups + 1] * (rows // BLOCK)
    for c in range(rows // CHUNK):
        logden = denominator_chunk(c, points_ref, tiles_ref, tiles, energy_ref)
        live_points(c, logden, points_ref, live_ref, fill_ref, first_block)
    logs_ref[:, 0:slots] = jnp.zeros((8, slots), F32)

    def one(j, carry):
        logs = state_log_sum(tiles_ref[j], live_ref, exponent_ref)
        logs_ref[:, pl.ds(pl.multiple_of(j * TILE, TILE), TILE)] = jnp.broadcast_to(logs, (8, TILE))
        return carry

    lax.fori_loop(0, tiles, one, 0)
    tail = tail_rows(None)

    def every(t, carry):
        head = jnp.concatenate([gathered_ref[2 * t], gathered_ref[2 * t + 1]], 1)
        logs = state_log_sum(jnp.concatenate([head, tail], 0), live_ref, exponent_ref)
        logs_ref[:, pl.ds(pl.multiple_of(slots + t * TILE, TILE), TILE)] = jnp.broadcast_to(logs, (8, TILE))
        return carry

    lax.fori_loop(0, groups * LANES // TILE, every, 0)


def weighted_tiles(logs_in_ref, tiles_in_ref, log_count_ref, tiles_ref, base):
    for j in range(tiles_ref.shape[0]):
        free = -log_sum_rows(logs_in_ref[:, j * TILE : (j + 1) * TILE])
        if base is not None:
            free = free + base
        weight = jnp.concatenate([log_count_ref[2 * j : 2 * j + 1, :], log_count_ref[2 * j + 1 : 2 * j + 2, :]], 1)
        tiles_ref[j, 0:COMP, :] = tiles_in_ref[j, 0:COMP, :]
        tiles_ref[j, COMP:DEPTH, :] = tail_rows(weight + free)


def third_kernel(
    meta_ref, logs_in_ref, tiles_in_ref, points_ref, log_count_ref,
    free_ref, logden_ref,
    tiles_ref, energy_ref,
):
    copies, rows = logden_ref.shape
    slots = tiles_ref.shape[0] * TILE
    tiles = (meta_ref[copies] + TILE - 1) // TILE
    base = log_sum_rows(logs_in_ref[:, slots + LANES : slots + 2 * LANES])[:, 0:1]
    own = log_sum_rows(logs_in_ref[:, slots : slots + LANES])
    free_ref[...] = jnp.broadcast_to(base - own, free_ref.shape)
    weighted_tiles(logs_in_ref, tiles_in_ref, log_count_ref, tiles_ref, base)
    for c in range(rows // CHUNK):
        logden = denominator_chunk(c, points_ref, tiles_ref, tiles, energy_ref)
        for b in range(CHUNK // LANES):
            turned = jnp.broadcast_to(logden[b * LANES : (b + 1) * LANES, :], (LANES, LANES)).T
            at = c * CHUNK + b * LANES
            logden_ref[:, at : at + LANES] = turned[0:copies, :]


def merge_kernel(logs_ref, copies_ref):
    for j in range(logs_ref.shape[1] // TILE):
        logs = log_sum_rows(logs_ref[:, j * TILE : (j + 1) * TILE])
        copies_ref[:, j * TILE : (j + 1) * TILE] = jnp.broadcast_to(logs, (copies_ref.shape[0], TILE))


def merge_last_kernel(logs_ref, copies_ref):
    copies = copies_ref.shape[0]
    slots = copies_ref.shape[1] - 2 * LANES
    for j in range(slots // TILE):
        logs = log_sum_rows(logs_ref[:, j * TILE : (j + 1) * TILE])
        copies_ref[:, j * TILE : (j + 1) * TILE] = jnp.broadcast_to(logs, (copies, TILE))
    for t in range(copies):
        at = slots + t * LANES
        logs = log_sum_rows(logs_ref[:, at : at + LANES])
        copies_ref[t : t + 1, slots : slots + LANES] = logs
        if t == 0:
            copies_ref[:, slots + LANES :] = jnp.broadcast_to(logs, (copies, LANES))


def shards(components, coefficients, block_window, block_fill):
    groups = lax.axis_size(STATE)
    samps = lax.axis_size(SAMP)
    position = lax.axis_index(STATE)
    rows = components.shape[1] // groups
    slots = min(samps * block_window.shape[0], groups * LANES)
    slot_rows = slots // LANES
    tile_count = slots // TILE
    shape = jax.ShapeDtypeStruct
    vmem = pl.BlockSpec(memory_space=pltpu.VMEM)
    smem = pl.BlockSpec(memory_space=pltpu.SMEM)
    params = pltpu.CompilerParams(vmem_limit_bytes=50 << 20)

    blocks = copies_of_each(jnp.stack([block_window, block_fill]), SAMP)
    gathered = copies_of_each(coefficients, STATE)
    place, meta, log_count = pl.pallas_call(
        count_kernel,
        out_shape=(
            shape((groups, LANES), jnp.int32), shape((groups + 8, LANES), jnp.int32), shape((slot_rows, LANES), F32),
        ),
        in_specs=[vmem], out_specs=(vmem, vmem, vmem), compiler_params=params, name="count",
    )(blocks)
    meta = jnp.concatenate([meta[: groups + 1, 0], position.astype(jnp.int32)[None]])

    work = [
        pltpu.VMEM((tile_count, CHUNK, TILE), F32), pltpu.VMEM((rows, DEPTH), BF16), pltpu.VMEM((rows, TILE), F32),
    ]
    full = lambda dims: pl.BlockSpec(dims, lambda i, m, f: (0,) * len(dims))
    logs, tiles, points = pl.pallas_call(
        first_kernel,
        out_shape=(shape((samps, slots), F32), shape((tile_count, DEPTH, TILE), BF16), shape((rows, DEPTH), BF16)),
        grid_spec=pltpu.PrefetchScalarGridSpec(
            num_scalar_prefetch=2, grid=(1,),
            in_specs=[
                full(gathered.shape), pl.BlockSpec((COMP, rows), lambda i, m, f: (0, m[groups + 1])),
                full(place.shape), full(log_count.shape),
            ],
            out_specs=(full((samps, slots)), full((tile_count, DEPTH, TILE)), full((rows, DEPTH))),
            scratch_shapes=[pltpu.VMEM((slot_rows + 2, COMP, LANES), F32), *work],
        ),
        compiler_params=params, name="first",
    )(meta, block_fill, gathered, components, place, log_count)
    logs = exchanged(logs, SAMP)
    logs = pl.pallas_call(
        merge_kernel, out_shape=shape((groups, slots), F32), in_specs=[vmem], out_specs=vmem, name="merge",
    )(logs)
    logs = exchanged(logs, STATE)
    logs = pl.pallas_call(
        second_kernel,
        out_shape=shape((samps, slots + groups * LANES), F32),
        in_specs=[smem, smem, vmem, vmem, vmem, vmem, vmem], out_specs=vmem,
        scratch_shapes=[pltpu.VMEM((tile_count, DEPTH, TILE), BF16), *work],
        compiler_params=params, name="second",
    )(meta, block_fill, logs, gathered, tiles, points, log_count)
    logs = exchanged(logs, SAMP)
    logs = pl.pallas_call(
        merge_last_kernel, out_shape=shape((groups, slots + 2 * LANES), F32), in_specs=[vmem], out_specs=vmem,
        name="merge_last",
    )(logs)
    logs = exchanged(logs, STATE)
    free, logden = pl.pallas_call(
        third_kernel,
        out_shape=(shape((8, LANES), F32), shape((groups, rows), F32)),
        in_specs=[smem, vmem, vmem, vmem, vmem], out_specs=(vmem, vmem),
        scratch_shapes=[pltpu.VMEM((tile_count, DEPTH, TILE), BF16), pltpu.VMEM((tile_count, CHUNK, TILE), F32)],
        compiler_params=params, name="third",
    )(meta, logs, tiles, points, log_count)
    return free[0], exchanged(logden, STATE).reshape(-1)


def solution(mesh):
    torus = Mesh(mesh.devices.reshape(4, 2, 8, 4), ("samp_0", "samp_1", "state_0", "state_1"))
    placed = (P(None, SAMP), P(None, STATE), P(SAMP), P(SAMP))
    return jax.shard_map(
        shards, mesh=torus, in_specs=placed, out_specs=(P(STATE), P(SAMP)), check_vma=False
    )
```

```python
import functools

import jax
import jax.numpy as jnp
from jax import lax
from jax.experimental import pallas as pl
from jax.experimental.pallas import tpu as pltpu
from jax.sharding import Mesh
from jax.sharding import PartitionSpec as P


BLOCK = 128
LANES = 128
COMP = 64
TILE = 256
DEPTH = 128
CHUNK = 256
TAIL = 16
LEAST = 1e-25
SPREAD = 50.0
STATE = ("state_0", "state_1")
SAMP = ("samp_0", "samp_1")
NEGATIVE = -1e30
BF16 = jnp.bfloat16
F32 = jnp.float32


def exchanged(copies, axes):
    return lax.all_to_all(copies, axes, split_axis=0, concat_axis=0, tiled=True)


def copies_of_each(x, axes):
    return exchanged(jnp.broadcast_to(x, (lax.axis_size(axes), *x.shape)), axes)


def iota(shape, dim):
    return lax.broadcasted_iota(jnp.int32, shape, dim)


def dot_nt(a, b):
    return lax.dot_general(a, b, (((1,), (1,)), ((), ())), preferred_element_type=F32)


def dot(a, b):
    return jnp.dot(a, b, preferred_element_type=F32)


def three_parts(x):
    high = x.astype(BF16).astype(F32)
    rest = x - high
    middle = rest.astype(BF16).astype(F32)
    return high, middle, rest - middle


def log_sum(logs):
    highest = jnp.max(logs, axis=0)
    return highest + jnp.log(jnp.sum(jnp.exp(logs - highest[None]), axis=0))


def log_sum_pieces(logs_ref):
    pieces = logs_ref.shape[0]
    highest = functools.reduce(jnp.maximum, [logs_ref[p] for p in range(pieces)])
    totals = functools.reduce(jnp.add, [jnp.exp(logs_ref[p] - highest) for p in range(pieces)])
    return highest + jnp.log(totals)


def chunk(c):
    return pl.ds(c * CHUNK, CHUNK)


def halves(combine, x):
    return combine(x[:, :LANES], x[:, LANES:])


def count_kernel(
    spot_ref, blocks_ref, components_ref, place_ref, meta_ref, log_count_ref, points_ref,
):
    groups = place_ref.shape[0]
    slots = log_count_ref.shape[0]
    rows = points_ref.shape[0]
    width = blocks_ref.shape[2]
    counts = jnp.zeros((groups, LANES), F32)
    for s in range(blocks_ref.shape[0]):
        window = blocks_ref[s, 0:1, :]
        fill = blocks_ref[s, 1:2, :]
        of_group = jnp.where(iota((groups, width), 0) == window >> 7, fill, 0).astype(F32).astype(BF16)
        of_lane = jnp.where(iota((LANES, width), 0) == (window & 127), 1.0, 0.0).astype(BF16)
        counts = counts + dot_nt(of_group, of_lane)
    counted = counts > 0
    packed = jnp.where(counted, 1.0, 0.0).astype(BF16)
    before = jnp.where(iota((LANES, LANES), 0) < iota((LANES, LANES), 1), 1.0, 0.0).astype(BF16)
    within = dot(packed, before)
    total = dot(packed, jnp.ones((LANES, LANES), BF16))
    earlier = jnp.where(iota((groups, groups), 1) < iota((groups, groups), 0), 1.0, 0.0).astype(BF16)
    offset_int = dot(earlier, total.astype(BF16)).astype(jnp.int32)
    within_int = within.astype(jnp.int32)
    place_ref[...] = jnp.where(counted, (offset_int & 127) + within_int, -1)
    meta_ref[0:groups, :] = offset_int >> 7
    everything = jnp.sum(total, axis=0, keepdims=True).astype(jnp.int32)
    meta_ref[groups : groups + 8, :] = jnp.broadcast_to(everything, (8, LANES))
    whole = jnp.where(counted, offset_int + within_int, -1)
    counts_int = counts.astype(jnp.int32)
    digits = (counts_int >> 14, (counts_int >> 7) & 127, counts_int & 127)
    gathered = jnp.zeros((3 * slots, LANES), F32)
    for t in range(groups):
        row = whole[t : t + 1, :]
        slot = iota((slots, LANES), 0) == row >> 7
        parts = [jnp.where(slot, d[t : t + 1, :], 0).astype(F32) for d in digits]
        of_lane = jnp.where(iota((LANES, LANES), 0) == (row & 127), 1.0, 0.0).astype(BF16)
        gathered = gathered + dot_nt(jnp.concatenate(parts, 0).astype(BF16), of_lane)
    compact = gathered[0:slots] * 16384.0 + gathered[slots : 2 * slots] * 128.0 + gathered[2 * slots :]
    log_count_ref[...] = jnp.where(compact > 0, jnp.log(jnp.maximum(compact, 1.0)), NEGATIVE)
    half = COMP // 2
    own = pl.multiple_of(spot_ref[1] * half, half)
    lane = iota((LANES, DEPTH - COMP), 1)
    ones = jnp.where((lane >= 3) & (lane < 6), 1.0, 0.0)
    for b in range(rows // LANES):
        at = slice(b * LANES, (b + 1) * LANES)
        mine = components_ref[pl.ds(own, half), at].astype(F32)
        other = components_ref[pl.ds(pl.multiple_of(half - own, half), half), at].astype(F32)
        turned = -jnp.concatenate([mine, other], 0).T
        points_ref[at, :] = jnp.concatenate([turned, ones], 1).astype(BF16)


def tail_rows(weight):
    row = iota((TAIL, TILE), 0)
    rows = jnp.where(row < 3, 1.0, 0.0)
    if weight is not None:
        for k, part in enumerate(three_parts(weight)):
            rows = jnp.where(row == 3 + k, part, rows)
    return rows.astype(BF16)


def with_shift(points, shift):
    lane = iota(points.shape, 1)
    for k, part in enumerate(three_parts(shift)):
        points = jnp.where(lane == COMP + k, part, points)
    return points


def tile_row(rows, j):
    return jnp.concatenate([rows[2 * j : 2 * j + 1, :], rows[2 * j + 1 : 2 * j + 2, :]], 1)


def find_denominators(points_ref, tiles_ref, pairs, energy_ref, highest_ref, totals_ref):
    rows = points_ref.shape[0]
    highest_ref[...] = jnp.full(highest_ref.shape, 4 * NEGATIVE, F32)
    totals_ref[...] = jnp.zeros(totals_ref.shape, F32)

    def find(i, carry):
        for c in range(rows // CHUNK):
            top = highest_ref[chunk(c), :]
            for k in range(2):
                exponents = dot(points_ref[chunk(c), :], tiles_ref[2 * i + k])
                energy_ref[2 * i + k, chunk(c), :] = exponents
                top = jnp.maximum(top, halves(jnp.maximum, exponents))
            highest_ref[chunk(c), :] = top
        return carry

    lax.fori_loop(0, pairs, find, 0)
    for c in range(rows // CHUNK):
        top = jnp.max(highest_ref[chunk(c), :], axis=1, keepdims=True)
        highest_ref[chunk(c), :] = jnp.broadcast_to(top, (CHUNK, LANES))

    def add(i, carry):
        for c in range(rows // CHUNK):
            top = highest_ref[chunk(c), :]
            top = jnp.concatenate([top, top], 1)
            sums = totals_ref[chunk(c), :]
            for k in range(2):
                sums = sums + halves(jnp.add, jnp.exp(energy_ref[2 * i + k, chunk(c), :] - top))
            totals_ref[chunk(c), :] = sums
        return carry

    lax.fori_loop(0, pairs, add, 0)
    for c in range(rows // CHUNK):
        sums = jnp.sum(totals_ref[chunk(c), :], axis=1, keepdims=True)
        logden = highest_ref[chunk(c), :][:, 0:1] + jnp.log(sums)
        totals_ref[chunk(c), :] = jnp.broadcast_to(logden, (CHUNK, LANES))


def denominators_near(base_ref, anchored_ref, tiles_ref, pairs, totals_ref):
    rows = anchored_ref.shape[0]
    totals_ref[...] = jnp.zeros(totals_ref.shape, F32)

    def add(i, carry):
        for c in range(rows // CHUNK):
            sums = totals_ref[chunk(c), :]
            for k in range(2):
                sums = sums + halves(jnp.add, jnp.exp(dot(anchored_ref[chunk(c), :], tiles_ref[2 * i + k])))
            totals_ref[chunk(c), :] = sums
        return carry

    lax.fori_loop(0, pairs, add, 0)
    for c in range(rows // CHUNK):
        sums = jnp.sum(totals_ref[chunk(c), :], axis=1, keepdims=True)
        logden = base_ref[chunk(c), :][:, 0:1] + jnp.log(sums)
        totals_ref[chunk(c), :] = jnp.broadcast_to(logden, (CHUNK, LANES))


def put_live(points_ref, totals_ref, live_ref, fill_ref, first_block, anchored_ref=None):
    row = iota((BLOCK, LANES), 0)
    for b in range(points_ref.shape[0] // BLOCK):
        at = pl.ds(b * BLOCK, BLOCK)
        points = points_ref[at, :].astype(F32)
        logden = totals_ref[at, :]
        if anchored_ref is not None:
            anchored_ref[at, :] = with_shift(points, -logden).astype(BF16)
        shift = jnp.where(row < fill_ref[first_block + b], -logden, NEGATIVE)
        live_ref[at, :] = with_shift(points, shift).astype(BF16)


def exponents_and_highest(tile, live_ref, exponent_ref):
    highest = None
    for c in range(live_ref.shape[0] // CHUNK):
        exponents = dot(live_ref[chunk(c), :], tile)
        exponent_ref[chunk(c), :] = exponents
        top = jnp.max(exponents.reshape(CHUNK // 8, 8, TILE), axis=0)
        highest = top if highest is None else jnp.maximum(highest, top)
    return jnp.max(highest, axis=0, keepdims=True)


def log_of_sum(highest, exponent_ref):
    totals = jnp.zeros((8, TILE), F32)
    for c in range(exponent_ref.shape[0] // CHUNK):
        grown = jnp.exp(exponent_ref[chunk(c), :] - highest)
        totals = totals + jnp.sum(grown.reshape(CHUNK // 8, 8, TILE), axis=0)
    return highest + jnp.log(jnp.sum(totals, axis=0, keepdims=True))


def put_rows(logs_ref, first, logs):
    logs_ref[pl.ds(first, 1), :] = logs[:, :LANES]
    logs_ref[pl.ds(first + 1, 1), :] = logs[:, LANES:]


def counted_log_sums(total, weight_ref, tiles_ref, pairs, live_ref, exponent_ref, logs_ref, low_ref):
    low_ref[...] = jnp.zeros(low_ref.shape, F32)
    logs_ref[0 : weight_ref.shape[0], :] = jnp.zeros(weight_ref.shape, F32)

    def finish(j, logs):
        weight = jnp.concatenate([weight_ref[pl.ds(2 * j, 1), :], weight_ref[pl.ds(2 * j + 1, 1), :]], 1)
        valid = iota((1, TILE), 1) < total - j * TILE
        put_rows(logs_ref, 2 * j, jnp.where(valid, logs - weight, 0.0))
        return valid

    def one(i, carry):
        for k in range(2):
            j = 2 * i + k
            totals = jnp.zeros((8, TILE), F32)
            for c in range(live_ref.shape[0] // CHUNK):
                grown = jnp.exp(dot(live_ref[chunk(c), :], tiles_ref[j]))
                totals = totals + jnp.sum(grown.reshape(CHUNK // 8, 8, TILE), axis=0)
            totals = jnp.sum(totals, axis=0, keepdims=True)
            valid = finish(j, jnp.log(totals))
            low_ref[0:1, :] = jnp.maximum(low_ref[0:1, :], jnp.where(valid & (totals < LEAST), 1.0, 0.0))
        return carry

    lax.fori_loop(0, pairs, one, 0)

    @pl.when(jnp.max(low_ref[...]) > 0)
    def _():
        def again(j, carry):
            highest = exponents_and_highest(tiles_ref[j], live_ref, exponent_ref)
            finish(j, log_of_sum(highest, exponent_ref))
            return carry

        lax.fori_loop(0, 2 * pairs, again, 0)


def weighted_tiles(total, logs, log_count_ref, tiles_in_ref, tiles_ref, weight_ref):
    valid = iota(logs.shape, 0) * LANES + iota(logs.shape, 1) < total
    free = jnp.where(valid, -logs, 4 * NEGATIVE)
    highest = jnp.max(jnp.max(free, axis=0, keepdims=True), axis=1, keepdims=True)
    free = jnp.where(valid, free - highest, 0.0)
    weight = log_count_ref[...] + free
    weight_ref[...] = weight
    for j in range(tiles_ref.shape[0]):
        tiles_ref[j, 0:COMP, :] = tiles_in_ref[j, 0:COMP, :]
        tiles_ref[j, COMP : COMP + TAIL, :] = tail_rows(tile_row(weight, j))
        tiles_ref[j, COMP + TAIL : DEPTH, :] = jnp.zeros((DEPTH - COMP - TAIL, TILE), BF16)
    return highest, jnp.min(free)


def first_kernel(
    meta_ref, fill_ref, mine_ref, other_ref, place_ref, log_count_ref, points_ref,
    logs_ref, tiles_ref, anchored_ref, base_ref,
    packed_ref, energy_ref, highest_ref, live_ref, exponent_ref, low_ref, rows_ref,
):
    groups = mine_ref.shape[0]
    total = meta_ref[groups]
    pairs = (total + 2 * TILE - 1) // (2 * TILE)
    packed_ref[...] = jnp.zeros(packed_ref.shape, F32)
    for t in range(groups):
        chosen = jnp.where(iota((2 * LANES, LANES), 0) == place_ref[t : t + 1, :], 1.0, 0.0).astype(BF16)
        moved = dot_nt(jnp.concatenate([mine_ref[t], other_ref[t]], 0), chosen)
        at = meta_ref[t]
        packed_ref[at] += moved[:, :LANES]
        packed_ref[at + 1] += moved[:, LANES:]
    log_count = log_count_ref[...]
    for j in range(tiles_ref.shape[0]):
        tiles_ref[j, 0:COMP, :] = jnp.concatenate([packed_ref[2 * j], packed_ref[2 * j + 1]], 1).astype(BF16)
        tiles_ref[j, COMP : COMP + TAIL, :] = tail_rows(tile_row(log_count, j))
        tiles_ref[j, COMP + TAIL : DEPTH, :] = jnp.zeros((DEPTH - COMP - TAIL, TILE), BF16)
    find_denominators(points_ref, tiles_ref, pairs, energy_ref, highest_ref, base_ref)
    first_block = meta_ref[groups + 1] * (points_ref.shape[0] // BLOCK)
    put_live(points_ref, base_ref, live_ref, fill_ref, first_block, anchored_ref)
    counted_log_sums(total, log_count_ref, tiles_ref, pairs, live_ref, exponent_ref, rows_ref, low_ref)
    logs_ref[...] = jnp.broadcast_to(rows_ref[...][None], logs_ref.shape)


def new_denominators(least, base_ref, anchored_ref, points_ref, tiles_ref, pairs, energy_ref, highest_ref, totals_ref):
    near = least > -SPREAD

    @pl.when(near)
    def _():
        denominators_near(base_ref, anchored_ref, tiles_ref, pairs, totals_ref)

    @pl.when(jnp.logical_not(near))
    def _():
        find_denominators(points_ref, tiles_ref, pairs, energy_ref, highest_ref, totals_ref)


def second_kernel(
    meta_ref, fill_ref, logs_in_ref, mine_ref, other_ref, log_count_ref, tiles_in_ref, points_ref, anchored_ref, base_ref,
    logs_ref,
    tiles_ref, weight_ref, energy_ref, highest_ref, totals_ref, live_ref, exponent_ref, second_ref, low_ref, rows_ref,
):
    groups = mine_ref.shape[0]
    slot_rows = weight_ref.shape[0]
    total = meta_ref[groups]
    pairs = (total + 2 * TILE - 1) // (2 * TILE)
    logs = log_sum_pieces(logs_in_ref)
    _, least = weighted_tiles(total, logs, log_count_ref, tiles_in_ref, tiles_ref, weight_ref)
    new_denominators(
        least, base_ref, anchored_ref, points_ref, tiles_ref, pairs, energy_ref, highest_ref, totals_ref
    )
    first_block = meta_ref[groups + 1] * (points_ref.shape[0] // BLOCK)
    put_live(points_ref, totals_ref, live_ref, fill_ref, first_block)
    counted_log_sums(total, weight_ref, tiles_ref, pairs, live_ref, exponent_ref, rows_ref, low_ref)
    rest = jnp.concatenate([tail_rows(None), jnp.zeros((DEPTH - COMP - TAIL, TILE), BF16)], 0)
    last = groups * LANES // TILE - 1

    def every_tile(t):
        parts = [jnp.concatenate([mine_ref[2 * t + k], other_ref[2 * t + k]], 0) for k in range(2)]
        tile = jnp.concatenate([jnp.concatenate(parts, 1), rest], 0)
        return tile

    def two(i, highest):
        after = exponents_and_highest(every_tile(2 * i + 1), live_ref, second_ref)
        put_rows(rows_ref, slot_rows + 4 * i, log_of_sum(highest, exponent_ref))
        highest = exponents_and_highest(every_tile(jnp.minimum(2 * i + 2, last)), live_ref, exponent_ref)
        put_rows(rows_ref, slot_rows + 4 * i + 2, log_of_sum(after, second_ref))
        return highest

    start = exponents_and_highest(every_tile(0), live_ref, exponent_ref)
    lax.fori_loop(0, (last + 1) // 2, two, start)
    logs_ref[...] = jnp.broadcast_to(rows_ref[...][None], logs_ref.shape)


def third_kernel(
    meta_ref, logs_in_ref, log_count_ref, tiles_in_ref, points_ref, anchored_ref, base_ref,
    free_ref, logden_ref,
    tiles_ref, weight_ref, energy_ref, highest_ref, totals_ref,
):
    copies = logden_ref.shape[0]
    slot_rows = weight_ref.shape[0]
    total = meta_ref[copies]
    pairs = (total + 2 * TILE - 1) // (2 * TILE)
    logs = log_sum_pieces(logs_in_ref)
    zero = logs[slot_rows + 1 : slot_rows + 2, 0:1]
    free_ref[...] = jnp.broadcast_to(zero - logs[slot_rows : slot_rows + 1, :], free_ref.shape)
    highest, least = weighted_tiles(
        total, logs[:slot_rows], log_count_ref, tiles_in_ref, tiles_ref, weight_ref
    )
    new_denominators(
        least, base_ref, anchored_ref, points_ref, tiles_ref, pairs, energy_ref, highest_ref, totals_ref
    )
    turned = [totals_ref[pl.ds(b * LANES, LANES), :].T[0:1, :] for b in range(points_ref.shape[0] // LANES)]
    logden = jnp.concatenate(turned, 0) + (highest + zero)
    logden_ref[...] = jnp.broadcast_to(logden[None], logden_ref.shape)


def shards(components, coefficients, block_window, block_fill):
    groups = lax.axis_size(STATE)
    samps = lax.axis_size(SAMP)
    position = lax.axis_index(STATE)
    core = lax.axis_index(SAMP[1])
    rows = components.shape[1] // groups
    slots = min(samps * block_window.shape[0], groups * LANES)
    slot_rows = slots // LANES
    tile_count = slots // TILE
    shape = jax.ShapeDtypeStruct
    vmem = pl.BlockSpec(memory_space=pltpu.VMEM)
    smem = pl.BlockSpec(memory_space=pltpu.SMEM)
    params = pltpu.CompilerParams(vmem_limit_bytes=24 << 20)
    whole = lambda dims: pl.BlockSpec(dims, lambda i, m: (0,) * len(dims))

    half = COMP // 2
    mine = copies_of_each(lax.dynamic_slice_in_dim(coefficients, core * half, half, 0), STATE)
    blocks = jnp.stack([block_window, block_fill])[None]
    blocks = jnp.concatenate([blocks, lax.ppermute(blocks, SAMP[1], [(0, 1), (1, 0)])], 0)
    along = lax.axis_size(SAMP[0])
    turns = [[(i, (i + k) % along) for i in range(along)] for k in range(1, along)]
    blocks = jnp.concatenate([blocks] + [lax.ppermute(blocks, SAMP[0], turn) for turn in turns], 0)
    other = lax.ppermute(mine, SAMP[1], [(0, 1), (1, 0)])
    spot = jnp.stack([position, core]).astype(jnp.int32)
    place, meta, log_count, points = pl.pallas_call(
        count_kernel,
        out_shape=(
            shape((groups, LANES), jnp.int32), shape((groups + 8, LANES), jnp.int32), shape((slot_rows, LANES), F32),
            shape((rows, DEPTH), BF16),
        ),
        grid_spec=pltpu.PrefetchScalarGridSpec(
            num_scalar_prefetch=1, grid=(1,),
            in_specs=[whole(blocks.shape), pl.BlockSpec((COMP, rows), lambda i, m: (0, m[0]))],
            out_specs=(whole((groups, LANES)), whole((groups + 8, LANES)), whole((slot_rows, LANES)), whole((rows, DEPTH))),
        ),
        compiler_params=params, name="count",
    )(spot, blocks, components)
    meta = jnp.concatenate([meta[: groups + 1, 0], spot[:1]])

    tiles_work = pltpu.VMEM((tile_count, DEPTH, TILE), BF16)
    weight_work = pltpu.VMEM((slot_rows, LANES), F32)
    energy_work = pltpu.VMEM((tile_count, rows, TILE), F32)
    column_work = pltpu.VMEM((rows, LANES), F32)
    live_work = pltpu.VMEM((rows, DEPTH), BF16)
    exponent_work = pltpu.VMEM((rows, TILE), F32)
    low_work = pltpu.VMEM((8, TILE), F32)
    logs, tiles, anchored, base = pl.pallas_call(
        first_kernel,
        out_shape=(
            shape((samps, slot_rows, LANES), F32), shape((tile_count, DEPTH, TILE), BF16), shape((rows, DEPTH), BF16),
            shape((rows, LANES), F32),
        ),
        in_specs=[smem, smem, vmem, vmem, vmem, vmem, vmem], out_specs=(vmem,) * 4,
        scratch_shapes=[
            pltpu.VMEM((slot_rows + 2, COMP, LANES), F32), energy_work, column_work, live_work, exponent_work, low_work,
            weight_work,
        ],
        compiler_params=params, name="first",
    )(meta, block_fill, mine, other, place, log_count, points)
    logs = log_sum(exchanged(logs, SAMP))
    logs = copies_of_each(logs, STATE)
    logs = pl.pallas_call(
        second_kernel,
        out_shape=shape((samps, slot_rows + groups, LANES), F32),
        in_specs=[smem, smem] + [vmem] * 8, out_specs=vmem,
        scratch_shapes=[
            tiles_work, weight_work, energy_work, column_work, column_work, live_work, exponent_work, exponent_work,
            low_work, pltpu.VMEM((slot_rows + groups, LANES), F32),
        ],
        compiler_params=params, name="second",
    )(meta, block_fill, logs, mine, other, log_count, tiles, points, anchored, base)
    logs = log_sum(exchanged(logs, SAMP))
    every = logs[slot_rows:]
    logs = jnp.concatenate(
        [
            jnp.broadcast_to(logs[None, :slot_rows], (groups, slot_rows, LANES)), every[:, None, :],
            jnp.broadcast_to(every[0], (groups, 1, LANES)), jnp.zeros((groups, 6, LANES), F32),
        ],
        1,
    )
    logs = exchanged(logs, STATE)
    free, logden = pl.pallas_call(
        third_kernel,
        out_shape=(shape((8, LANES), F32), shape((groups, rows // LANES, LANES), F32)),
        in_specs=[smem] + [vmem] * 6, out_specs=(vmem, vmem),
        scratch_shapes=[tiles_work, weight_work, energy_work, column_work, column_work],
        compiler_params=params, name="third",
    )(meta, logs, log_count, tiles, points, anchored, base)
    return free[0], exchanged(logden, STATE).reshape(-1)


def solution(mesh):
    torus = Mesh(mesh.devices.reshape(4, 2, 8, 4), ("samp_0", "samp_1", "state_0", "state_1"))
    placed = (P(None, SAMP), P(None, STATE), P(SAMP), P(SAMP))
    return jax.shard_map(
        shards, mesh=torus, in_specs=placed, out_specs=(P(STATE), P(SAMP)), check_vma=False
    )
```

```python
import functools

import jax
import jax.numpy as jnp
from jax import lax
from jax.experimental import pallas as pl
from jax.experimental.pallas import tpu as pltpu
from jax.sharding import Mesh
from jax.sharding import PartitionSpec as P


BLOCK = 128
LANES = 128
COMP = 64
TILE = 256
DEPTH = 128
CHUNK = 256
TAIL = 16
LEAST = 1e-25
SPREAD = 50.0
SMALL_ROWS = 8
SMALL = (SMALL_ROWS - 1) * LANES - 1
STATE = ("state_0", "state_1")
SAMP = ("samp_0", "samp_1")
NEGATIVE = -1e30
BF16 = jnp.bfloat16
F32 = jnp.float32


def exchanged(copies, axes):
    return lax.all_to_all(copies, axes, split_axis=0, concat_axis=0, tiled=True)


def copies_of_each(x, axes):
    return exchanged(jnp.broadcast_to(x, (lax.axis_size(axes), *x.shape)), axes)


def iota(shape, dim):
    return lax.broadcasted_iota(jnp.int32, shape, dim)


def dot_nt(a, b):
    return lax.dot_general(a, b, (((1,), (1,)), ((), ())), preferred_element_type=F32)


def dot(a, b):
    return jnp.dot(a, b, preferred_element_type=F32)


def three_parts(x):
    high = x.astype(BF16).astype(F32)
    rest = x - high
    middle = rest.astype(BF16).astype(F32)
    return high, middle, rest - middle


def log_sum(logs):
    highest = jnp.max(logs, axis=0)
    return highest + jnp.log(jnp.sum(jnp.exp(logs - highest[None]), axis=0))


def log_sum_pieces(logs_ref):
    pieces = logs_ref.shape[0]
    highest = functools.reduce(jnp.maximum, [logs_ref[p] for p in range(pieces)])
    totals = functools.reduce(jnp.add, [jnp.exp(logs_ref[p] - highest) for p in range(pieces)])
    return highest + jnp.log(totals)


def chunk(c):
    return pl.ds(c * CHUNK, CHUNK)


def halves(combine, x):
    return combine(x[:, :LANES], x[:, LANES:])


def points_kernel(spot_ref, block_ref, points_ref):
    rows = points_ref.shape[0]
    half = COMP // 2
    own = pl.multiple_of(spot_ref[1] * half, half)
    lane = iota((LANES, DEPTH - COMP), 1)
    ones = jnp.where((lane >= 3) & (lane < 6), 1.0, 0.0)
    for b in range(rows // LANES):
        at = slice(b * LANES, (b + 1) * LANES)
        mine = block_ref[pl.ds(own, half), at].astype(F32)
        other = block_ref[pl.ds(pl.multiple_of(half - own, half), half), at].astype(F32)
        turned = -jnp.concatenate([mine, other], 0).T
        points_ref[at, :] = jnp.concatenate([turned, ones], 1).astype(BF16)


def count_kernel(*refs):
    blocks_refs, (place_ref, meta_ref, log_count_ref) = refs[:-3], refs[-3:]
    groups = place_ref.shape[0]
    slots = log_count_ref.shape[0]
    width = blocks_refs[0].shape[2]
    counts = jnp.zeros((groups, LANES), F32)
    for blocks_ref, s in [(r, s) for r in blocks_refs for s in range(r.shape[0])]:
        window = blocks_ref[s, 0:1, :]
        fill = blocks_ref[s, 1:2, :]
        of_group = jnp.where(iota((groups, width), 0) == window >> 7, fill, 0).astype(F32).astype(BF16)
        of_lane = jnp.where(iota((LANES, width), 0) == (window & 127), 1.0, 0.0).astype(BF16)
        counts = counts + dot_nt(of_group, of_lane)
    counted = counts > 0
    packed = jnp.where(counted, 1.0, 0.0).astype(BF16)
    before = jnp.where(iota((LANES, LANES), 0) < iota((LANES, LANES), 1), 1.0, 0.0).astype(BF16)
    within = dot(packed, before)
    total = dot(packed, jnp.ones((LANES, LANES), BF16))
    earlier = jnp.where(iota((groups, groups), 1) < iota((groups, groups), 0), 1.0, 0.0).astype(BF16)
    offset_int = dot(earlier, total.astype(BF16)).astype(jnp.int32)
    within_int = within.astype(jnp.int32)
    place_ref[...] = jnp.where(counted, (offset_int & 127) + within_int, -1)
    meta_ref[0:groups, :] = offset_int >> 7
    everything = jnp.sum(total, axis=0, keepdims=True).astype(jnp.int32)
    meta_ref[groups : groups + 8, :] = jnp.broadcast_to(everything, (8, LANES))
    whole = jnp.where(counted, offset_int + within_int, -1)
    counts_int = counts.astype(jnp.int32)
    digits = (counts_int >> 14, (counts_int >> 7) & 127, counts_int & 127)
    gathered = jnp.zeros((3 * slots, LANES), F32)
    for t in range(groups):
        row = whole[t : t + 1, :]
        slot = iota((slots, LANES), 0) == row >> 7
        parts = [jnp.where(slot, d[t : t + 1, :], 0).astype(F32) for d in digits]
        of_lane = jnp.where(iota((LANES, LANES), 0) == (row & 127), 1.0, 0.0).astype(BF16)
        gathered = gathered + dot_nt(jnp.concatenate(parts, 0).astype(BF16), of_lane)
    compact = gathered[0:slots] * 16384.0 + gathered[slots : 2 * slots] * 128.0 + gathered[2 * slots :]
    log_count_ref[...] = jnp.where(compact > 0, jnp.log(jnp.maximum(compact, 1.0)), NEGATIVE)


def tail_rows(weight):
    row = iota((TAIL, TILE), 0)
    rows = jnp.where(row < 3, 1.0, 0.0)
    if weight is not None:
        for k, part in enumerate(three_parts(weight)):
            rows = jnp.where(row == 3 + k, part, rows)
    return rows.astype(BF16)


def with_shift(points, shift):
    lane = iota(points.shape, 1)
    for k, part in enumerate(three_parts(shift)):
        points = jnp.where(lane == COMP + k, part, points)
    return points


def tile_row(rows, j):
    return jnp.concatenate([rows[2 * j : 2 * j + 1, :], rows[2 * j + 1 : 2 * j + 2, :]], 1)


def find_denominators(points_ref, tiles_ref, pairs, energy_ref, highest_ref, totals_ref):
    rows = points_ref.shape[0]
    highest_ref[...] = jnp.full(highest_ref.shape, 4 * NEGATIVE, F32)
    totals_ref[...] = jnp.zeros(totals_ref.shape, F32)

    def find(i, carry):
        for c in range(rows // CHUNK):
            top = highest_ref[chunk(c), :]
            for k in range(2):
                exponents = dot(points_ref[chunk(c), :], tiles_ref[2 * i + k])
                energy_ref[2 * i + k, chunk(c), :] = exponents
                top = jnp.maximum(top, halves(jnp.maximum, exponents))
            highest_ref[chunk(c), :] = top
        return carry

    lax.fori_loop(0, pairs, find, 0)
    for c in range(rows // CHUNK):
        top = jnp.max(highest_ref[chunk(c), :], axis=1, keepdims=True)
        highest_ref[chunk(c), :] = jnp.broadcast_to(top, (CHUNK, LANES))

    def add(i, carry):
        for c in range(rows // CHUNK):
            top = highest_ref[chunk(c), :]
            top = jnp.concatenate([top, top], 1)
            sums = totals_ref[chunk(c), :]
            for k in range(2):
                sums = sums + halves(jnp.add, jnp.exp(energy_ref[2 * i + k, chunk(c), :] - top))
            totals_ref[chunk(c), :] = sums
        return carry

    lax.fori_loop(0, pairs, add, 0)
    for c in range(rows // CHUNK):
        sums = jnp.sum(totals_ref[chunk(c), :], axis=1, keepdims=True)
        logden = highest_ref[chunk(c), :][:, 0:1] + jnp.log(sums)
        totals_ref[chunk(c), :] = jnp.broadcast_to(logden, (CHUNK, LANES))


def denominators_near(base_ref, anchored_ref, tiles_ref, pairs, totals_ref):
    rows = anchored_ref.shape[0]
    totals_ref[...] = jnp.zeros(totals_ref.shape, F32)

    def add(i, carry):
        for c in range(rows // CHUNK):
            sums = totals_ref[chunk(c), :]
            for k in range(2):
                sums = sums + halves(jnp.add, jnp.exp(dot(anchored_ref[chunk(c), :], tiles_ref[2 * i + k])))
            totals_ref[chunk(c), :] = sums
        return carry

    lax.fori_loop(0, pairs, add, 0)
    for c in range(rows // CHUNK):
        sums = jnp.sum(totals_ref[chunk(c), :], axis=1, keepdims=True)
        logden = base_ref[chunk(c), :][:, 0:1] + jnp.log(sums)
        totals_ref[chunk(c), :] = jnp.broadcast_to(logden, (CHUNK, LANES))


def put_live(points_ref, totals_ref, live_ref, fill_ref, first_block, anchored_ref=None):
    row = iota((BLOCK, LANES), 0)
    for b in range(points_ref.shape[0] // BLOCK):
        at = pl.ds(b * BLOCK, BLOCK)
        points = points_ref[at, :].astype(F32)
        logden = totals_ref[at, :]
        if anchored_ref is not None:
            anchored_ref[at, :] = with_shift(points, -logden).astype(BF16)
        shift = jnp.where(row < fill_ref[first_block + b], -logden, NEGATIVE)
        live_ref[at, :] = with_shift(points, shift).astype(BF16)


def exponents_and_highest(tile, live_ref, exponent_ref):
    highest = None
    for c in range(live_ref.shape[0] // CHUNK):
        exponents = dot(live_ref[chunk(c), :], tile)
        exponent_ref[chunk(c), :] = exponents
        top = jnp.max(exponents.reshape(CHUNK // 8, 8, TILE), axis=0)
        highest = top if highest is None else jnp.maximum(highest, top)
    return jnp.max(highest, axis=0, keepdims=True)


def log_of_sum(highest, exponent_ref):
    totals = jnp.zeros((8, TILE), F32)
    for c in range(exponent_ref.shape[0] // CHUNK):
        grown = jnp.exp(exponent_ref[chunk(c), :] - highest)
        totals = totals + jnp.sum(grown.reshape(CHUNK // 8, 8, TILE), axis=0)
    return highest + jnp.log(jnp.sum(totals, axis=0, keepdims=True))


def put_rows(logs_ref, first, logs):
    logs_ref[pl.ds(first, 1), :] = logs[:, :LANES]
    logs_ref[pl.ds(first + 1, 1), :] = logs[:, LANES:]


def counted_log_sums(total, weight_ref, tiles_ref, pairs, live_ref, exponent_ref, logs_ref, low_ref):
    low_ref[...] = jnp.zeros(low_ref.shape, F32)
    logs_ref[0 : weight_ref.shape[0], :] = jnp.zeros(weight_ref.shape, F32)

    def finish(j, logs):
        weight = jnp.concatenate([weight_ref[pl.ds(2 * j, 1), :], weight_ref[pl.ds(2 * j + 1, 1), :]], 1)
        valid = iota((1, TILE), 1) < total - j * TILE
        put_rows(logs_ref, 2 * j, jnp.where(valid, logs - weight, 0.0))
        return valid

    def one(i, carry):
        for k in range(2):
            j = 2 * i + k
            totals = jnp.zeros((8, TILE), F32)
            for c in range(live_ref.shape[0] // CHUNK):
                grown = jnp.exp(dot(live_ref[chunk(c), :], tiles_ref[j]))
                totals = totals + jnp.sum(grown.reshape(CHUNK // 8, 8, TILE), axis=0)
            totals = jnp.sum(totals, axis=0, keepdims=True)
            valid = finish(j, jnp.log(totals))
            low_ref[0:1, :] = jnp.maximum(low_ref[0:1, :], jnp.where(valid & (totals < LEAST), 1.0, 0.0))
        return carry

    lax.fori_loop(0, pairs, one, 0)

    @pl.when(jnp.max(low_ref[...]) > 0)
    def _():
        def again(j, carry):
            highest = exponents_and_highest(tiles_ref[j], live_ref, exponent_ref)
            finish(j, log_of_sum(highest, exponent_ref))
            return carry

        lax.fori_loop(0, 2 * pairs, again, 0)


def weighted_tiles(total, logs, log_count_ref, tiles_in_ref, tiles_ref, weight_ref):
    valid = iota(logs.shape, 0) * LANES + iota(logs.shape, 1) < total
    free = jnp.where(valid, -logs, 4 * NEGATIVE)
    highest = jnp.max(jnp.max(free, axis=0, keepdims=True), axis=1, keepdims=True)
    free = jnp.where(valid, free - highest, 0.0)
    weight = log_count_ref[0 : weight_ref.shape[0], :] + free
    weight_ref[...] = weight
    for j in range(tiles_ref.shape[0]):
        tiles_ref[j, 0:COMP, :] = tiles_in_ref[j, 0:COMP, :]
        tiles_ref[j, COMP : COMP + TAIL, :] = tail_rows(tile_row(weight, j))
        tiles_ref[j, COMP + TAIL : DEPTH, :] = jnp.zeros((DEPTH - COMP - TAIL, TILE), BF16)
    return highest, jnp.min(free)


def first_kernel(
    meta_ref, fill_ref, mine_ref, other_ref, place_ref, log_count_ref, points_ref,
    logs_ref, tiles_ref, anchored_ref, base_ref,
    packed_ref, energy_ref, highest_ref, live_ref, exponent_ref, low_ref, rows_ref, weight_ref,
):
    groups = mine_ref.shape[0]
    total = meta_ref[groups]
    pairs = (total + 2 * TILE - 1) // (2 * TILE)
    packed_ref[...] = jnp.zeros(packed_ref.shape, F32)
    for t in range(groups):
        chosen = jnp.where(iota((2 * LANES, LANES), 0) == place_ref[t : t + 1, :], 1.0, 0.0).astype(BF16)
        moved = dot_nt(jnp.concatenate([mine_ref[t], other_ref[t]], 0), chosen)
        at = meta_ref[t]
        packed_ref[at] += moved[:, :LANES]
        packed_ref[at + 1] += moved[:, LANES:]
    log_count = log_count_ref[0 : logs_ref.shape[1], :]
    weight_ref[...] = log_count
    for j in range(tiles_ref.shape[0]):
        tiles_ref[j, 0:COMP, :] = jnp.concatenate([packed_ref[2 * j], packed_ref[2 * j + 1]], 1).astype(BF16)
        tiles_ref[j, COMP : COMP + TAIL, :] = tail_rows(tile_row(log_count, j))
        tiles_ref[j, COMP + TAIL : DEPTH, :] = jnp.zeros((DEPTH - COMP - TAIL, TILE), BF16)
    find_denominators(points_ref, tiles_ref, pairs, energy_ref, highest_ref, base_ref)
    first_block = meta_ref[groups + 1] * (points_ref.shape[0] // BLOCK)
    put_live(points_ref, base_ref, live_ref, fill_ref, first_block, anchored_ref)
    counted_log_sums(total, weight_ref, tiles_ref, pairs, live_ref, exponent_ref, rows_ref, low_ref)
    logs_ref[...] = jnp.broadcast_to(rows_ref[...][None], logs_ref.shape)


def new_denominators(least, base_ref, anchored_ref, points_ref, tiles_ref, pairs, energy_ref, highest_ref, totals_ref):
    near = least > -SPREAD

    @pl.when(near)
    def _():
        denominators_near(base_ref, anchored_ref, tiles_ref, pairs, totals_ref)

    @pl.when(jnp.logical_not(near))
    def _():
        find_denominators(points_ref, tiles_ref, pairs, energy_ref, highest_ref, totals_ref)


def second_kernel(
    meta_ref, fill_ref, logs_in_ref, mine_ref, other_ref, log_count_ref, tiles_in_ref, points_ref, anchored_ref, base_ref,
    logs_ref,
    tiles_ref, weight_ref, energy_ref, highest_ref, totals_ref, live_ref, exponent_ref, second_ref, low_ref, rows_ref,
):
    groups = mine_ref.shape[0]
    slot_rows = weight_ref.shape[0]
    total = meta_ref[groups]
    pairs = (total + 2 * TILE - 1) // (2 * TILE)
    logs = log_sum_pieces(logs_in_ref)
    _, least = weighted_tiles(total, logs, log_count_ref, tiles_in_ref, tiles_ref, weight_ref)
    new_denominators(
        least, base_ref, anchored_ref, points_ref, tiles_ref, pairs, energy_ref, highest_ref, totals_ref
    )
    first_block = meta_ref[groups + 1] * (points_ref.shape[0] // BLOCK)
    put_live(points_ref, totals_ref, live_ref, fill_ref, first_block)
    counted_log_sums(total, weight_ref, tiles_ref, pairs, live_ref, exponent_ref, rows_ref, low_ref)
    rest = jnp.concatenate([tail_rows(None), jnp.zeros((DEPTH - COMP - TAIL, TILE), BF16)], 0)
    last = groups * LANES // TILE - 1

    def every_tile(t):
        parts = [jnp.concatenate([mine_ref[2 * t + k], other_ref[2 * t + k]], 0) for k in range(2)]
        tile = jnp.concatenate([jnp.concatenate(parts, 1), rest], 0)
        return tile

    def step(t, here_ref, highest, next_ref):
        tile = every_tile(jnp.minimum(t + 1, last))
        totals = jnp.zeros((8, TILE), F32)
        tops = []
        for c in range(live_ref.shape[0] // CHUNK):
            exponents = dot(live_ref[chunk(c), :], tile)
            next_ref[chunk(c), :] = exponents
            tops.append(jnp.max(exponents.reshape(CHUNK // 8, 8, TILE), axis=0))
            grown = jnp.exp(here_ref[chunk(c), :] - highest)
            totals = totals + jnp.sum(grown.reshape(CHUNK // 8, 8, TILE), axis=0)
        logs = highest + jnp.log(jnp.sum(totals, axis=0, keepdims=True))
        put_rows(rows_ref, slot_rows + 2 * t, logs)
        return jnp.max(functools.reduce(jnp.maximum, tops), axis=0, keepdims=True)

    def two(i, highest):
        highest = step(2 * i, exponent_ref, highest, second_ref)
        return step(2 * i + 1, second_ref, highest, exponent_ref)

    start = exponents_and_highest(every_tile(0), live_ref, exponent_ref)
    lax.fori_loop(0, (last + 1) // 2, two, start)
    logs_ref[...] = jnp.broadcast_to(rows_ref[...][None], logs_ref.shape)


def places(slot_rows):
    if slot_rows == SMALL_ROWS:
        return (slot_rows - 1, slot_rows - 2), LANES - 1
    return (slot_rows, slot_rows + 1), 0


def third_kernel(
    meta_ref, logs_in_ref, log_count_ref, tiles_in_ref, points_ref, anchored_ref, base_ref,
    free_ref, logden_ref,
    tiles_ref, weight_ref, energy_ref, highest_ref, totals_ref,
):
    copies = logden_ref.shape[0]
    slot_rows = weight_ref.shape[0]
    total = meta_ref[copies]
    pairs = (total + 2 * TILE - 1) // (2 * TILE)
    logs = log_sum_pieces(logs_in_ref)
    (own_row, zero_row), zero_lane = places(slot_rows)
    zero = logs[zero_row : zero_row + 1, zero_lane : zero_lane + 1]
    free_ref[...] = jnp.broadcast_to(zero - logs[own_row : own_row + 1, :], free_ref.shape)
    highest, least = weighted_tiles(
        total, logs[:slot_rows], log_count_ref, tiles_in_ref, tiles_ref, weight_ref
    )
    new_denominators(
        least, base_ref, anchored_ref, points_ref, tiles_ref, pairs, energy_ref, highest_ref, totals_ref
    )
    turned = [totals_ref[pl.ds(b * LANES, LANES), :].T[0:1, :] for b in range(points_ref.shape[0] // LANES)]
    logden = jnp.concatenate(turned, 0) + (highest + zero)
    logden_ref[...] = jnp.broadcast_to(logden[None], logden_ref.shape)


def last_message(logs, slot_rows, groups):
    counted, every = logs[:slot_rows], logs[slot_rows:]
    row, lane = iota(counted.shape, 0), iota(counted.shape, 1)
    if slot_rows == SMALL_ROWS:
        counted = jnp.where((row == slot_rows - 2) & (lane == LANES - 1), every[0, 0], counted)
        return jnp.where(row == slot_rows - 1, every[:, None, :], counted[None])
    return jnp.concatenate(
        [
            jnp.broadcast_to(counted[None], (groups, slot_rows, LANES)), every[:, None, :],
            jnp.broadcast_to(every[0], (groups, 1, LANES)), jnp.zeros((groups, 6, LANES), F32),
        ],
        1,
    )


def iterated(slot_rows, meta, block_fill, mine, other, place, log_count, points):
    samps = lax.axis_size(SAMP)
    groups = mine.shape[0]
    rows = points.shape[0]
    tile_count = slot_rows * LANES // TILE
    shape = jax.ShapeDtypeStruct
    vmem = pl.BlockSpec(memory_space=pltpu.VMEM)
    smem = pl.BlockSpec(memory_space=pltpu.SMEM)
    params = pltpu.CompilerParams(vmem_limit_bytes=24 << 20)
    tiles_work = pltpu.VMEM((tile_count, DEPTH, TILE), BF16)
    weight_work = pltpu.VMEM((slot_rows, LANES), F32)
    energy_work = pltpu.VMEM((tile_count, rows, TILE), F32)
    column_work = pltpu.VMEM((rows, LANES), F32)
    live_work = pltpu.VMEM((rows, DEPTH), BF16)
    exponent_work = pltpu.VMEM((rows, TILE), F32)
    low_work = pltpu.VMEM((8, TILE), F32)
    logs, tiles, anchored, base = pl.pallas_call(
        first_kernel,
        out_shape=(
            shape((samps, slot_rows, LANES), F32), shape((tile_count, DEPTH, TILE), BF16), shape((rows, DEPTH), BF16),
            shape((rows, LANES), F32),
        ),
        in_specs=[smem, smem, vmem, vmem, vmem, vmem, vmem], out_specs=(vmem,) * 4,
        scratch_shapes=[
            pltpu.VMEM((slot_rows + 2, COMP, LANES), F32), energy_work, column_work, live_work, exponent_work, low_work,
            weight_work, weight_work,
        ],
        compiler_params=params, name="first",
    )(meta, block_fill, mine, other, place, log_count, points)
    logs = log_sum(exchanged(logs, SAMP))
    logs = copies_of_each(logs, STATE)
    logs = pl.pallas_call(
        second_kernel,
        out_shape=shape((samps, slot_rows + groups, LANES), F32),
        in_specs=[smem, smem] + [vmem] * 8, out_specs=vmem,
        scratch_shapes=[
            tiles_work, weight_work, energy_work, column_work, column_work, live_work, exponent_work, exponent_work,
            low_work, pltpu.VMEM((slot_rows + groups, LANES), F32),
        ],
        compiler_params=params, name="second",
    )(meta, block_fill, logs, mine, other, log_count, tiles, points, anchored, base)
    logs = last_message(log_sum(exchanged(logs, SAMP)), slot_rows, groups)
    logs = exchanged(logs, STATE)
    free, logden = pl.pallas_call(
        third_kernel,
        out_shape=(shape((8, LANES), F32), shape((groups, rows // LANES, LANES), F32)),
        in_specs=[smem] + [vmem] * 6, out_specs=(vmem, vmem),
        scratch_shapes=[tiles_work, weight_work, energy_work, column_work, column_work],
        compiler_params=params, name="third",
    )(meta, logs, log_count, tiles, points, anchored, base)
    return free[0], exchanged(logden, STATE).reshape(-1)


def shards(components, coefficients, block_window, block_fill):
    groups = lax.axis_size(STATE)
    samps = lax.axis_size(SAMP)
    position = lax.axis_index(STATE)
    core = lax.axis_index(SAMP[1])
    rows = components.shape[1] // groups
    slot_rows = min(samps * block_window.shape[0] // LANES, groups)
    shape = jax.ShapeDtypeStruct
    vmem = pl.BlockSpec(memory_space=pltpu.VMEM)
    params = pltpu.CompilerParams(vmem_limit_bytes=24 << 20)
    spot = jnp.stack([position, core]).astype(jnp.int32)

    half = COMP // 2
    mine = copies_of_each(lax.dynamic_slice_in_dim(coefficients, core * half, half, 0), STATE)
    blocks = jnp.stack([block_window, block_fill])[None]
    blocks = jnp.concatenate([blocks, lax.ppermute(blocks, SAMP[1], [(0, 1), (1, 0)])], 0)
    along = lax.axis_size(SAMP[0])
    turns = [[(i, (i + k) % along) for i in range(along)] for k in range(1, along)]
    pieces = [blocks] + [lax.ppermute(blocks, SAMP[0], turn) for turn in turns]
    points = pl.pallas_call(
        points_kernel,
        out_shape=shape((rows, DEPTH), BF16),
        in_specs=[pl.BlockSpec(memory_space=pltpu.SMEM), vmem], out_specs=vmem,
        compiler_params=params, name="points",
    )(spot, lax.dynamic_slice_in_dim(components, position * rows, rows, 1))
    other = lax.ppermute(mine, SAMP[1], [(0, 1), (1, 0)])
    place, meta, log_count = pl.pallas_call(
        count_kernel,
        out_shape=(
            shape((groups, LANES), jnp.int32), shape((groups + 8, LANES), jnp.int32),
            shape((slot_rows, LANES), F32),
        ),
        in_specs=[vmem] * len(pieces), out_specs=(vmem, vmem, vmem), compiler_params=params, name="count",
    )(*pieces)
    total = meta[groups, 0]
    meta = jnp.concatenate([meta[: groups + 1, 0], spot[:1]])
    return lax.cond(
        total <= SMALL,
        functools.partial(iterated, SMALL_ROWS), functools.partial(iterated, slot_rows),
        meta, block_fill, mine, other, place, log_count, points,
    )


def solution(mesh):
    torus = Mesh(mesh.devices.reshape(4, 2, 8, 4), ("samp_0", "samp_1", "state_0", "state_1"))
    placed = (P(None, SAMP), P(None, STATE), P(SAMP), P(SAMP))
    return jax.shard_map(
        shards, mesh=torus, in_specs=placed, out_specs=(P(STATE), P(SAMP)), check_vma=False
    )
```

```python
import functools

import jax
import jax.numpy as jnp
from jax import lax
from jax.experimental import pallas as pl
from jax.experimental.pallas import tpu as pltpu
from jax.sharding import Mesh
from jax.sharding import PartitionSpec as P


BLOCK = 128
LANES = 128
COMP = 64
TILE = 256
DEPTH = 128
CHUNK = 256
TAIL = 16
LEAST = 1e-25
SPREAD = 50.0
SMALL_ROWS = 8
SMALL = (SMALL_ROWS - 1) * LANES - 1
STATE = ("state_0", "state_1")
SAMP = ("samp_0", "samp_1")
NEGATIVE = -1e30
BF16 = jnp.bfloat16
F32 = jnp.float32


def exchanged(copies, axes):
    return lax.all_to_all(copies, axes, split_axis=0, concat_axis=0, tiled=True)


def copies_of_each(x, axes):
    return exchanged(jnp.broadcast_to(x, (lax.axis_size(axes), *x.shape)), axes)


def iota(shape, dim):
    return lax.broadcasted_iota(jnp.int32, shape, dim)


def dot_nt(a, b):
    return lax.dot_general(a, b, (((1,), (1,)), ((), ())), preferred_element_type=F32)


def dot(a, b):
    return jnp.dot(a, b, preferred_element_type=F32)


def three_parts(x):
    high = x.astype(BF16).astype(F32)
    rest = x - high
    middle = rest.astype(BF16).astype(F32)
    return high, middle, rest - middle


def log_sum(logs):
    highest = jnp.max(logs, axis=0)
    return highest + jnp.log(jnp.sum(jnp.exp(logs - highest[None]), axis=0))


def log_sum_pieces(logs_ref):
    pieces = logs_ref.shape[0]
    highest = functools.reduce(jnp.maximum, [logs_ref[p] for p in range(pieces)])
    totals = functools.reduce(jnp.add, [jnp.exp(logs_ref[p] - highest) for p in range(pieces)])
    return highest + jnp.log(totals)


def chunk(c):
    return pl.ds(c * CHUNK, CHUNK)


def halves(combine, x):
    return combine(x[:, :LANES], x[:, LANES:])


def points_kernel(spot_ref, block_ref, points_ref):
    rows = points_ref.shape[0]
    half = COMP // 2
    own = pl.multiple_of(spot_ref[1] * half, half)
    lane = iota((LANES, DEPTH - COMP), 1)
    ones = jnp.where((lane >= 3) & (lane < 6), 1.0, 0.0)
    for b in range(rows // LANES):
        at = slice(b * LANES, (b + 1) * LANES)
        mine = block_ref[pl.ds(own, half), at].astype(F32)
        other = block_ref[pl.ds(pl.multiple_of(half - own, half), half), at].astype(F32)
        turned = -jnp.concatenate([mine, other], 0).T
        points_ref[at, :] = jnp.concatenate([turned, ones], 1).astype(BF16)


def count_kernel(*refs):
    blocks_refs, (place_ref, meta_ref, log_count_ref) = refs[:-3], refs[-3:]
    groups = place_ref.shape[0]
    slots = log_count_ref.shape[0]
    width = blocks_refs[0].shape[2]
    counts = jnp.zeros((groups, LANES), F32)
    for blocks_ref, s in [(r, s) for r in blocks_refs for s in range(r.shape[0])]:
        window = blocks_ref[s, 0:1, :]
        fill = blocks_ref[s, 1:2, :]
        of_group = jnp.where(iota((groups, width), 0) == window >> 7, fill, 0).astype(F32).astype(BF16)
        of_lane = jnp.where(iota((LANES, width), 0) == (window & 127), 1.0, 0.0).astype(BF16)
        counts = counts + dot_nt(of_group, of_lane)
    counted = counts > 0
    packed = jnp.where(counted, 1.0, 0.0).astype(BF16)
    before = jnp.where(iota((LANES, LANES), 0) < iota((LANES, LANES), 1), 1.0, 0.0).astype(BF16)
    within = dot(packed, before)
    total = dot(packed, jnp.ones((LANES, LANES), BF16))
    earlier = jnp.where(iota((groups, groups), 1) < iota((groups, groups), 0), 1.0, 0.0).astype(BF16)
    offset_int = dot(earlier, total.astype(BF16)).astype(jnp.int32)
    within_int = within.astype(jnp.int32)
    place_ref[...] = jnp.where(counted, (offset_int & 127) + within_int, -1)
    meta_ref[0:groups, :] = offset_int >> 7
    everything = jnp.sum(total, axis=0, keepdims=True).astype(jnp.int32)
    meta_ref[groups : groups + 8, :] = jnp.broadcast_to(everything, (8, LANES))
    whole = jnp.where(counted, offset_int + within_int, -1)
    counts_int = counts.astype(jnp.int32)
    digits = (counts_int >> 14, (counts_int >> 7) & 127, counts_int & 127)
    gathered = jnp.zeros((3 * slots, LANES), F32)
    for t in range(groups):
        row = whole[t : t + 1, :]
        slot = iota((slots, LANES), 0) == row >> 7
        parts = [jnp.where(slot, d[t : t + 1, :], 0).astype(F32) for d in digits]
        of_lane = jnp.where(iota((LANES, LANES), 0) == (row & 127), 1.0, 0.0).astype(BF16)
        gathered = gathered + dot_nt(jnp.concatenate(parts, 0).astype(BF16), of_lane)
    compact = gathered[0:slots] * 16384.0 + gathered[slots : 2 * slots] * 128.0 + gathered[2 * slots :]
    log_count_ref[...] = jnp.where(compact > 0, jnp.log(jnp.maximum(compact, 1.0)), NEGATIVE)


def tail_rows(weight):
    row = iota((TAIL, TILE), 0)
    rows = jnp.where(row < 3, 1.0, 0.0)
    if weight is not None:
        for k, part in enumerate(three_parts(weight)):
            rows = jnp.where(row == 3 + k, part, rows)
    return rows.astype(BF16)


def with_shift(points, shift):
    lane = iota(points.shape, 1)
    for k, part in enumerate(three_parts(shift)):
        points = jnp.where(lane == COMP + k, part, points)
    return points


def tile_row(rows, j):
    return jnp.concatenate([rows[2 * j : 2 * j + 1, :], rows[2 * j + 1 : 2 * j + 2, :]], 1)


def find_denominators(points_ref, tiles_ref, pairs, energy_ref, highest_ref, totals_ref):
    rows = points_ref.shape[0]
    highest_ref[...] = jnp.full(highest_ref.shape, 4 * NEGATIVE, F32)
    totals_ref[...] = jnp.zeros(totals_ref.shape, F32)

    def find(i, carry):
        for c in range(rows // CHUNK):
            top = highest_ref[chunk(c), :]
            for k in range(2):
                exponents = dot(points_ref[chunk(c), :], tiles_ref[2 * i + k])
                energy_ref[2 * i + k, chunk(c), :] = exponents
                top = jnp.maximum(top, halves(jnp.maximum, exponents))
            highest_ref[chunk(c), :] = top
        return carry

    lax.fori_loop(0, pairs, find, 0)
    for c in range(rows // CHUNK):
        top = jnp.max(highest_ref[chunk(c), :], axis=1, keepdims=True)
        highest_ref[chunk(c), :] = jnp.broadcast_to(top, (CHUNK, LANES))

    def add(i, carry):
        for c in range(rows // CHUNK):
            top = highest_ref[chunk(c), :]
            top = jnp.concatenate([top, top], 1)
            sums = totals_ref[chunk(c), :]
            for k in range(2):
                sums = sums + halves(jnp.add, jnp.exp(energy_ref[2 * i + k, chunk(c), :] - top))
            totals_ref[chunk(c), :] = sums
        return carry

    lax.fori_loop(0, pairs, add, 0)
    for c in range(rows // CHUNK):
        sums = jnp.sum(totals_ref[chunk(c), :], axis=1, keepdims=True)
        logden = highest_ref[chunk(c), :][:, 0:1] + jnp.log(sums)
        totals_ref[chunk(c), :] = jnp.broadcast_to(logden, (CHUNK, LANES))


def denominators_near(base_ref, anchored_ref, tiles_ref, pairs, totals_ref):
    rows = anchored_ref.shape[0]
    totals_ref[...] = jnp.zeros(totals_ref.shape, F32)

    def add(i, carry):
        for c in range(rows // CHUNK):
            sums = totals_ref[chunk(c), :]
            for k in range(2):
                sums = sums + halves(jnp.add, jnp.exp(dot(anchored_ref[chunk(c), :], tiles_ref[2 * i + k])))
            totals_ref[chunk(c), :] = sums
        return carry

    lax.fori_loop(0, pairs, add, 0)
    for c in range(rows // CHUNK):
        sums = jnp.sum(totals_ref[chunk(c), :], axis=1, keepdims=True)
        logden = base_ref[chunk(c), :][:, 0:1] + jnp.log(sums)
        totals_ref[chunk(c), :] = jnp.broadcast_to(logden, (CHUNK, LANES))


def put_live(points_ref, totals_ref, live_ref, fill_ref, first_block, anchored_ref=None):
    row = iota((BLOCK, LANES), 0)
    for b in range(points_ref.shape[0] // BLOCK):
        at = pl.ds(b * BLOCK, BLOCK)
        points = points_ref[at, :].astype(F32)
        logden = totals_ref[at, :]
        if anchored_ref is not None:
            anchored_ref[at, :] = with_shift(points, -logden).astype(BF16)
        shift = jnp.where(row < fill_ref[first_block + b], -logden, NEGATIVE)
        live_ref[at, :] = with_shift(points, shift).astype(BF16)


def exponents_and_highest(tile, live_ref, exponent_ref):
    highest = None
    for c in range(live_ref.shape[0] // CHUNK):
        exponents = dot(live_ref[chunk(c), :], tile)
        exponent_ref[chunk(c), :] = exponents
        top = jnp.max(exponents.reshape(CHUNK // 8, 8, TILE), axis=0)
        highest = top if highest is None else jnp.maximum(highest, top)
    return jnp.max(highest, axis=0, keepdims=True)


def log_of_sum(highest, exponent_ref):
    totals = jnp.zeros((8, TILE), F32)
    for c in range(exponent_ref.shape[0] // CHUNK):
        grown = jnp.exp(exponent_ref[chunk(c), :] - highest)
        totals = totals + jnp.sum(grown.reshape(CHUNK // 8, 8, TILE), axis=0)
    return highest + jnp.log(jnp.sum(totals, axis=0, keepdims=True))


def put_rows(logs_ref, first, logs):
    logs_ref[pl.ds(first, 1), :] = logs[:, :LANES]
    logs_ref[pl.ds(first + 1, 1), :] = logs[:, LANES:]


def counted_log_sums(total, weight_ref, tiles_ref, pairs, live_ref, exponent_ref, logs_ref, low_ref):
    low_ref[...] = jnp.zeros(low_ref.shape, F32)
    logs_ref[0 : weight_ref.shape[0], :] = jnp.zeros(weight_ref.shape, F32)

    def finish(j, logs):
        weight = jnp.concatenate([weight_ref[pl.ds(2 * j, 1), :], weight_ref[pl.ds(2 * j + 1, 1), :]], 1)
        valid = iota((1, TILE), 1) < total - j * TILE
        put_rows(logs_ref, 2 * j, jnp.where(valid, logs - weight, 0.0))
        return valid

    def one(i, carry):
        for k in range(2):
            j = 2 * i + k
            totals = jnp.zeros((8, TILE), F32)
            for c in range(live_ref.shape[0] // CHUNK):
                grown = jnp.exp(dot(live_ref[chunk(c), :], tiles_ref[j]))
                totals = totals + jnp.sum(grown.reshape(CHUNK // 8, 8, TILE), axis=0)
            totals = jnp.sum(totals, axis=0, keepdims=True)
            valid = finish(j, jnp.log(totals))
            low_ref[0:1, :] = jnp.maximum(low_ref[0:1, :], jnp.where(valid & (totals < LEAST), 1.0, 0.0))
        return carry

    lax.fori_loop(0, pairs, one, 0)

    @pl.when(jnp.max(low_ref[...]) > 0)
    def _():
        def again(j, carry):
            highest = exponents_and_highest(tiles_ref[j], live_ref, exponent_ref)
            finish(j, log_of_sum(highest, exponent_ref))
            return carry

        lax.fori_loop(0, 2 * pairs, again, 0)


def weighted_tiles(total, logs, log_count_ref, tiles_in_ref, tiles_ref, weight_ref):
    valid = iota(logs.shape, 0) * LANES + iota(logs.shape, 1) < total
    free = jnp.where(valid, -logs, 4 * NEGATIVE)
    highest = jnp.max(jnp.max(free, axis=0, keepdims=True), axis=1, keepdims=True)
    free = jnp.where(valid, free - highest, 0.0)
    weight = log_count_ref[0 : weight_ref.shape[0], :] + free
    weight_ref[...] = weight
    for j in range(tiles_ref.shape[0]):
        tiles_ref[j, 0:COMP, :] = tiles_in_ref[j, 0:COMP, :]
        tiles_ref[j, COMP : COMP + TAIL, :] = tail_rows(tile_row(weight, j))
        tiles_ref[j, COMP + TAIL : DEPTH, :] = jnp.zeros((DEPTH - COMP - TAIL, TILE), BF16)
    return highest, jnp.min(free)


def first_kernel(
    meta_ref, fill_ref, mine_ref, other_ref, place_ref, log_count_ref, points_ref,
    logs_ref, tiles_ref, anchored_ref, base_ref,
    packed_ref, energy_ref, highest_ref, live_ref, exponent_ref, low_ref, rows_ref, weight_ref,
):
    groups = mine_ref.shape[0]
    total = meta_ref[groups]
    pairs = (total + 2 * TILE - 1) // (2 * TILE)
    packed_ref[...] = jnp.zeros(packed_ref.shape, F32)
    for t in range(groups):
        chosen = jnp.where(iota((2 * LANES, LANES), 0) == place_ref[t : t + 1, :], 1.0, 0.0).astype(BF16)
        moved = dot_nt(jnp.concatenate([mine_ref[t], other_ref[t]], 0), chosen)
        at = meta_ref[t]
        packed_ref[at] += moved[:, :LANES]
        packed_ref[at + 1] += moved[:, LANES:]
    log_count = log_count_ref[0 : logs_ref.shape[1], :]
    weight_ref[...] = log_count
    for j in range(tiles_ref.shape[0]):
        tiles_ref[j, 0:COMP, :] = jnp.concatenate([packed_ref[2 * j], packed_ref[2 * j + 1]], 1).astype(BF16)
        tiles_ref[j, COMP : COMP + TAIL, :] = tail_rows(tile_row(log_count, j))
        tiles_ref[j, COMP + TAIL : DEPTH, :] = jnp.zeros((DEPTH - COMP - TAIL, TILE), BF16)
    find_denominators(points_ref, tiles_ref, pairs, energy_ref, highest_ref, base_ref)
    first_block = meta_ref[groups + 1] * (points_ref.shape[0] // BLOCK)
    put_live(points_ref, base_ref, live_ref, fill_ref, first_block, anchored_ref)
    counted_log_sums(total, weight_ref, tiles_ref, pairs, live_ref, exponent_ref, rows_ref, low_ref)
    logs_ref[...] = jnp.broadcast_to(rows_ref[...][None], logs_ref.shape)


def new_denominators(least, base_ref, anchored_ref, points_ref, tiles_ref, pairs, energy_ref, highest_ref, totals_ref):
    near = least > -SPREAD

    @pl.when(near)
    def _():
        denominators_near(base_ref, anchored_ref, tiles_ref, pairs, totals_ref)

    @pl.when(jnp.logical_not(near))
    def _():
        find_denominators(points_ref, tiles_ref, pairs, energy_ref, highest_ref, totals_ref)


def second_kernel(
    meta_ref, fill_ref, logs_in_ref, mine_ref, other_ref, log_count_ref, tiles_in_ref, points_ref, anchored_ref, base_ref,
    logs_ref,
    tiles_ref, weight_ref, energy_ref, highest_ref, totals_ref, live_ref, exponent_ref, second_ref, low_ref, rows_ref,
):
    groups = mine_ref.shape[0]
    slot_rows = weight_ref.shape[0]
    total = meta_ref[groups]
    pairs = (total + 2 * TILE - 1) // (2 * TILE)
    logs = log_sum_pieces(logs_in_ref)
    _, least = weighted_tiles(total, logs, log_count_ref, tiles_in_ref, tiles_ref, weight_ref)
    new_denominators(
        least, base_ref, anchored_ref, points_ref, tiles_ref, pairs, energy_ref, highest_ref, totals_ref
    )
    first_block = meta_ref[groups + 1] * (points_ref.shape[0] // BLOCK)
    put_live(points_ref, totals_ref, live_ref, fill_ref, first_block)
    counted_log_sums(total, weight_ref, tiles_ref, pairs, live_ref, exponent_ref, rows_ref, low_ref)
    rest = jnp.concatenate([tail_rows(None), jnp.zeros((DEPTH - COMP - TAIL, TILE), BF16)], 0)
    last = groups * LANES // TILE - 1

    def every_tile(t):
        parts = [jnp.concatenate([mine_ref[2 * t + k], other_ref[2 * t + k]], 0) for k in range(2)]
        tile = jnp.concatenate([jnp.concatenate(parts, 1), rest], 0)
        return tile

    def step(t, here_ref, highest, next_ref):
        tile = every_tile(jnp.minimum(t + 1, last))
        totals = jnp.zeros((8, TILE), F32)
        tops = []
        for c in range(live_ref.shape[0] // CHUNK):
            exponents = dot(live_ref[chunk(c), :], tile)
            next_ref[chunk(c), :] = exponents
            tops.append(jnp.max(exponents.reshape(CHUNK // 8, 8, TILE), axis=0))
            grown = jnp.exp(here_ref[chunk(c), :] - highest)
            totals = totals + jnp.sum(grown.reshape(CHUNK // 8, 8, TILE), axis=0)
        logs = highest + jnp.log(jnp.sum(totals, axis=0, keepdims=True))
        put_rows(rows_ref, slot_rows + 2 * t, logs)
        return jnp.max(functools.reduce(jnp.maximum, tops), axis=0, keepdims=True)

    def two(i, highest):
        highest = step(2 * i, exponent_ref, highest, second_ref)
        return step(2 * i + 1, second_ref, highest, exponent_ref)

    start = exponents_and_highest(every_tile(0), live_ref, exponent_ref)
    lax.fori_loop(0, (last + 1) // 2, two, start)
    logs_ref[...] = jnp.broadcast_to(rows_ref[...][None], logs_ref.shape)


def message_kernel(logs_ref, message_ref):
    groups = message_ref.shape[0]
    slot_rows = logs_ref.shape[1] - groups
    (own_row, zero_row), zero_lane = places(slot_rows)
    logs = log_sum_pieces(logs_ref)
    rows = message_ref.shape[1]
    common = logs[0:slot_rows, :]
    if rows > slot_rows:
        common = jnp.concatenate([common, jnp.zeros((rows - slot_rows, LANES), F32)], 0)
    row, lane = iota(common.shape, 0), iota(common.shape, 1)
    common = jnp.where((row == zero_row) & (lane == zero_lane), logs[slot_rows : slot_rows + 1, 0:1], common)
    for t in range(groups):
        own = logs[slot_rows + t : slot_rows + t + 1, :]
        message_ref[t] = jnp.where(row == own_row, own, common)


def places(slot_rows):
    if slot_rows == SMALL_ROWS:
        return (slot_rows - 1, slot_rows - 2), LANES - 1
    return (slot_rows, slot_rows + 1), 0


def third_kernel(
    meta_ref, logs_in_ref, log_count_ref, tiles_in_ref, points_ref, anchored_ref, base_ref,
    free_ref, logden_ref,
    tiles_ref, weight_ref, energy_ref, highest_ref, totals_ref,
):
    copies = logden_ref.shape[0]
    slot_rows = weight_ref.shape[0]
    total = meta_ref[copies]
    pairs = (total + 2 * TILE - 1) // (2 * TILE)
    logs = log_sum_pieces(logs_in_ref)
    (own_row, zero_row), zero_lane = places(slot_rows)
    zero = logs[zero_row : zero_row + 1, zero_lane : zero_lane + 1]
    free_ref[...] = zero - logs[own_row : own_row + 1, :]
    highest, least = weighted_tiles(
        total, logs[:slot_rows], log_count_ref, tiles_in_ref, tiles_ref, weight_ref
    )
    new_denominators(
        least, base_ref, anchored_ref, points_ref, tiles_ref, pairs, energy_ref, highest_ref, totals_ref
    )
    turned = [totals_ref[pl.ds(b * LANES, LANES), :].T[0:1, :] for b in range(points_ref.shape[0] // LANES)]
    logden = jnp.concatenate(turned, 0) + (highest + zero)
    logden_ref[...] = jnp.broadcast_to(logden[None], logden_ref.shape)


def iterated(slot_rows, meta, block_fill, mine, other, place, log_count, points):
    samps = lax.axis_size(SAMP)
    groups = mine.shape[0]
    rows = points.shape[0]
    tile_count = slot_rows * LANES // TILE
    shape = jax.ShapeDtypeStruct
    vmem = pl.BlockSpec(memory_space=pltpu.VMEM)
    smem = pl.BlockSpec(memory_space=pltpu.SMEM)
    params = pltpu.CompilerParams(vmem_limit_bytes=24 << 20)
    tiles_work = pltpu.VMEM((tile_count, DEPTH, TILE), BF16)
    weight_work = pltpu.VMEM((slot_rows, LANES), F32)
    energy_work = pltpu.VMEM((tile_count, rows, TILE), F32)
    column_work = pltpu.VMEM((rows, LANES), F32)
    live_work = pltpu.VMEM((rows, DEPTH), BF16)
    exponent_work = pltpu.VMEM((rows, TILE), F32)
    low_work = pltpu.VMEM((8, TILE), F32)
    logs, tiles, anchored, base = pl.pallas_call(
        first_kernel,
        out_shape=(
            shape((samps, slot_rows, LANES), F32), shape((tile_count, DEPTH, TILE), BF16), shape((rows, DEPTH), BF16),
            shape((rows, LANES), F32),
        ),
        in_specs=[smem, smem, vmem, vmem, vmem, vmem, vmem], out_specs=(vmem,) * 4,
        scratch_shapes=[
            pltpu.VMEM((slot_rows + 2, COMP, LANES), F32), energy_work, column_work, live_work, exponent_work, low_work,
            weight_work, weight_work,
        ],
        compiler_params=params, name="first",
    )(meta, block_fill, mine, other, place, log_count, points)
    logs = log_sum(exchanged(logs, SAMP))
    logs = copies_of_each(logs, STATE)
    logs = pl.pallas_call(
        second_kernel,
        out_shape=shape((samps, slot_rows + groups, LANES), F32),
        in_specs=[smem, smem] + [vmem] * 8, out_specs=vmem,
        scratch_shapes=[
            tiles_work, weight_work, energy_work, column_work, column_work, live_work, exponent_work, exponent_work,
            low_work, pltpu.VMEM((slot_rows + groups, LANES), F32),
        ],
        compiler_params=params, name="second",
    )(meta, block_fill, logs, mine, other, log_count, tiles, points, anchored, base)
    logs = pl.pallas_call(
        message_kernel,
        out_shape=shape((groups, slot_rows if slot_rows == SMALL_ROWS else slot_rows + 8, LANES), F32),
        in_specs=[vmem], out_specs=vmem, compiler_params=params, name="message",
    )(exchanged(logs, SAMP))
    logs = exchanged(logs, STATE)
    return pl.pallas_call(
        third_kernel,
        out_shape=(shape((1, LANES), F32), shape((groups, rows // LANES, LANES), F32)),
        in_specs=[smem] + [vmem] * 6, out_specs=(vmem, vmem),
        scratch_shapes=[tiles_work, weight_work, energy_work, column_work, column_work],
        compiler_params=params, name="third",
    )(meta, logs, log_count, tiles, points, anchored, base)


def shards(components, coefficients, block_window, block_fill):
    groups = lax.axis_size(STATE)
    samps = lax.axis_size(SAMP)
    position = lax.axis_index(STATE)
    core = lax.axis_index(SAMP[1])
    rows = components.shape[1] // groups
    slot_rows = min(samps * block_window.shape[0] // LANES, groups)
    shape = jax.ShapeDtypeStruct
    vmem = pl.BlockSpec(memory_space=pltpu.VMEM)
    params = pltpu.CompilerParams(vmem_limit_bytes=24 << 20)
    spot = jnp.stack([position, core]).astype(jnp.int32)

    half = COMP // 2
    mine = copies_of_each(lax.dynamic_slice_in_dim(coefficients, core * half, half, 0), STATE)
    blocks = jnp.stack([block_window, block_fill])[None]
    blocks = jnp.concatenate([blocks, lax.ppermute(blocks, SAMP[1], [(0, 1), (1, 0)])], 0)
    along = lax.axis_size(SAMP[0])
    turns = [[(i, (i + k) % along) for i in range(along)] for k in range(1, along)]
    pieces = [blocks] + [lax.ppermute(blocks, SAMP[0], turn) for turn in turns]
    points = pl.pallas_call(
        points_kernel,
        out_shape=shape((rows, DEPTH), BF16),
        in_specs=[pl.BlockSpec(memory_space=pltpu.SMEM), vmem], out_specs=vmem,
        compiler_params=params, name="points",
    )(spot, lax.dynamic_slice_in_dim(components, position * rows, rows, 1))
    other = lax.ppermute(mine, SAMP[1], [(0, 1), (1, 0)])
    place, meta, log_count = pl.pallas_call(
        count_kernel,
        out_shape=(
            shape((groups, LANES), jnp.int32), shape((groups + 8, LANES), jnp.int32),
            shape((slot_rows, LANES), F32),
        ),
        in_specs=[vmem] * len(pieces), out_specs=(vmem, vmem, vmem), compiler_params=params, name="count",
    )(*pieces)
    total = meta[groups, 0]
    meta = jnp.concatenate([meta[: groups + 1, 0], spot[:1]])
    free, logden = lax.cond(
        total <= SMALL,
        functools.partial(iterated, SMALL_ROWS), functools.partial(iterated, slot_rows),
        meta, block_fill, mine, other, place, log_count, points,
    )
    return free.reshape(-1), exchanged(logden, STATE).reshape(-1)


def solution(mesh):
    torus = Mesh(mesh.devices.reshape(4, 2, 8, 4), ("samp_0", "samp_1", "state_0", "state_1"))
    placed = (P(None, SAMP), P(None, STATE), P(SAMP), P(SAMP))
    return jax.shard_map(
        shards, mesh=torus, in_specs=placed, out_specs=(P(STATE), P(SAMP)), check_vma=False
    )
```

```python
import functools

import jax
import jax.numpy as jnp
from jax import lax
from jax.experimental import pallas as pl
from jax.experimental.pallas import tpu as pltpu
from jax.sharding import Mesh
from jax.sharding import PartitionSpec as P


BLOCK = 128
LANES = 128
COMP = 64
TILE = 256
PARTS = 3
LOG2E = 1.4426950408889634
LN2 = 0.6931471805599453
CHUNK = 512
TAIL = 16
LEAST = 1e-25
SPREAD = 72.0
SMALL_ROWS = 8
SMALL = (SMALL_ROWS - 1) * LANES - 1
STATE = ("state_0", "state_1")
SAMP = ("samp_0", "samp_1")
NEGATIVE = -1e30
BF16 = jnp.bfloat16
F32 = jnp.float32


def exchanged(copies, axes):
    return lax.all_to_all(copies, axes, split_axis=0, concat_axis=0, tiled=True)


def copies_of_each(x, axes):
    return exchanged(jnp.broadcast_to(x, (lax.axis_size(axes), *x.shape)), axes)


def iota(shape, dim):
    return lax.broadcasted_iota(jnp.int32, shape, dim)


def dot_nt(a, b):
    return lax.dot_general(a, b, (((1,), (1,)), ((), ())), preferred_element_type=F32)


def dot(a, b):
    return jnp.dot(a, b, preferred_element_type=F32)


def three_parts(x):
    high = x.astype(BF16).astype(F32)
    rest = x - high
    middle = rest.astype(BF16).astype(F32)
    return high, middle, rest - middle


def log_sum(logs):
    highest = jnp.max(logs, axis=0)
    return highest + jnp.log(jnp.sum(jnp.exp(logs - highest[None]), axis=0))


def log_sum_pieces(logs_ref):
    pieces = logs_ref.shape[0]
    highest = functools.reduce(jnp.maximum, [logs_ref[p] for p in range(pieces)])
    totals = functools.reduce(jnp.add, [jnp.exp(logs_ref[p] - highest) for p in range(pieces)])
    return highest + jnp.log(totals)


def chunk(c):
    return pl.ds(c * CHUNK if isinstance(c, int) else pl.multiple_of(c * CHUNK, CHUNK), CHUNK)


def halves(combine, x):
    return combine(x[:, :LANES], x[:, LANES:])


def points_kernel(spot_ref, block_ref, head_ref, points_ref):
    rows = points_ref.shape[0]
    half = COMP // 2
    own = pl.multiple_of(spot_ref[1] * half, half)
    lane = iota((LANES, LANES - COMP), 1)
    ones = jnp.where((lane >= 3) & (lane < 6), 1.0, 0.0)
    for b in range(rows // LANES):
        at = slice(b * LANES, (b + 1) * LANES)
        mine = block_ref[pl.ds(own, half), at].astype(F32)
        other = block_ref[pl.ds(pl.multiple_of(half - own, half), half), at].astype(F32)
        high, middle, low = three_parts(jnp.concatenate([mine, other], 0).T * -LOG2E)
        head_ref[at, :] = jnp.concatenate([high, middle], 1).astype(BF16)
        points_ref[at, :] = jnp.concatenate([low, ones], 1).astype(BF16)


def count_kernel(*refs):
    blocks_refs, (place_ref, meta_ref, log_count_ref) = refs[:-3], refs[-3:]
    groups = place_ref.shape[0]
    slots = log_count_ref.shape[0]
    width = blocks_refs[0].shape[2]
    counts = jnp.zeros((groups, LANES), F32)
    for blocks_ref, s in [(r, s) for r in blocks_refs for s in range(r.shape[0])]:
        window = blocks_ref[s, 0:1, :]
        fill = blocks_ref[s, 1:2, :]
        of_group = jnp.where(iota((groups, width), 0) == window >> 7, fill, 0).astype(F32).astype(BF16)
        of_lane = jnp.where(iota((LANES, width), 0) == (window & 127), 1.0, 0.0).astype(BF16)
        counts = counts + dot_nt(of_group, of_lane)
    counted = counts > 0
    packed = jnp.where(counted, 1.0, 0.0).astype(BF16)
    before = jnp.where(iota((LANES, LANES), 0) < iota((LANES, LANES), 1), 1.0, 0.0).astype(BF16)
    within = dot(packed, before)
    total = dot(packed, jnp.ones((LANES, LANES), BF16))
    earlier = jnp.where(iota((groups, groups), 1) < iota((groups, groups), 0), 1.0, 0.0).astype(BF16)
    offset_int = dot(earlier, total.astype(BF16)).astype(jnp.int32)
    within_int = within.astype(jnp.int32)
    place_ref[...] = jnp.where(counted, (offset_int & 127) + within_int, -1)
    meta_ref[0:groups, :] = offset_int >> 7
    everything = jnp.sum(total, axis=0, keepdims=True).astype(jnp.int32)
    meta_ref[groups : groups + 8, :] = jnp.broadcast_to(everything, (8, LANES))
    whole = jnp.where(counted, offset_int + within_int, -1)
    counts_int = counts.astype(jnp.int32)
    digits = (counts_int >> 14, (counts_int >> 7) & 127, counts_int & 127)
    gathered = jnp.zeros((3 * slots, LANES), F32)
    for t in range(groups):
        row = whole[t : t + 1, :]
        slot = iota((slots, LANES), 0) == row >> 7
        parts = [jnp.where(slot, d[t : t + 1, :], 0).astype(F32) for d in digits]
        of_lane = jnp.where(iota((LANES, LANES), 0) == (row & 127), 1.0, 0.0).astype(BF16)
        gathered = gathered + dot_nt(jnp.concatenate(parts, 0).astype(BF16), of_lane)
    compact = gathered[0:slots] * 16384.0 + gathered[slots : 2 * slots] * 128.0 + gathered[2 * slots :]
    log_count_ref[...] = jnp.where(compact > 0, jnp.log2(jnp.maximum(compact, 1.0)), NEGATIVE)


def tail_rows(weight):
    row = iota((TAIL, TILE), 0)
    rows = jnp.where(row < 3, 1.0, 0.0)
    if weight is not None:
        for k, part in enumerate(three_parts(weight)):
            rows = jnp.where(row == 3 + k, part, rows)
    return jnp.concatenate([rows.astype(BF16), jnp.zeros((LANES - COMP - TAIL, TILE), BF16)], 0)


def whole_tile(coefs, tail):
    return jnp.concatenate([coefs] * PARTS + [tail], 0)


def against(head_ref, points_ref, c, tile):
    return dot(jnp.concatenate([head_ref[chunk(c), :], points_ref[chunk(c), :]], 1), tile)


def with_shift(points, shift):
    lane = iota(points.shape, 1)
    for k, part in enumerate(three_parts(shift)):
        points = jnp.where(lane == COMP + k, part, points)
    return points


def tile_row(rows, j):
    return jnp.concatenate([rows[2 * j : 2 * j + 1, :], rows[2 * j + 1 : 2 * j + 2, :]], 1)


def over_tiles(tile_count, pairs, body, carry):
    if tile_count * TILE == SMALL_ROWS * LANES:
        for j in range(tile_count):
            carry = body(j, carry)
        return carry
    return lax.fori_loop(0, 2 * pairs, body, carry)


def exact_denominators(c, head_ref, points_ref, coefs_ref, tails_ref, pairs, energy_ref):
    def find(j, top):
        exponents = against(head_ref, points_ref, c, whole_tile(coefs_ref[j], tails_ref[j]))
        energy_ref[j] = exponents
        return jnp.maximum(top, halves(jnp.maximum, exponents))

    tile_count = coefs_ref.shape[0]
    top = over_tiles(tile_count, pairs, find, jnp.full((CHUNK, LANES), 4 * NEGATIVE, F32))
    top = jnp.max(top, axis=1, keepdims=True)

    def add(j, sums):
        return sums + halves(jnp.add, jnp.exp2(energy_ref[j] - top))

    sums = over_tiles(tile_count, pairs, add, jnp.zeros((CHUNK, LANES), F32))
    return jnp.broadcast_to(top + jnp.log2(jnp.sum(sums, axis=1, keepdims=True)), (CHUNK, LANES))


def near_denominators(c, base_ref, head_ref, anchored_ref, coefs_ref, tails_ref, pairs):
    def add(j, sums):
        tile = whole_tile(coefs_ref[j], tails_ref[j])
        return sums + halves(jnp.add, jnp.exp2(against(head_ref, anchored_ref, c, tile)))

    sums = over_tiles(coefs_ref.shape[0], pairs, add, jnp.zeros((CHUNK, LANES), F32))
    return base_ref[chunk(c), :] + jnp.log2(jnp.sum(sums, axis=1, keepdims=True))


def put_live(c, points_ref, logden, live_ref, fill_ref, first_block):
    row = iota((BLOCK, LANES), 0)
    for b in range(CHUNK // BLOCK):
        at = pl.ds(pl.multiple_of(c * CHUNK + b * BLOCK, BLOCK), BLOCK)
        here = -logden[b * BLOCK : (b + 1) * BLOCK, :]
        shift = jnp.where(row < fill_ref[first_block + c * (CHUNK // BLOCK) + b], here, NEGATIVE)
        live_ref[at, :] = with_shift(points_ref[at, :].astype(F32), shift).astype(BF16)


def each_chunk(rows, body):
    def one(c, carry):
        body(c)
        return carry

    lax.fori_loop(0, rows // CHUNK, one, 0)


def exponents_and_highest(tile, head_ref, live_ref, exponent_ref):
    highest = None
    for c in range(live_ref.shape[0] // CHUNK):
        exponents = against(head_ref, live_ref, c, tile)
        exponent_ref[chunk(c), :] = exponents
        top = jnp.max(exponents.reshape(CHUNK // 8, 8, TILE), axis=0)
        highest = top if highest is None else jnp.maximum(highest, top)
    return jnp.max(highest, axis=0, keepdims=True)


def log_of_sum(highest, exponent_ref):
    totals = jnp.zeros((8, TILE), F32)
    for c in range(exponent_ref.shape[0] // CHUNK):
        grown = jnp.exp2(exponent_ref[chunk(c), :] - highest)
        totals = totals + jnp.sum(grown.reshape(CHUNK // 8, 8, TILE), axis=0)
    return highest + jnp.log2(jnp.sum(totals, axis=0, keepdims=True))


def put_rows(logs_ref, first, logs):
    logs = logs * LN2
    logs_ref[pl.ds(first, 1), :] = logs[:, :LANES]
    logs_ref[pl.ds(first + 1, 1), :] = logs[:, LANES:]


def counted_log_sums(total, weight_ref, coefs_ref, tails_ref, pairs, head_ref, live_ref, exponent_ref, logs_ref, low_ref):
    low_ref[...] = jnp.zeros(low_ref.shape, F32)
    logs_ref[0 : weight_ref.shape[0], :] = jnp.zeros(weight_ref.shape, F32)

    def finish(j, logs):
        weight = jnp.concatenate([weight_ref[pl.ds(2 * j, 1), :], weight_ref[pl.ds(2 * j + 1, 1), :]], 1)
        valid = iota((1, TILE), 1) < total - j * TILE
        put_rows(logs_ref, 2 * j, jnp.where(valid, logs - weight, 0.0))
        return valid

    def one(i, carry):
        for k in range(2):
            j = 2 * i + k
            totals = jnp.zeros((8, TILE), F32)
            tile = whole_tile(coefs_ref[j], tails_ref[j])
            for c in range(live_ref.shape[0] // CHUNK):
                grown = jnp.exp2(against(head_ref, live_ref, c, tile))
                totals = totals + jnp.sum(grown.reshape(CHUNK // 8, 8, TILE), axis=0)
            totals = jnp.sum(totals, axis=0, keepdims=True)
            valid = finish(j, jnp.log2(totals))
            low_ref[0:1, :] = jnp.maximum(low_ref[0:1, :], jnp.where(valid & (totals < LEAST), 1.0, 0.0))
        return carry

    lax.fori_loop(0, pairs, one, 0)

    @pl.when(jnp.max(low_ref[...]) > 0)
    def _():
        def again(j, carry):
            highest = exponents_and_highest(whole_tile(coefs_ref[j], tails_ref[j]), head_ref, live_ref, exponent_ref)
            finish(j, log_of_sum(highest, exponent_ref))
            return carry

        lax.fori_loop(0, 2 * pairs, again, 0)


def weighted_tails(total, logs, log_count_ref, tails_ref, weight_ref):
    valid = iota(logs.shape, 0) * LANES + iota(logs.shape, 1) < total
    free = jnp.where(valid, logs * -LOG2E, 4 * NEGATIVE)
    highest = jnp.max(jnp.max(free, axis=0, keepdims=True), axis=1, keepdims=True)
    free = jnp.where(valid, free - highest, 0.0)
    weight = log_count_ref[0 : weight_ref.shape[0], :] + free
    weight_ref[...] = weight
    for j in range(tails_ref.shape[0]):
        tails_ref[j] = tail_rows(tile_row(weight, j))
    return highest, jnp.min(free)


def first_kernel(
    meta_ref, fill_ref, mine_ref, other_ref, place_ref, log_count_ref, head_ref, points_ref,
    logs_ref, coefs_ref, anchored_ref, base_ref,
    tails_ref, packed_ref, energy_ref, live_ref, exponent_ref, low_ref, rows_ref, weight_ref,
):
    groups = mine_ref.shape[0]
    total = meta_ref[groups]
    pairs = (total + 2 * TILE - 1) // (2 * TILE)
    packed_ref[...] = jnp.zeros(packed_ref.shape, F32)
    for t in range(groups):
        chosen = jnp.where(iota((2 * LANES, LANES), 0) == place_ref[t : t + 1, :], 1.0, 0.0).astype(BF16)
        moved = dot_nt(jnp.concatenate([mine_ref[t], other_ref[t]], 0), chosen)
        at = meta_ref[t]
        packed_ref[at] += moved[:, :LANES]
        packed_ref[at + 1] += moved[:, LANES:]
    log_count = log_count_ref[0 : logs_ref.shape[1], :]
    weight_ref[...] = log_count
    for j in range(coefs_ref.shape[0]):
        coefs_ref[j] = jnp.concatenate([packed_ref[2 * j], packed_ref[2 * j + 1]], 1).astype(BF16)
        tails_ref[j] = tail_rows(tile_row(log_count, j))
    first_block = meta_ref[groups + 1] * (points_ref.shape[0] // BLOCK)

    def denominators(c):
        logden = exact_denominators(c, head_ref, points_ref, coefs_ref, tails_ref, pairs, energy_ref)
        base_ref[chunk(c), :] = logden
        anchored_ref[chunk(c), :] = with_shift(points_ref[chunk(c), :].astype(F32), -logden).astype(BF16)
        put_live(c, points_ref, logden, live_ref, fill_ref, first_block)

    each_chunk(points_ref.shape[0], denominators)
    counted_log_sums(
        total, weight_ref, coefs_ref, tails_ref, pairs, head_ref, live_ref, exponent_ref, rows_ref, low_ref
    )
    logs_ref[...] = jnp.broadcast_to(rows_ref[...][None], logs_ref.shape)


def new_denominators(least, base_ref, head_ref, anchored_ref, points_ref, coefs_ref, tails_ref, pairs, energy_ref, put):
    rows = points_ref.shape[0]
    near = least > -SPREAD

    @pl.when(near)
    def _():
        each_chunk(
            rows,
            lambda c: put(c, near_denominators(c, base_ref, head_ref, anchored_ref, coefs_ref, tails_ref, pairs)),
        )

    @pl.when(jnp.logical_not(near))
    def _():
        each_chunk(
            rows, lambda c: put(c, exact_denominators(c, head_ref, points_ref, coefs_ref, tails_ref, pairs, energy_ref))
        )


def second_kernel(
    meta_ref, fill_ref, logs_in_ref, mine_ref, other_ref, log_count_ref, coefs_ref, head_ref, points_ref, anchored_ref,
    base_ref,
    logs_ref,
    tails_ref, weight_ref, energy_ref, live_ref, exponent_ref, low_ref, rows_ref,
):
    groups = mine_ref.shape[0]
    slot_rows = weight_ref.shape[0]
    total = meta_ref[groups]
    pairs = (total + 2 * TILE - 1) // (2 * TILE)
    logs = log_sum_pieces(logs_in_ref)
    _, least = weighted_tails(total, logs, log_count_ref, tails_ref, weight_ref)
    first_block = meta_ref[groups + 1] * (points_ref.shape[0] // BLOCK)
    new_denominators(
        least, base_ref, head_ref, anchored_ref, points_ref, coefs_ref, tails_ref, pairs, energy_ref,
        lambda c, logden: put_live(c, points_ref, logden, live_ref, fill_ref, first_block),
    )
    counted_log_sums(
        total, weight_ref, coefs_ref, tails_ref, pairs, head_ref, live_ref, exponent_ref, rows_ref, low_ref
    )
    tail = tail_rows(None)
    last = groups * LANES // TILE - 1

    def every_tile(t):
        parts = [jnp.concatenate([mine_ref[2 * t + k], other_ref[2 * t + k]], 0) for k in range(2)]
        return whole_tile(jnp.concatenate(parts, 1), tail)

    def step(t, highest):
        tile = every_tile(jnp.minimum(t + 1, last))
        totals = jnp.zeros((8, TILE), F32)
        tops = []
        for c in range(live_ref.shape[0] // CHUNK):
            grown = jnp.exp2(exponent_ref[chunk(c), :] - highest)
            totals = totals + jnp.sum(grown.reshape(CHUNK // 8, 8, TILE), axis=0)
            exponents = against(head_ref, live_ref, c, tile)
            exponent_ref[chunk(c), :] = exponents
            tops.append(jnp.max(exponents.reshape(CHUNK // 8, 8, TILE), axis=0))
        logs = highest + jnp.log2(jnp.sum(totals, axis=0, keepdims=True))
        put_rows(rows_ref, slot_rows + 2 * t, logs)
        return jnp.max(functools.reduce(jnp.maximum, tops), axis=0, keepdims=True)

    start = exponents_and_highest(every_tile(0), head_ref, live_ref, exponent_ref)
    lax.fori_loop(0, last + 1, step, start, unroll=2)
    logs_ref[...] = jnp.broadcast_to(rows_ref[...][None], logs_ref.shape)


def message_kernel(logs_ref, message_ref):
    groups = message_ref.shape[0]
    slot_rows = logs_ref.shape[1] - groups
    (own_row, zero_row), zero_lane = places(slot_rows)
    logs = log_sum_pieces(logs_ref)
    rows = message_ref.shape[1]
    common = logs[0:slot_rows, :]
    if rows > slot_rows:
        common = jnp.concatenate([common, jnp.zeros((rows - slot_rows, LANES), F32)], 0)
    row, lane = iota(common.shape, 0), iota(common.shape, 1)
    common = jnp.where((row == zero_row) & (lane == zero_lane), logs[slot_rows : slot_rows + 1, 0:1], common)
    for t in range(groups):
        own = logs[slot_rows + t : slot_rows + t + 1, :]
        message_ref[t] = jnp.where(row == own_row, own, common)


def places(slot_rows):
    if slot_rows == SMALL_ROWS:
        return (slot_rows - 1, slot_rows - 2), LANES - 1
    return (slot_rows, slot_rows + 1), 0


def third_kernel(
    meta_ref, logs_in_ref, log_count_ref, coefs_ref, head_ref, points_ref, anchored_ref, base_ref,
    free_ref, logden_ref,
    tails_ref, weight_ref, energy_ref, totals_ref,
):
    copies = logden_ref.shape[0]
    slot_rows = weight_ref.shape[0]
    total = meta_ref[copies]
    pairs = (total + 2 * TILE - 1) // (2 * TILE)
    logs = log_sum_pieces(logs_in_ref)
    (own_row, zero_row), zero_lane = places(slot_rows)
    zero = logs[zero_row : zero_row + 1, zero_lane : zero_lane + 1]
    free_ref[...] = zero - logs[own_row : own_row + 1, :]
    highest, least = weighted_tails(total, logs[:slot_rows], log_count_ref, tails_ref, weight_ref)

    def put(c, logden):
        totals_ref[chunk(c), :] = logden

    new_denominators(
        least, base_ref, head_ref, anchored_ref, points_ref, coefs_ref, tails_ref, pairs, energy_ref, put
    )
    turned = [totals_ref[pl.ds(b * LANES, LANES), :].T[0:1, :] for b in range(points_ref.shape[0] // LANES)]
    logden = (jnp.concatenate(turned, 0) + highest) * LN2 + zero
    logden_ref[...] = jnp.broadcast_to(logden[None], logden_ref.shape)


def iterated(slot_rows, meta, block_fill, mine, other, place, log_count, head, points):
    samps = lax.axis_size(SAMP)
    groups = mine.shape[0]
    rows = points.shape[0]
    tile_count = slot_rows * LANES // TILE
    shape = jax.ShapeDtypeStruct
    vmem = pl.BlockSpec(memory_space=pltpu.VMEM)
    smem = pl.BlockSpec(memory_space=pltpu.SMEM)
    params = pltpu.CompilerParams(vmem_limit_bytes=24 << 20)
    tails_work = pltpu.VMEM((tile_count, LANES - COMP, TILE), BF16)
    weight_work = pltpu.VMEM((slot_rows, LANES), F32)
    energy_work = pltpu.VMEM((tile_count, CHUNK, TILE), F32)
    live_work = pltpu.VMEM((rows, LANES), BF16)
    exponent_work = pltpu.VMEM((rows, TILE), F32)
    low_work = pltpu.VMEM((8, TILE), F32)
    logs, coefs, anchored, base = pl.pallas_call(
        first_kernel,
        out_shape=(
            shape((samps, slot_rows, LANES), F32), shape((tile_count, COMP, TILE), BF16), shape((rows, LANES), BF16),
            shape((rows, LANES), F32),
        ),
        in_specs=[smem, smem] + [vmem] * 6, out_specs=(vmem,) * 4,
        scratch_shapes=[
            tails_work, pltpu.VMEM((slot_rows + 2, COMP, LANES), F32), energy_work, live_work, exponent_work, low_work,
            weight_work, weight_work,
        ],
        compiler_params=params, name="first",
    )(meta, block_fill, mine, other, place, log_count, head, points)
    logs = log_sum(exchanged(logs, SAMP))
    logs = copies_of_each(logs, STATE)
    logs = pl.pallas_call(
        second_kernel,
        out_shape=shape((samps, slot_rows + groups, LANES), F32),
        in_specs=[smem, smem] + [vmem] * 9, out_specs=vmem,
        scratch_shapes=[
            tails_work, weight_work, energy_work, live_work, exponent_work,
            low_work, pltpu.VMEM((slot_rows + groups, LANES), F32),
        ],
        compiler_params=params, name="second",
    )(meta, block_fill, logs, mine, other, log_count, coefs, head, points, anchored, base)
    logs = pl.pallas_call(
        message_kernel,
        out_shape=shape((groups, slot_rows if slot_rows == SMALL_ROWS else slot_rows + 8, LANES), F32),
        in_specs=[vmem], out_specs=vmem, compiler_params=params, name="message",
    )(exchanged(logs, SAMP))
    logs = exchanged(logs, STATE)
    return pl.pallas_call(
        third_kernel,
        out_shape=(shape((1, LANES), F32), shape((groups, rows // LANES, LANES), F32)),
        in_specs=[smem] + [vmem] * 7, out_specs=(vmem, vmem),
        scratch_shapes=[tails_work, weight_work, energy_work, pltpu.VMEM((rows, LANES), F32)],
        compiler_params=params, name="third",
    )(meta, logs, log_count, coefs, head, points, anchored, base)


def shards(components, coefficients, block_window, block_fill):
    groups = lax.axis_size(STATE)
    samps = lax.axis_size(SAMP)
    position = lax.axis_index(STATE)
    core = lax.axis_index(SAMP[1])
    rows = components.shape[1] // groups
    slot_rows = min(samps * block_window.shape[0] // LANES, groups)
    shape = jax.ShapeDtypeStruct
    vmem = pl.BlockSpec(memory_space=pltpu.VMEM)
    params = pltpu.CompilerParams(vmem_limit_bytes=24 << 20)
    spot = jnp.stack([position, core]).astype(jnp.int32)

    half = COMP // 2
    mine = copies_of_each(lax.dynamic_slice_in_dim(coefficients, core * half, half, 0), STATE)
    blocks = jnp.stack([block_window, block_fill])[None]
    blocks = jnp.concatenate([blocks, lax.ppermute(blocks, SAMP[1], [(0, 1), (1, 0)])], 0)
    along = lax.axis_size(SAMP[0])
    turns = [[(i, (i + k) % along) for i in range(along)] for k in range(1, along)]
    pieces = [blocks] + [lax.ppermute(blocks, SAMP[0], turn) for turn in turns]
    head, points = pl.pallas_call(
        points_kernel,
        out_shape=(shape((rows, LANES), BF16), shape((rows, LANES), BF16)),
        in_specs=[pl.BlockSpec(memory_space=pltpu.SMEM), vmem], out_specs=(vmem, vmem),
        compiler_params=params, name="points",
    )(spot, lax.dynamic_slice_in_dim(components, position * rows, rows, 1))
    other = lax.ppermute(mine, SAMP[1], [(0, 1), (1, 0)])
    place, meta, log_count = pl.pallas_call(
        count_kernel,
        out_shape=(
            shape((groups, LANES), jnp.int32), shape((groups + 8, LANES), jnp.int32),
            shape((slot_rows, LANES), F32),
        ),
        in_specs=[vmem] * len(pieces), out_specs=(vmem, vmem, vmem), compiler_params=params, name="count",
    )(*pieces)
    total = meta[groups, 0]
    meta = jnp.concatenate([meta[: groups + 1, 0], spot[:1]])
    free, logden = lax.cond(
        total <= SMALL,
        functools.partial(iterated, SMALL_ROWS), functools.partial(iterated, slot_rows),
        meta, block_fill, mine, other, place, log_count, head, points,
    )
    return free.reshape(-1), exchanged(logden, STATE).reshape(-1)


def solution(mesh):
    torus = Mesh(mesh.devices.reshape(4, 2, 8, 4), ("samp_0", "samp_1", "state_0", "state_1"))
    placed = (P(None, SAMP), P(None, STATE), P(SAMP), P(SAMP))
    return jax.shard_map(
        shards, mesh=torus, in_specs=placed, out_specs=(P(STATE), P(SAMP)), check_vma=False
    )
```

```python
import functools

import jax
import jax.numpy as jnp
from jax import lax
from jax.experimental import pallas as pl
from jax.experimental.pallas import tpu as pltpu
from jax.sharding import Mesh
from jax.sharding import PartitionSpec as P


BLOCK = 128
LANES = 128
COMP = 64
TILE = 256
PARTS = 3
LOG2E = 1.4426950408889634
LN2 = 0.6931471805599453
CHUNK = 512
TAIL = 16
LEAST = 1e-25
SPREAD = 72.0
SMALL_ROWS = 8
SMALL = (SMALL_ROWS - 1) * LANES - 1
STATE = ("state_0", "state_1")
SAMP = ("samp_0", "samp_1")
NEGATIVE = -1e30
BF16 = jnp.bfloat16
F32 = jnp.float32


def exchanged(copies, axes):
    return lax.all_to_all(copies, axes, split_axis=0, concat_axis=0, tiled=True)


def copies_of_each(x, axes):
    return exchanged(jnp.broadcast_to(x, (lax.axis_size(axes), *x.shape)), axes)


def iota(shape, dim):
    return lax.broadcasted_iota(jnp.int32, shape, dim)


def dot_nt(a, b):
    return lax.dot_general(a, b, (((1,), (1,)), ((), ())), preferred_element_type=F32)


def dot(a, b):
    return jnp.dot(a, b, preferred_element_type=F32)


def three_parts(x):
    high = x.astype(BF16).astype(F32)
    rest = x - high
    middle = rest.astype(BF16).astype(F32)
    return high, middle, rest - middle


def log_sum(logs):
    highest = jnp.max(logs, axis=0)
    return highest + jnp.log(jnp.sum(jnp.exp(logs - highest[None]), axis=0))


def log_sum_pieces(logs_ref):
    pieces = logs_ref.shape[0]
    highest = functools.reduce(jnp.maximum, [logs_ref[p] for p in range(pieces)])
    totals = functools.reduce(jnp.add, [jnp.exp(logs_ref[p] - highest) for p in range(pieces)])
    return highest + jnp.log(totals)


def chunk(c):
    return pl.ds(c * CHUNK if isinstance(c, int) else pl.multiple_of(c * CHUNK, CHUNK), CHUNK)


def halves(combine, x):
    return combine(x[:, :LANES], x[:, LANES:])


def points_kernel(spot_ref, fill_ref, block_ref, head_ref, points_ref, dead_ref):
    rows = points_ref.shape[0]
    half = COMP // 2
    own = pl.multiple_of(spot_ref[1] * half, half)
    lane = iota((LANES, LANES - COMP), 1)
    ones = jnp.where((lane >= 3) & (lane < 6), 1.0, 0.0)
    for b in range(rows // LANES):
        at = slice(b * LANES, (b + 1) * LANES)
        mine = block_ref[pl.ds(own, half), at].astype(F32)
        other = block_ref[pl.ds(pl.multiple_of(half - own, half), half), at].astype(F32)
        high, middle, low = three_parts(jnp.concatenate([mine, other], 0).T * -LOG2E)
        head_ref[at, :] = jnp.concatenate([high, middle], 1).astype(BF16)
        points_ref[at, :] = jnp.concatenate([low, ones], 1).astype(BF16)
        fill = fill_ref[spot_ref[0] * (rows // BLOCK) + b]
        dead_ref[at, :] = jnp.where(iota((BLOCK, LANES), 0) < fill, 0.0, NEGATIVE)


def count_kernel(*refs):
    blocks_refs, (place_ref, meta_ref, log_count_ref) = refs[:-3], refs[-3:]
    groups = place_ref.shape[0]
    slots = log_count_ref.shape[0]
    width = blocks_refs[0].shape[2]
    counts = jnp.zeros((groups, LANES), F32)
    for blocks_ref, s in [(r, s) for r in blocks_refs for s in range(r.shape[0])]:
        window = blocks_ref[s, 0:1, :]
        fill = blocks_ref[s, 1:2, :]
        of_group = jnp.where(iota((groups, width), 0) == window >> 7, fill, 0).astype(F32).astype(BF16)
        of_lane = jnp.where(iota((LANES, width), 0) == (window & 127), 1.0, 0.0).astype(BF16)
        counts = counts + dot_nt(of_group, of_lane)
    counted = counts > 0
    packed = jnp.where(counted, 1.0, 0.0).astype(BF16)
    before = jnp.where(iota((LANES, LANES), 0) < iota((LANES, LANES), 1), 1.0, 0.0).astype(BF16)
    within = dot(packed, before)
    total = dot(packed, jnp.ones((LANES, LANES), BF16))
    earlier = jnp.where(iota((groups, groups), 1) < iota((groups, groups), 0), 1.0, 0.0).astype(BF16)
    offset_int = dot(earlier, total.astype(BF16)).astype(jnp.int32)
    within_int = within.astype(jnp.int32)
    place_ref[...] = jnp.where(counted, (offset_int & 127) + within_int, -1)
    meta_ref[0:groups, :] = offset_int >> 7
    everything = jnp.sum(total, axis=0, keepdims=True).astype(jnp.int32)
    meta_ref[groups : groups + 8, :] = jnp.broadcast_to(everything, (8, LANES))
    whole = jnp.where(counted, offset_int + within_int, -1)
    counts_int = counts.astype(jnp.int32)
    digits = (counts_int >> 14, (counts_int >> 7) & 127, counts_int & 127)
    gathered = jnp.zeros((3 * slots, LANES), F32)
    for t in range(groups):
        row = whole[t : t + 1, :]
        slot = iota((slots, LANES), 0) == row >> 7
        parts = [jnp.where(slot, d[t : t + 1, :], 0).astype(F32) for d in digits]
        of_lane = jnp.where(iota((LANES, LANES), 0) == (row & 127), 1.0, 0.0).astype(BF16)
        gathered = gathered + dot_nt(jnp.concatenate(parts, 0).astype(BF16), of_lane)
    compact = gathered[0:slots] * 16384.0 + gathered[slots : 2 * slots] * 128.0 + gathered[2 * slots :]
    log_count_ref[...] = jnp.where(compact > 0, jnp.log2(jnp.maximum(compact, 1.0)), NEGATIVE)


def tail_rows(weight):
    row = iota((TAIL, TILE), 0)
    rows = jnp.where(row < 3, 1.0, 0.0)
    if weight is not None:
        for k, part in enumerate(three_parts(weight)):
            rows = jnp.where(row == 3 + k, part, rows)
    return jnp.concatenate([rows.astype(BF16), jnp.zeros((LANES - COMP - TAIL, TILE), BF16)], 0)


def whole_tile(coefs, tail):
    return jnp.concatenate([coefs] * PARTS + [tail], 0)


def against(head_ref, points_ref, c, tile):
    return dot(jnp.concatenate([head_ref[chunk(c), :], points_ref[chunk(c), :]], 1), tile)


def with_shift(points, shift):
    lane = iota(points.shape, 1)
    for k, part in enumerate(three_parts(shift)):
        points = jnp.where(lane == COMP + k, part, points)
    return points


def tile_row(rows, j):
    return jnp.concatenate([rows[2 * j : 2 * j + 1, :], rows[2 * j + 1 : 2 * j + 2, :]], 1)


def over_tiles(tile_count, body, carry):
    if tile_count * TILE == SMALL_ROWS * LANES:
        for j in range(tile_count):
            carry = body(j, carry)
        return carry
    return lax.fori_loop(0, tile_count, body, carry)


def exact_denominators(c, head_ref, points_ref, coefs_ref, tails_ref, energy_ref):
    def find(j, top):
        exponents = against(head_ref, points_ref, c, whole_tile(coefs_ref[j], tails_ref[j]))
        energy_ref[j] = exponents
        return jnp.maximum(top, halves(jnp.maximum, exponents))

    tile_count = coefs_ref.shape[0]
    top = over_tiles(tile_count, find, jnp.full((CHUNK, LANES), 4 * NEGATIVE, F32))
    top = jnp.max(top, axis=1, keepdims=True)

    def add(j, sums):
        return sums + halves(jnp.add, jnp.exp2(energy_ref[j] - top))

    sums = over_tiles(tile_count, add, jnp.zeros((CHUNK, LANES), F32))
    return jnp.broadcast_to(top + jnp.log2(jnp.sum(sums, axis=1, keepdims=True)), (CHUNK, LANES))


def near_denominators(c, base_ref, head_ref, anchored_ref, coefs_ref, tails_ref):
    def add(j, sums):
        tile = whole_tile(coefs_ref[j], tails_ref[j])
        return sums + halves(jnp.add, jnp.exp2(against(head_ref, anchored_ref, c, tile)))

    sums = over_tiles(coefs_ref.shape[0], add, jnp.zeros((CHUNK, LANES), F32))
    return base_ref[chunk(c), :] + jnp.log2(jnp.sum(sums, axis=1, keepdims=True))


def put_live(c, points_ref, logden, live_ref, dead_ref):
    shift = dead_ref[chunk(c), :] - logden
    live_ref[chunk(c), :] = with_shift(points_ref[chunk(c), :].astype(F32), shift).astype(BF16)


def each_chunk(rows, body):
    def one(c, carry):
        body(c)
        return carry

    lax.fori_loop(0, rows // CHUNK, one, 0)


def exponents_and_highest(tile, head_ref, live_ref, exponent_ref):
    highest = None
    for c in range(live_ref.shape[0] // CHUNK):
        exponents = against(head_ref, live_ref, c, tile)
        exponent_ref[chunk(c), :] = exponents
        top = jnp.max(exponents.reshape(CHUNK // 8, 8, TILE), axis=0)
        highest = top if highest is None else jnp.maximum(highest, top)
    return jnp.max(highest, axis=0, keepdims=True)


def log_of_sum(highest, exponent_ref):
    totals = jnp.zeros((8, TILE), F32)
    for c in range(exponent_ref.shape[0] // CHUNK):
        grown = jnp.exp2(exponent_ref[chunk(c), :] - highest)
        totals = totals + jnp.sum(grown.reshape(CHUNK // 8, 8, TILE), axis=0)
    return highest + jnp.log2(jnp.sum(totals, axis=0, keepdims=True))


def put_rows(logs_ref, first, logs):
    logs = logs * LN2
    logs_ref[pl.ds(first, 1), :] = logs[:, :LANES]
    logs_ref[pl.ds(first + 1, 1), :] = logs[:, LANES:]


def counted_log_sums(weight_ref, coefs_ref, tails_ref, head_ref, live_ref, exponent_ref, logs_ref, low_ref):
    low_ref[...] = jnp.zeros(low_ref.shape, F32)
    logs_ref[0 : weight_ref.shape[0], :] = jnp.zeros(weight_ref.shape, F32)

    def finish(j, logs):
        weight = jnp.concatenate([weight_ref[pl.ds(2 * j, 1), :], weight_ref[pl.ds(2 * j + 1, 1), :]], 1)
        valid = weight > NEGATIVE / 2
        put_rows(logs_ref, 2 * j, jnp.where(valid, logs - weight, 0.0))
        return valid

    def one(i, carry):
        for k in range(2):
            j = 2 * i + k
            totals = jnp.zeros((8, TILE), F32)
            tile = whole_tile(coefs_ref[j], tails_ref[j])
            for c in range(live_ref.shape[0] // CHUNK):
                grown = jnp.exp2(against(head_ref, live_ref, c, tile))
                totals = totals + jnp.sum(grown.reshape(CHUNK // 8, 8, TILE), axis=0)
            totals = jnp.sum(totals, axis=0, keepdims=True)
            valid = finish(j, jnp.log2(totals))
            low_ref[0:1, :] = jnp.maximum(low_ref[0:1, :], jnp.where(valid & (totals < LEAST), 1.0, 0.0))
        return carry

    lax.fori_loop(0, coefs_ref.shape[0] // 2, one, 0)

    @pl.when(jnp.max(low_ref[...]) > 0)
    def _():
        def again(j, carry):
            highest = exponents_and_highest(whole_tile(coefs_ref[j], tails_ref[j]), head_ref, live_ref, exponent_ref)
            finish(j, log_of_sum(highest, exponent_ref))
            return carry

        lax.fori_loop(0, coefs_ref.shape[0], again, 0)


def weighted_tails(logs, log_count_ref, tails_ref, weight_ref):
    log_count = log_count_ref[0 : weight_ref.shape[0], :]
    valid = log_count > NEGATIVE / 2
    free = jnp.where(valid, logs * -LOG2E, 4 * NEGATIVE)
    highest = jnp.max(jnp.max(free, axis=0, keepdims=True), axis=1, keepdims=True)
    free = jnp.where(valid, free - highest, 0.0)
    weight = log_count + free
    weight_ref[...] = weight
    for j in range(tails_ref.shape[0]):
        tails_ref[j] = tail_rows(tile_row(weight, j))
    return highest, jnp.min(free)


def first_kernel(
    meta_ref, mine_ref, other_ref, place_ref, log_count_ref, head_ref, points_ref, dead_ref,
    logs_ref, coefs_ref, anchored_ref, base_ref,
    tails_ref, packed_ref, energy_ref, live_ref, exponent_ref, low_ref, rows_ref, weight_ref,
):
    groups = mine_ref.shape[0]
    packed_ref[...] = jnp.zeros(packed_ref.shape, F32)
    for t in range(groups):
        chosen = jnp.where(iota((2 * LANES, LANES), 0) == place_ref[t : t + 1, :], 1.0, 0.0).astype(BF16)
        moved = dot_nt(jnp.concatenate([mine_ref[t], other_ref[t]], 0), chosen)
        at = meta_ref[t]
        packed_ref[at] += moved[:, :LANES]
        packed_ref[at + 1] += moved[:, LANES:]
    log_count = log_count_ref[0 : logs_ref.shape[1], :]
    weight_ref[...] = log_count
    for j in range(coefs_ref.shape[0]):
        coefs_ref[j] = jnp.concatenate([packed_ref[2 * j], packed_ref[2 * j + 1]], 1).astype(BF16)
        tails_ref[j] = tail_rows(tile_row(log_count, j))

    def denominators(c):
        logden = exact_denominators(c, head_ref, points_ref, coefs_ref, tails_ref, energy_ref)
        base_ref[chunk(c), :] = logden
        anchored_ref[chunk(c), :] = with_shift(points_ref[chunk(c), :].astype(F32), -logden).astype(BF16)
        put_live(c, points_ref, logden, live_ref, dead_ref)

    each_chunk(points_ref.shape[0], denominators)
    counted_log_sums(
        weight_ref, coefs_ref, tails_ref, head_ref, live_ref, exponent_ref, rows_ref, low_ref
    )
    logs_ref[...] = jnp.broadcast_to(rows_ref[...][None], logs_ref.shape)


def new_denominators(least, base_ref, head_ref, anchored_ref, points_ref, coefs_ref, tails_ref, energy_ref, put):
    rows = points_ref.shape[0]
    near = least > -SPREAD

    @pl.when(near)
    def _():
        each_chunk(
            rows,
            lambda c: put(c, near_denominators(c, base_ref, head_ref, anchored_ref, coefs_ref, tails_ref)),
        )

    @pl.when(jnp.logical_not(near))
    def _():
        each_chunk(
            rows, lambda c: put(c, exact_denominators(c, head_ref, points_ref, coefs_ref, tails_ref, energy_ref))
        )


def second_kernel(
    logs_in_ref, mine_ref, other_ref, log_count_ref, coefs_ref, head_ref, points_ref, dead_ref, anchored_ref,
    base_ref,
    logs_ref,
    tails_ref, weight_ref, energy_ref, live_ref, exponent_ref, low_ref, rows_ref,
):
    groups = mine_ref.shape[0]
    slot_rows = weight_ref.shape[0]
    logs = log_sum_pieces(logs_in_ref)
    _, least = weighted_tails(logs, log_count_ref, tails_ref, weight_ref)
    new_denominators(
        least, base_ref, head_ref, anchored_ref, points_ref, coefs_ref, tails_ref, energy_ref,
        lambda c, logden: put_live(c, points_ref, logden, live_ref, dead_ref),
    )
    counted_log_sums(
        weight_ref, coefs_ref, tails_ref, head_ref, live_ref, exponent_ref, rows_ref, low_ref
    )
    tail = tail_rows(None)
    last = groups * LANES // TILE - 1

    def every_tile(t):
        parts = [jnp.concatenate([mine_ref[2 * t + k], other_ref[2 * t + k]], 0) for k in range(2)]
        return whole_tile(jnp.concatenate(parts, 1), tail)

    def step(t, highest):
        tile = every_tile(jnp.minimum(t + 1, last))
        totals = jnp.zeros((8, TILE), F32)
        tops = []
        for c in range(live_ref.shape[0] // CHUNK):
            grown = jnp.exp2(exponent_ref[chunk(c), :] - highest)
            totals = totals + jnp.sum(grown.reshape(CHUNK // 8, 8, TILE), axis=0)
            exponents = against(head_ref, live_ref, c, tile)
            exponent_ref[chunk(c), :] = exponents
            tops.append(jnp.max(exponents.reshape(CHUNK // 8, 8, TILE), axis=0))
        logs = highest + jnp.log2(jnp.sum(totals, axis=0, keepdims=True))
        put_rows(rows_ref, slot_rows + 2 * t, logs)
        return jnp.max(functools.reduce(jnp.maximum, tops), axis=0, keepdims=True)

    start = exponents_and_highest(every_tile(0), head_ref, live_ref, exponent_ref)
    lax.fori_loop(0, last + 1, step, start, unroll=2)
    logs_ref[...] = jnp.broadcast_to(rows_ref[...][None], logs_ref.shape)


def message_kernel(logs_ref, message_ref):
    groups = message_ref.shape[0]
    slot_rows = logs_ref.shape[1] - groups
    (own_row, zero_row), zero_lane = places(slot_rows)
    logs = log_sum_pieces(logs_ref)
    rows = message_ref.shape[1]
    common = logs[0:slot_rows, :]
    if rows > slot_rows:
        common = jnp.concatenate([common, jnp.zeros((rows - slot_rows, LANES), F32)], 0)
    row, lane = iota(common.shape, 0), iota(common.shape, 1)
    common = jnp.where((row == zero_row) & (lane == zero_lane), logs[slot_rows : slot_rows + 1, 0:1], common)
    for t in range(groups):
        own = logs[slot_rows + t : slot_rows + t + 1, :]
        message_ref[t] = jnp.where(row == own_row, own, common)


def places(slot_rows):
    if slot_rows == SMALL_ROWS:
        return (slot_rows - 1, slot_rows - 2), LANES - 1
    return (slot_rows, slot_rows + 1), 0


def third_kernel(
    logs_in_ref, log_count_ref, coefs_ref, head_ref, points_ref, anchored_ref, base_ref,
    free_ref, logden_ref,
    tails_ref, weight_ref, energy_ref, totals_ref,
):
    slot_rows = weight_ref.shape[0]
    logs = log_sum_pieces(logs_in_ref)
    (own_row, zero_row), zero_lane = places(slot_rows)
    zero = logs[zero_row : zero_row + 1, zero_lane : zero_lane + 1]
    free_ref[...] = zero - logs[own_row : own_row + 1, :]
    highest, least = weighted_tails(logs[:slot_rows], log_count_ref, tails_ref, weight_ref)

    def put(c, logden):
        totals_ref[chunk(c), :] = logden

    new_denominators(
        least, base_ref, head_ref, anchored_ref, points_ref, coefs_ref, tails_ref, energy_ref, put
    )
    turned = [totals_ref[pl.ds(b * LANES, LANES), :].T[0:1, :] for b in range(points_ref.shape[0] // LANES)]
    logden = (jnp.concatenate(turned, 0) + highest) * LN2 + zero
    logden_ref[...] = jnp.broadcast_to(logden[None], logden_ref.shape)


def iterated(slot_rows, meta, mine, other, place, log_count, head, points, dead):
    samps = lax.axis_size(SAMP)
    groups = mine.shape[0]
    rows = points.shape[0]
    tile_count = slot_rows * LANES // TILE
    shape = jax.ShapeDtypeStruct
    vmem = pl.BlockSpec(memory_space=pltpu.VMEM)
    smem = pl.BlockSpec(memory_space=pltpu.SMEM)
    params = pltpu.CompilerParams(vmem_limit_bytes=24 << 20)
    tails_work = pltpu.VMEM((tile_count, LANES - COMP, TILE), BF16)
    weight_work = pltpu.VMEM((slot_rows, LANES), F32)
    energy_work = pltpu.VMEM((tile_count, CHUNK, TILE), F32)
    live_work = pltpu.VMEM((rows, LANES), BF16)
    exponent_work = pltpu.VMEM((rows, TILE), F32)
    low_work = pltpu.VMEM((8, TILE), F32)
    logs, coefs, anchored, base = pl.pallas_call(
        first_kernel,
        out_shape=(
            shape((samps, slot_rows, LANES), F32), shape((tile_count, COMP, TILE), BF16), shape((rows, LANES), BF16),
            shape((rows, LANES), F32),
        ),
        in_specs=[smem] + [vmem] * 7, out_specs=(vmem,) * 4,
        scratch_shapes=[
            tails_work, pltpu.VMEM((slot_rows + 2, COMP, LANES), F32), energy_work, live_work, exponent_work, low_work,
            weight_work, weight_work,
        ],
        compiler_params=params, name="first",
    )(meta, mine, other, place, log_count, head, points, dead)
    logs = log_sum(exchanged(logs, SAMP))
    logs = copies_of_each(logs, STATE)
    logs = pl.pallas_call(
        second_kernel,
        out_shape=shape((samps, slot_rows + groups, LANES), F32),
        in_specs=[vmem] * 10, out_specs=vmem,
        scratch_shapes=[
            tails_work, weight_work, energy_work, live_work, exponent_work,
            low_work, pltpu.VMEM((slot_rows + groups, LANES), F32),
        ],
        compiler_params=params, name="second",
    )(logs, mine, other, log_count, coefs, head, points, dead, anchored, base)
    logs = pl.pallas_call(
        message_kernel,
        out_shape=shape((groups, slot_rows if slot_rows == SMALL_ROWS else slot_rows + 8, LANES), F32),
        in_specs=[vmem], out_specs=vmem, compiler_params=params, name="message",
    )(exchanged(logs, SAMP))
    logs = exchanged(logs, STATE)
    return pl.pallas_call(
        third_kernel,
        out_shape=(shape((1, LANES), F32), shape((groups, rows // LANES, LANES), F32)),
        in_specs=[vmem] * 7, out_specs=(vmem, vmem),
        scratch_shapes=[tails_work, weight_work, energy_work, pltpu.VMEM((rows, LANES), F32)],
        compiler_params=params, name="third",
    )(logs, log_count, coefs, head, points, anchored, base)


def shards(components, coefficients, block_window, block_fill):
    groups = lax.axis_size(STATE)
    samps = lax.axis_size(SAMP)
    position = lax.axis_index(STATE)
    core = lax.axis_index(SAMP[1])
    rows = components.shape[1] // groups
    slot_rows = min(samps * block_window.shape[0] // LANES, groups)
    shape = jax.ShapeDtypeStruct
    vmem = pl.BlockSpec(memory_space=pltpu.VMEM)
    smem = pl.BlockSpec(memory_space=pltpu.SMEM)
    params = pltpu.CompilerParams(vmem_limit_bytes=24 << 20)
    spot = jnp.stack([position, core]).astype(jnp.int32)

    half = COMP // 2
    mine = copies_of_each(lax.dynamic_slice_in_dim(coefficients, core * half, half, 0), STATE)
    blocks = jnp.stack([block_window, block_fill])[None]
    blocks = jnp.concatenate([blocks, lax.ppermute(blocks, SAMP[1], [(0, 1), (1, 0)])], 0)
    along = lax.axis_size(SAMP[0])
    turns = [[(i, (i + k) % along) for i in range(along)] for k in range(1, along)]
    pieces = [blocks] + [lax.ppermute(blocks, SAMP[0], turn) for turn in turns]
    head, points, dead = pl.pallas_call(
        points_kernel,
        out_shape=(shape((rows, LANES), BF16), shape((rows, LANES), BF16), shape((rows, LANES), F32)),
        in_specs=[smem, smem, vmem], out_specs=(vmem, vmem, vmem),
        compiler_params=params, name="points",
    )(spot, block_fill, lax.dynamic_slice_in_dim(components, position * rows, rows, 1))
    other = lax.ppermute(mine, SAMP[1], [(0, 1), (1, 0)])
    place, meta, log_count = pl.pallas_call(
        count_kernel,
        out_shape=(
            shape((groups, LANES), jnp.int32), shape((groups + 8, LANES), jnp.int32),
            shape((slot_rows, LANES), F32),
        ),
        in_specs=[vmem] * len(pieces), out_specs=(vmem, vmem, vmem), compiler_params=params, name="count",
    )(*pieces)
    total = meta[groups, 0]
    meta = meta[:groups, 0]
    free, logden = lax.cond(
        total <= SMALL,
        functools.partial(iterated, SMALL_ROWS), functools.partial(iterated, slot_rows),
        meta, mine, other, place, log_count, head, points, dead,
    )
    return free.reshape(-1), exchanged(logden, STATE).reshape(-1)


def solution(mesh):
    torus = Mesh(mesh.devices.reshape(4, 2, 8, 4), ("samp_0", "samp_1", "state_0", "state_1"))
    placed = (P(None, SAMP), P(None, STATE), P(SAMP), P(SAMP))
    return jax.shard_map(
        shards, mesh=torus, in_specs=placed, out_specs=(P(STATE), P(SAMP)), check_vma=False
    )
```

```python
import functools

import jax
import jax.numpy as jnp
from jax import lax
from jax.experimental import pallas as pl
from jax.experimental.pallas import tpu as pltpu
from jax.sharding import Mesh
from jax.sharding import PartitionSpec as P


BLOCK = 128
LANES = 128
COMP = 64
TILE = 256
PARTS = 3
LOG2E = 1.4426950408889634
LN2 = 0.6931471805599453
CHUNK = 512
TAIL = 16
LEAST = 1e-25
SPREAD = 72.0
SMALL_ROWS = 8
SMALL = (SMALL_ROWS - 1) * LANES - 1
STATE = ("state_0", "state_1")
SAMP = ("samp_0", "samp_1")
NEGATIVE = -1e30
BF16 = jnp.bfloat16
F32 = jnp.float32


def exchanged(copies, axes):
    return lax.all_to_all(copies, axes, split_axis=0, concat_axis=0, tiled=True)


def copies_of_each(x, axes):
    return exchanged(jnp.broadcast_to(x, (lax.axis_size(axes), *x.shape)), axes)


def iota(shape, dim):
    return lax.broadcasted_iota(jnp.int32, shape, dim)


def dot_nt(a, b):
    return lax.dot_general(a, b, (((1,), (1,)), ((), ())), preferred_element_type=F32)


def dot(a, b):
    return jnp.dot(a, b, preferred_element_type=F32)


def three_parts(x):
    high = x.astype(BF16).astype(F32)
    rest = x - high
    middle = rest.astype(BF16).astype(F32)
    return high, middle, rest - middle


def log_sum(logs):
    highest = jnp.max(logs, axis=0)
    return highest + jnp.log(jnp.sum(jnp.exp(logs - highest[None]), axis=0))


def log_sum_pieces(logs_ref):
    pieces = logs_ref.shape[0]
    highest = functools.reduce(jnp.maximum, [logs_ref[p] for p in range(pieces)])
    totals = functools.reduce(jnp.add, [jnp.exp(logs_ref[p] - highest) for p in range(pieces)])
    return highest + jnp.log(totals)


def chunk(c):
    return pl.ds(c * CHUNK if isinstance(c, int) else pl.multiple_of(c * CHUNK, CHUNK), CHUNK)


def halves(combine, x):
    return combine(x[:, :LANES], x[:, LANES:])


def points_kernel(spot_ref, own_ref, block_ref, head_ref, points_ref, dead_ref):
    rows = points_ref.shape[0]
    half = COMP // 2
    own = pl.multiple_of(spot_ref[1] * half, half)
    lane = iota((LANES, LANES - COMP), 1)
    ones = jnp.where((lane >= 3) & (lane < 6), 1.0, 0.0)
    for b in range(rows // LANES):
        at = slice(b * LANES, (b + 1) * LANES)
        mine = block_ref[pl.ds(own, half), at].astype(F32)
        other = block_ref[pl.ds(pl.multiple_of(half - own, half), half), at].astype(F32)
        high, middle, low = three_parts(jnp.concatenate([mine, other], 0).T * -LOG2E)
        head_ref[at, :] = jnp.concatenate([high, middle], 1).astype(BF16)
        points_ref[at, :] = jnp.concatenate([low, ones], 1).astype(BF16)
        fills = own_ref[0, 1:2, :]
        chosen = iota(fills.shape, 1) == spot_ref[0] * (rows // BLOCK) + b
        fill = jnp.sum(jnp.where(chosen, fills.astype(F32), 0.0), axis=1, keepdims=True)
        dead_ref[at, :] = jnp.where(iota((BLOCK, LANES), 0).astype(F32) < fill, 0.0, NEGATIVE)


def count_kernel(*refs):
    blocks_refs, (place_ref, meta_ref, digits_ref) = refs[:-3], refs[-3:]
    groups = place_ref.shape[0]
    width = blocks_refs[0].shape[2]
    counts = jnp.zeros((groups, LANES), F32)
    for blocks_ref, s in [(r, s) for r in blocks_refs for s in range(r.shape[0])]:
        window = blocks_ref[s, 0:1, :]
        fill = blocks_ref[s, 1:2, :]
        of_group = jnp.where(iota((groups, width), 0) == window >> 7, fill, 0).astype(F32).astype(BF16)
        of_lane = jnp.where(iota((LANES, width), 0) == (window & 127), 1.0, 0.0).astype(BF16)
        counts = counts + dot_nt(of_group, of_lane)
    counted = counts > 0
    packed = jnp.where(counted, 1.0, 0.0).astype(BF16)
    before = jnp.where(iota((LANES, LANES), 0) < iota((LANES, LANES), 1), 1.0, 0.0).astype(BF16)
    within = dot(packed, before)
    total = dot(packed, jnp.ones((LANES, LANES), BF16))
    earlier = jnp.where(iota((groups, groups), 1) < iota((groups, groups), 0), 1.0, 0.0).astype(BF16)
    offset_int = dot(earlier, total.astype(BF16)).astype(jnp.int32)
    within_int = within.astype(jnp.int32)
    place_ref[...] = jnp.where(counted, (offset_int & 127) + within_int, -1)
    meta_ref[0:groups, :] = offset_int >> 7
    everything = jnp.sum(total, axis=0, keepdims=True).astype(jnp.int32)
    meta_ref[groups : groups + 8, :] = jnp.broadcast_to(everything, (8, LANES))
    counts_int = counts.astype(jnp.int32)
    digits = [d.astype(F32) for d in (counts_int >> 14, (counts_int >> 7) & 127, counts_int & 127)]
    row = iota((TAIL, LANES), 0)
    for t in range(groups):
        rows = jnp.zeros((TAIL, LANES), F32)
        for k, digit in enumerate(digits):
            rows = jnp.where(row == k, digit[t : t + 1, :], rows)
        digits_ref[t] = rows.astype(BF16)


def tail_rows(weight):
    row = iota((TAIL, TILE), 0)
    rows = jnp.where(row < 3, 1.0, 0.0)
    if weight is not None:
        for k, part in enumerate(three_parts(weight)):
            rows = jnp.where(row == 3 + k, part, rows)
    return jnp.concatenate([rows.astype(BF16), jnp.zeros((LANES - COMP - TAIL, TILE), BF16)], 0)


def whole_tile(coefs, tail):
    return jnp.concatenate([coefs] * PARTS + [tail], 0)


def against(head_ref, points_ref, c, tile):
    return dot(jnp.concatenate([head_ref[chunk(c), :], points_ref[chunk(c), :]], 1), tile)


def with_shift(points, shift):
    lane = iota(points.shape, 1)
    for k, part in enumerate(three_parts(shift)):
        points = jnp.where(lane == COMP + k, part, points)
    return points


def tile_row(rows, j):
    return jnp.concatenate([rows[2 * j : 2 * j + 1, :], rows[2 * j + 1 : 2 * j + 2, :]], 1)


def over_tiles(tile_count, body, carry):
    if tile_count * TILE == SMALL_ROWS * LANES:
        for j in range(tile_count):
            carry = body(j, carry)
        return carry
    return lax.fori_loop(0, tile_count, body, carry)


def exact_denominators(c, head_ref, points_ref, coefs_ref, tails_ref, energy_ref):
    def find(j, top):
        exponents = against(head_ref, points_ref, c, whole_tile(coefs_ref[j], tails_ref[j]))
        energy_ref[j] = exponents
        return jnp.maximum(top, halves(jnp.maximum, exponents))

    tile_count = coefs_ref.shape[0]
    top = over_tiles(tile_count, find, jnp.full((CHUNK, LANES), 4 * NEGATIVE, F32))
    top = jnp.max(top, axis=1, keepdims=True)

    def add(j, sums):
        return sums + halves(jnp.add, jnp.exp2(energy_ref[j] - top))

    sums = over_tiles(tile_count, add, jnp.zeros((CHUNK, LANES), F32))
    return jnp.broadcast_to(top + jnp.log2(jnp.sum(sums, axis=1, keepdims=True)), (CHUNK, LANES))


def near_denominators(c, base_ref, head_ref, anchored_ref, coefs_ref, tails_ref):
    def add(j, sums):
        tile = whole_tile(coefs_ref[j], tails_ref[j])
        return sums + halves(jnp.add, jnp.exp2(against(head_ref, anchored_ref, c, tile)))

    sums = over_tiles(coefs_ref.shape[0], add, jnp.zeros((CHUNK, LANES), F32))
    return base_ref[chunk(c), :] + jnp.log2(jnp.sum(sums, axis=1, keepdims=True))


def put_live(c, points_ref, logden, live_ref, dead_ref):
    shift = dead_ref[chunk(c), :] - logden
    live_ref[chunk(c), :] = with_shift(points_ref[chunk(c), :].astype(F32), shift).astype(BF16)


def each_chunk(rows, body):
    def one(c, carry):
        body(c)
        return carry

    lax.fori_loop(0, rows // CHUNK, one, 0)


def exponents_and_highest(tile, head_ref, live_ref, exponent_ref):
    highest = None
    for c in range(live_ref.shape[0] // CHUNK):
        exponents = against(head_ref, live_ref, c, tile)
        exponent_ref[chunk(c), :] = exponents
        top = jnp.max(exponents.reshape(CHUNK // 8, 8, TILE), axis=0)
        highest = top if highest is None else jnp.maximum(highest, top)
    return jnp.max(highest, axis=0, keepdims=True)


def log_of_sum(highest, exponent_ref):
    totals = jnp.zeros((8, TILE), F32)
    for c in range(exponent_ref.shape[0] // CHUNK):
        grown = jnp.exp2(exponent_ref[chunk(c), :] - highest)
        totals = totals + jnp.sum(grown.reshape(CHUNK // 8, 8, TILE), axis=0)
    return highest + jnp.log2(jnp.sum(totals, axis=0, keepdims=True))


def put_rows(logs_ref, first, logs):
    logs = logs * LN2
    logs_ref[pl.ds(first, 1), :] = logs[:, :LANES]
    logs_ref[pl.ds(first + 1, 1), :] = logs[:, LANES:]


def counted_log_sums(weight_ref, coefs_ref, tails_ref, head_ref, live_ref, exponent_ref, logs_ref, low_ref):
    low_ref[...] = jnp.zeros(low_ref.shape, F32)
    logs_ref[0 : weight_ref.shape[0], :] = jnp.zeros(weight_ref.shape, F32)

    def finish(j, logs):
        weight = jnp.concatenate([weight_ref[pl.ds(2 * j, 1), :], weight_ref[pl.ds(2 * j + 1, 1), :]], 1)
        valid = weight > NEGATIVE / 2
        put_rows(logs_ref, 2 * j, jnp.where(valid, logs - weight, 0.0))
        return valid

    def one(i, carry):
        for k in range(2):
            j = 2 * i + k
            totals = jnp.zeros((8, TILE), F32)
            tile = whole_tile(coefs_ref[j], tails_ref[j])
            for c in range(live_ref.shape[0] // CHUNK):
                grown = jnp.exp2(against(head_ref, live_ref, c, tile))
                totals = totals + jnp.sum(grown.reshape(CHUNK // 8, 8, TILE), axis=0)
            totals = jnp.sum(totals, axis=0, keepdims=True)
            valid = finish(j, jnp.log2(totals))
            low_ref[0:1, :] = jnp.maximum(low_ref[0:1, :], jnp.where(valid & (totals < LEAST), 1.0, 0.0))
        return carry

    lax.fori_loop(0, coefs_ref.shape[0] // 2, one, 0)

    @pl.when(jnp.max(low_ref[...]) > 0)
    def _():
        def again(j, carry):
            highest = exponents_and_highest(whole_tile(coefs_ref[j], tails_ref[j]), head_ref, live_ref, exponent_ref)
            finish(j, log_of_sum(highest, exponent_ref))
            return carry

        lax.fori_loop(0, coefs_ref.shape[0], again, 0)


def weighted_tails(logs, log_count_ref, tails_ref, weight_ref):
    log_count = log_count_ref[...]
    valid = log_count > NEGATIVE / 2
    free = jnp.where(valid, logs * -LOG2E, 4 * NEGATIVE)
    highest = jnp.max(jnp.max(free, axis=0, keepdims=True), axis=1, keepdims=True)
    free = jnp.where(valid, free - highest, 0.0)
    weight = log_count + free
    weight_ref[...] = weight
    for j in range(tails_ref.shape[0]):
        tails_ref[j] = tail_rows(tile_row(weight, j))
    return highest, jnp.min(free)


def first_kernel(
    meta_ref, mine_ref, other_ref, place_ref, digits_ref, head_ref, points_ref, dead_ref,
    logs_ref, log_count_ref, coefs_ref, anchored_ref, base_ref,
    tails_ref, packed_ref, energy_ref, live_ref, exponent_ref, low_ref, rows_ref,
):
    groups = mine_ref.shape[0]
    packed_ref[...] = jnp.zeros(packed_ref.shape, F32)
    for t in range(groups):
        chosen = jnp.where(iota((2 * LANES, LANES), 0) == place_ref[t : t + 1, :], 1.0, 0.0).astype(BF16)
        moved = dot_nt(jnp.concatenate([mine_ref[t], other_ref[t], digits_ref[t]], 0), chosen)
        at = meta_ref[t]
        packed_ref[at] += moved[:, :LANES]
        packed_ref[at + 1] += moved[:, LANES:]
    for h in range(log_count_ref.shape[0]):
        digits = [packed_ref[h, COMP + k : COMP + k + 1, :] for k in range(3)]
        counts = digits[0] * 16384.0 + digits[1] * 128.0 + digits[2]
        log_count_ref[h : h + 1, :] = jnp.where(counts > 0, jnp.log2(jnp.maximum(counts, 1.0)), NEGATIVE)
    log_count = log_count_ref[...]
    for j in range(coefs_ref.shape[0]):
        coefs_ref[j] = jnp.concatenate([packed_ref[2 * j, 0:COMP, :], packed_ref[2 * j + 1, 0:COMP, :]], 1).astype(BF16)
        tails_ref[j] = tail_rows(tile_row(log_count, j))

    def denominators(c):
        logden = exact_denominators(c, head_ref, points_ref, coefs_ref, tails_ref, energy_ref)
        base_ref[chunk(c), :] = logden
        anchored_ref[chunk(c), :] = with_shift(points_ref[chunk(c), :].astype(F32), -logden).astype(BF16)
        put_live(c, points_ref, logden, live_ref, dead_ref)

    each_chunk(points_ref.shape[0], denominators)
    counted_log_sums(
        log_count_ref, coefs_ref, tails_ref, head_ref, live_ref, exponent_ref, rows_ref, low_ref
    )
    logs_ref[...] = jnp.broadcast_to(rows_ref[...][None], logs_ref.shape)


def new_denominators(least, base_ref, head_ref, anchored_ref, points_ref, coefs_ref, tails_ref, energy_ref, put):
    rows = points_ref.shape[0]
    near = least > -SPREAD

    @pl.when(near)
    def _():
        each_chunk(
            rows,
            lambda c: put(c, near_denominators(c, base_ref, head_ref, anchored_ref, coefs_ref, tails_ref)),
        )

    @pl.when(jnp.logical_not(near))
    def _():
        each_chunk(
            rows, lambda c: put(c, exact_denominators(c, head_ref, points_ref, coefs_ref, tails_ref, energy_ref))
        )


def second_kernel(
    logs_in_ref, mine_ref, other_ref, log_count_ref, coefs_ref, head_ref, points_ref, dead_ref, anchored_ref,
    base_ref,
    logs_ref,
    tails_ref, weight_ref, energy_ref, live_ref, exponent_ref, low_ref, rows_ref,
):
    groups = mine_ref.shape[0]
    slot_rows = weight_ref.shape[0]
    logs = log_sum_pieces(logs_in_ref)
    _, least = weighted_tails(logs, log_count_ref, tails_ref, weight_ref)
    new_denominators(
        least, base_ref, head_ref, anchored_ref, points_ref, coefs_ref, tails_ref, energy_ref,
        lambda c, logden: put_live(c, points_ref, logden, live_ref, dead_ref),
    )
    counted_log_sums(
        weight_ref, coefs_ref, tails_ref, head_ref, live_ref, exponent_ref, rows_ref, low_ref
    )
    tail = tail_rows(None)
    last = groups * LANES // TILE - 1

    def every_tile(t):
        parts = [jnp.concatenate([mine_ref[2 * t + k], other_ref[2 * t + k]], 0) for k in range(2)]
        return whole_tile(jnp.concatenate(parts, 1), tail)

    def step(t, highest):
        tile = every_tile(jnp.minimum(t + 1, last))
        totals = jnp.zeros((8, TILE), F32)
        tops = []
        for c in range(live_ref.shape[0] // CHUNK):
            grown = jnp.exp2(exponent_ref[chunk(c), :] - highest)
            totals = totals + jnp.sum(grown.reshape(CHUNK // 8, 8, TILE), axis=0)
            exponents = against(head_ref, live_ref, c, tile)
            exponent_ref[chunk(c), :] = exponents
            tops.append(jnp.max(exponents.reshape(CHUNK // 8, 8, TILE), axis=0))
        logs = highest + jnp.log2(jnp.sum(totals, axis=0, keepdims=True))
        put_rows(rows_ref, slot_rows + 2 * t, logs)
        return jnp.max(functools.reduce(jnp.maximum, tops), axis=0, keepdims=True)

    start = exponents_and_highest(every_tile(0), head_ref, live_ref, exponent_ref)
    lax.fori_loop(0, last + 1, step, start, unroll=2)
    logs_ref[...] = jnp.broadcast_to(rows_ref[...][None], logs_ref.shape)


def message_kernel(logs_ref, message_ref):
    groups = message_ref.shape[0]
    slot_rows = logs_ref.shape[1] - groups
    (own_row, zero_row), zero_lane = places(slot_rows)
    logs = log_sum_pieces(logs_ref)
    rows = message_ref.shape[1]
    common = logs[0:slot_rows, :]
    if rows > slot_rows:
        common = jnp.concatenate([common, jnp.zeros((rows - slot_rows, LANES), F32)], 0)
    row, lane = iota(common.shape, 0), iota(common.shape, 1)
    common = jnp.where((row == zero_row) & (lane == zero_lane), logs[slot_rows : slot_rows + 1, 0:1], common)
    for t in range(groups):
        own = logs[slot_rows + t : slot_rows + t + 1, :]
        message_ref[t] = jnp.where(row == own_row, own, common)


def places(slot_rows):
    if slot_rows == SMALL_ROWS:
        return (slot_rows - 1, slot_rows - 2), LANES - 1
    return (slot_rows, slot_rows + 1), 0


def third_kernel(
    logs_in_ref, log_count_ref, coefs_ref, head_ref, points_ref, anchored_ref, base_ref,
    free_ref, logden_ref,
    tails_ref, weight_ref, energy_ref, totals_ref,
):
    slot_rows = weight_ref.shape[0]
    logs = log_sum_pieces(logs_in_ref)
    (own_row, zero_row), zero_lane = places(slot_rows)
    zero = logs[zero_row : zero_row + 1, zero_lane : zero_lane + 1]
    free_ref[...] = zero - logs[own_row : own_row + 1, :]
    highest, least = weighted_tails(logs[:slot_rows], log_count_ref, tails_ref, weight_ref)

    def put(c, logden):
        totals_ref[chunk(c), :] = logden

    new_denominators(
        least, base_ref, head_ref, anchored_ref, points_ref, coefs_ref, tails_ref, energy_ref, put
    )
    turned = [totals_ref[pl.ds(b * LANES, LANES), :].T[0:1, :] for b in range(points_ref.shape[0] // LANES)]
    logden = (jnp.concatenate(turned, 0) + highest) * LN2 + zero
    logden_ref[...] = jnp.broadcast_to(logden[None], logden_ref.shape)


def iterated(slot_rows, meta, mine, other, place, digits, head, points, dead):
    samps = lax.axis_size(SAMP)
    groups = mine.shape[0]
    rows = points.shape[0]
    tile_count = slot_rows * LANES // TILE
    shape = jax.ShapeDtypeStruct
    vmem = pl.BlockSpec(memory_space=pltpu.VMEM)
    smem = pl.BlockSpec(memory_space=pltpu.SMEM)
    params = pltpu.CompilerParams(vmem_limit_bytes=24 << 20)
    tails_work = pltpu.VMEM((tile_count, LANES - COMP, TILE), BF16)
    weight_work = pltpu.VMEM((slot_rows, LANES), F32)
    energy_work = pltpu.VMEM((tile_count, CHUNK, TILE), F32)
    live_work = pltpu.VMEM((rows, LANES), BF16)
    exponent_work = pltpu.VMEM((rows, TILE), F32)
    low_work = pltpu.VMEM((8, TILE), F32)
    logs, log_count, coefs, anchored, base = pl.pallas_call(
        first_kernel,
        out_shape=(
            shape((samps, slot_rows, LANES), F32), shape((slot_rows, LANES), F32), shape((tile_count, COMP, TILE), BF16), shape((rows, LANES), BF16),
            shape((rows, LANES), F32),
        ),
        in_specs=[smem] + [vmem] * 7, out_specs=(vmem,) * 5,
        scratch_shapes=[
            tails_work, pltpu.VMEM((slot_rows + 2, COMP + TAIL, LANES), F32), energy_work, live_work, exponent_work, low_work,
            weight_work,
        ],
        compiler_params=params, name="first",
    )(meta, mine, other, place, digits, head, points, dead)
    logs = log_sum(exchanged(logs, SAMP))
    logs = copies_of_each(logs, STATE)
    logs = pl.pallas_call(
        second_kernel,
        out_shape=shape((samps, slot_rows + groups, LANES), F32),
        in_specs=[vmem] * 10, out_specs=vmem,
        scratch_shapes=[
            tails_work, weight_work, energy_work, live_work, exponent_work,
            low_work, pltpu.VMEM((slot_rows + groups, LANES), F32),
        ],
        compiler_params=params, name="second",
    )(logs, mine, other, log_count, coefs, head, points, dead, anchored, base)
    logs = pl.pallas_call(
        message_kernel,
        out_shape=shape((groups, slot_rows if slot_rows == SMALL_ROWS else slot_rows + 8, LANES), F32),
        in_specs=[vmem], out_specs=vmem, compiler_params=params, name="message",
    )(exchanged(logs, SAMP))
    logs = exchanged(logs, STATE)
    return pl.pallas_call(
        third_kernel,
        out_shape=(shape((1, LANES), F32), shape((groups, rows // LANES, LANES), F32)),
        in_specs=[vmem] * 7, out_specs=(vmem, vmem),
        scratch_shapes=[tails_work, weight_work, energy_work, pltpu.VMEM((rows, LANES), F32)],
        compiler_params=params, name="third",
    )(logs, log_count, coefs, head, points, anchored, base)


def shards(components, coefficients, block_window, block_fill):
    groups = lax.axis_size(STATE)
    samps = lax.axis_size(SAMP)
    position = lax.axis_index(STATE)
    core = lax.axis_index(SAMP[1])
    rows = components.shape[1] // groups
    slot_rows = min(samps * block_window.shape[0] // LANES, groups)
    shape = jax.ShapeDtypeStruct
    vmem = pl.BlockSpec(memory_space=pltpu.VMEM)
    smem = pl.BlockSpec(memory_space=pltpu.SMEM)
    params = pltpu.CompilerParams(vmem_limit_bytes=24 << 20)
    spot = jnp.stack([position, core]).astype(jnp.int32)

    half = COMP // 2
    mine = copies_of_each(lax.dynamic_slice_in_dim(coefficients, core * half, half, 0), STATE)
    pair = jnp.stack([block_window, block_fill])[None]
    blocks = jnp.concatenate([pair, lax.ppermute(pair, SAMP[1], [(0, 1), (1, 0)])], 0)
    along = lax.axis_size(SAMP[0])
    turns = [[(i, (i + k) % along) for i in range(along)] for k in range(1, along)]
    pieces = [blocks] + [lax.ppermute(blocks, SAMP[0], turn) for turn in turns]
    head, points, dead = pl.pallas_call(
        points_kernel,
        out_shape=(shape((rows, LANES), BF16), shape((rows, LANES), BF16), shape((rows, LANES), F32)),
        in_specs=[smem, vmem, vmem], out_specs=(vmem, vmem, vmem),
        compiler_params=params, name="points",
    )(spot, pair, lax.dynamic_slice_in_dim(components, position * rows, rows, 1))
    other = lax.ppermute(mine, SAMP[1], [(0, 1), (1, 0)])
    place, meta, digits = pl.pallas_call(
        count_kernel,
        out_shape=(
            shape((groups, LANES), jnp.int32), shape((groups + 8, LANES), jnp.int32),
            shape((groups, TAIL, LANES), BF16),
        ),
        in_specs=[vmem] * len(pieces), out_specs=(vmem, vmem, vmem), compiler_params=params, name="count",
    )(*pieces)
    total = meta[groups, 0]
    meta = meta[:groups, 0]
    free, logden = lax.cond(
        total <= SMALL,
        functools.partial(iterated, SMALL_ROWS), functools.partial(iterated, slot_rows),
        meta, mine, other, place, digits, head, points, dead,
    )
    return free.reshape(-1), exchanged(logden, STATE).reshape(-1)


def solution(mesh):
    torus = Mesh(mesh.devices.reshape(4, 2, 8, 4), ("samp_0", "samp_1", "state_0", "state_1"))
    placed = (P(None, SAMP), P(None, STATE), P(SAMP), P(SAMP))
    return jax.shard_map(
        shards, mesh=torus, in_specs=placed, out_specs=(P(STATE), P(SAMP)), check_vma=False
    )
```

```python
import functools

import jax
import jax.numpy as jnp
from jax import lax
from jax.experimental import pallas as pl
from jax.experimental.pallas import tpu as pltpu
from jax.sharding import Mesh
from jax.sharding import PartitionSpec as P


BLOCK = 128
LANES = 128
COMP = 64
TILE = 256
PARTS = 3
LOG2E = 1.4426950408889634
LN2 = 0.6931471805599453
CHUNK = 512
TAIL = 16
LEAST = 1e-25
SPREAD = 72.0
SMALL_ROWS = 8
SMALL = (SMALL_ROWS - 1) * LANES - 1
STATE = ("state_0", "state_1")
SAMP = ("samp_0", "samp_1")
NEGATIVE = -1e30
BF16 = jnp.bfloat16
F32 = jnp.float32


def exchanged(copies, axes):
    return lax.all_to_all(copies, axes, split_axis=0, concat_axis=0, tiled=True)


def copies_of_each(x, axes):
    return exchanged(jnp.broadcast_to(x, (lax.axis_size(axes), *x.shape)), axes)


def iota(shape, dim):
    return lax.broadcasted_iota(jnp.int32, shape, dim)


def dot_nt(a, b):
    return lax.dot_general(a, b, (((1,), (1,)), ((), ())), preferred_element_type=F32)


def dot(a, b):
    return jnp.dot(a, b, preferred_element_type=F32)


def three_parts(x):
    high = x.astype(BF16).astype(F32)
    rest = x - high
    middle = rest.astype(BF16).astype(F32)
    return high, middle, rest - middle


def log_sum(logs):
    highest = jnp.max(logs, axis=0)
    return highest + jnp.log(jnp.sum(jnp.exp(logs - highest[None]), axis=0))


def log_sum_pieces(logs_ref):
    pieces = logs_ref.shape[0]
    highest = functools.reduce(jnp.maximum, [logs_ref[p] for p in range(pieces)])
    totals = functools.reduce(jnp.add, [jnp.exp(logs_ref[p] - highest) for p in range(pieces)])
    return highest + jnp.log(totals)


def chunk(c):
    return pl.ds(c * CHUNK if isinstance(c, int) else pl.multiple_of(c * CHUNK, CHUNK), CHUNK)


def halves(combine, x):
    return x if x.shape[1] == LANES else combine(x[:, :LANES], x[:, LANES:])


def used_tile(coefs_ref, tails_ref, j):
    width = LANES if isinstance(j, int) and j == SMALL_ROWS * LANES // TILE - 1 else TILE
    return whole_tile(coefs_ref[j], tails_ref[j])[:, :width]


def points_kernel(spot_ref, own_ref, block_ref, head_ref, points_ref, dead_ref):
    rows = points_ref.shape[0]
    half = COMP // 2
    own = pl.multiple_of(spot_ref[1] * half, half)
    lane = iota((LANES, LANES - COMP), 1)
    ones = jnp.where((lane >= 3) & (lane < 6), 1.0, 0.0)
    for b in range(rows // LANES):
        at = slice(b * LANES, (b + 1) * LANES)
        mine = block_ref[pl.ds(own, half), at].astype(F32)
        other = block_ref[pl.ds(pl.multiple_of(half - own, half), half), at].astype(F32)
        high, middle, low = three_parts(jnp.concatenate([mine, other], 0).T * -LOG2E)
        head_ref[at, :] = jnp.concatenate([high, middle], 1).astype(BF16)
        points_ref[at, :] = jnp.concatenate([low, ones], 1).astype(BF16)
        fills = own_ref[0, 1:2, :]
        chosen = iota(fills.shape, 1) == spot_ref[0] * (rows // BLOCK) + b
        fill = jnp.sum(jnp.where(chosen, fills.astype(F32), 0.0), axis=1, keepdims=True)
        dead_ref[at, :] = jnp.where(iota((BLOCK, LANES), 0).astype(F32) < fill, 0.0, NEGATIVE)


def count_kernel(*refs):
    blocks_refs, (place_ref, meta_ref, digits_ref) = refs[:-3], refs[-3:]
    groups = place_ref.shape[0]
    width = blocks_refs[0].shape[2]
    counts = jnp.zeros((groups, LANES), F32)
    for blocks_ref, s in [(r, s) for r in blocks_refs for s in range(r.shape[0])]:
        window = blocks_ref[s, 0:1, :]
        fill = blocks_ref[s, 1:2, :]
        of_group = jnp.where(iota((groups, width), 0) == window >> 7, fill, 0).astype(F32).astype(BF16)
        of_lane = jnp.where(iota((LANES, width), 0) == (window & 127), 1.0, 0.0).astype(BF16)
        counts = counts + dot_nt(of_group, of_lane)
    counted = counts > 0
    packed = jnp.where(counted, 1.0, 0.0).astype(BF16)
    before = jnp.where(iota((LANES, LANES), 0) < iota((LANES, LANES), 1), 1.0, 0.0).astype(BF16)
    within = dot(packed, before)
    total = dot(packed, jnp.ones((LANES, LANES), BF16))
    earlier = jnp.where(iota((groups, groups), 1) < iota((groups, groups), 0), 1.0, 0.0).astype(BF16)
    offset_int = dot(earlier, total.astype(BF16)).astype(jnp.int32)
    within_int = within.astype(jnp.int32)
    place_ref[...] = jnp.where(counted, (offset_int & 127) + within_int, -1)
    meta_ref[0:groups, :] = offset_int >> 7
    everything = jnp.sum(total, axis=0, keepdims=True).astype(jnp.int32)
    meta_ref[groups : groups + 8, :] = jnp.broadcast_to(everything, (8, LANES))
    counts_int = counts.astype(jnp.int32)
    digits = [d.astype(F32) for d in (counts_int >> 14, (counts_int >> 7) & 127, counts_int & 127)]
    row = iota((TAIL, LANES), 0)
    for t in range(groups):
        rows = jnp.zeros((TAIL, LANES), F32)
        for k, digit in enumerate(digits):
            rows = jnp.where(row == k, digit[t : t + 1, :], rows)
        digits_ref[t] = rows.astype(BF16)


def tail_rows(weight):
    row = iota((TAIL, TILE), 0)
    rows = jnp.where(row < 3, 1.0, 0.0)
    if weight is not None:
        for k, part in enumerate(three_parts(weight)):
            rows = jnp.where(row == 3 + k, part, rows)
    return jnp.concatenate([rows.astype(BF16), jnp.zeros((LANES - COMP - TAIL, TILE), BF16)], 0)


def whole_tile(coefs, tail):
    return jnp.concatenate([coefs] * PARTS + [tail], 0)


def against(head_ref, points_ref, c, tile):
    return dot(jnp.concatenate([head_ref[chunk(c), :], points_ref[chunk(c), :]], 1), tile)


def with_shift(points, shift):
    lane = iota(points.shape, 1)
    for k, part in enumerate(three_parts(shift)):
        points = jnp.where(lane == COMP + k, part, points)
    return points


def tile_row(rows, j):
    return jnp.concatenate([rows[2 * j : 2 * j + 1, :], rows[2 * j + 1 : 2 * j + 2, :]], 1)


def over_tiles(tile_count, body, carry):
    if tile_count * TILE == SMALL_ROWS * LANES:
        for j in range(tile_count):
            carry = body(j, carry)
        return carry
    return lax.fori_loop(0, tile_count, body, carry)


def exact_denominators(c, head_ref, points_ref, coefs_ref, tails_ref, energy_ref):
    def find(j, top):
        exponents = against(head_ref, points_ref, c, used_tile(coefs_ref, tails_ref, j))
        energy_ref[j, :, : exponents.shape[1]] = exponents
        return jnp.maximum(top, halves(jnp.maximum, exponents))

    tile_count = coefs_ref.shape[0]
    top = over_tiles(tile_count, find, jnp.full((CHUNK, LANES), 4 * NEGATIVE, F32))
    top = jnp.max(top, axis=1, keepdims=True)

    def add(j, sums):
        width = used_tile(coefs_ref, tails_ref, j).shape[1]
        return sums + halves(jnp.add, jnp.exp2(energy_ref[j, :, :width] - top))

    sums = over_tiles(tile_count, add, jnp.zeros((CHUNK, LANES), F32))
    return jnp.broadcast_to(top + jnp.log2(jnp.sum(sums, axis=1, keepdims=True)), (CHUNK, LANES))


def near_denominators(c, base_ref, head_ref, anchored_ref, coefs_ref, tails_ref):
    def add(j, sums):
        tile = used_tile(coefs_ref, tails_ref, j)
        return sums + halves(jnp.add, jnp.exp2(against(head_ref, anchored_ref, c, tile)))

    sums = over_tiles(coefs_ref.shape[0], add, jnp.zeros((CHUNK, LANES), F32))
    return base_ref[chunk(c), :] + jnp.log2(jnp.sum(sums, axis=1, keepdims=True))


def put_live(c, points_ref, logden, live_ref, dead_ref):
    shift = dead_ref[chunk(c), :] - logden
    live_ref[chunk(c), :] = with_shift(points_ref[chunk(c), :].astype(F32), shift).astype(BF16)


def each_chunk(rows, body):
    def one(c, carry):
        body(c)
        return carry

    lax.fori_loop(0, rows // CHUNK, one, 0)


def exponents_and_highest(tile, head_ref, live_ref, exponent_ref):
    highest = None
    for c in range(live_ref.shape[0] // CHUNK):
        exponents = against(head_ref, live_ref, c, tile)
        exponent_ref[chunk(c), :] = exponents
        top = jnp.max(exponents.reshape(CHUNK // 8, 8, TILE), axis=0)
        highest = top if highest is None else jnp.maximum(highest, top)
    return jnp.max(highest, axis=0, keepdims=True)


def log_of_sum(highest, exponent_ref):
    totals = jnp.zeros((8, TILE), F32)
    for c in range(exponent_ref.shape[0] // CHUNK):
        grown = jnp.exp2(exponent_ref[chunk(c), :] - highest)
        totals = totals + jnp.sum(grown.reshape(CHUNK // 8, 8, TILE), axis=0)
    return highest + jnp.log2(jnp.sum(totals, axis=0, keepdims=True))


def put_rows(logs_ref, first, logs):
    logs = logs * LN2
    logs_ref[pl.ds(first, 1), :] = logs[:, :LANES]
    logs_ref[pl.ds(first + 1, 1), :] = logs[:, LANES:]


def counted_log_sums(weight_ref, coefs_ref, tails_ref, head_ref, live_ref, exponent_ref, logs_ref, low_ref):
    low_ref[...] = jnp.zeros(low_ref.shape, F32)
    logs_ref[0 : weight_ref.shape[0], :] = jnp.zeros(weight_ref.shape, F32)

    def finish(j, logs):
        weight = jnp.concatenate([weight_ref[pl.ds(2 * j, 1), :], weight_ref[pl.ds(2 * j + 1, 1), :]], 1)
        valid = weight > NEGATIVE / 2
        put_rows(logs_ref, 2 * j, jnp.where(valid, logs - weight, 0.0))
        return valid

    def one(i, carry):
        for k in range(2):
            j = 2 * i + k
            totals = jnp.zeros((8, TILE), F32)
            tile = whole_tile(coefs_ref[j], tails_ref[j])
            for c in range(live_ref.shape[0] // CHUNK):
                grown = jnp.exp2(against(head_ref, live_ref, c, tile))
                totals = totals + jnp.sum(grown.reshape(CHUNK // 8, 8, TILE), axis=0)
            totals = jnp.sum(totals, axis=0, keepdims=True)
            valid = finish(j, jnp.log2(totals))
            low_ref[0:1, :] = jnp.maximum(low_ref[0:1, :], jnp.where(valid & (totals < LEAST), 1.0, 0.0))
        return carry

    lax.fori_loop(0, coefs_ref.shape[0] // 2, one, 0)

    @pl.when(jnp.max(low_ref[...]) > 0)
    def _():
        def again(j, carry):
            highest = exponents_and_highest(whole_tile(coefs_ref[j], tails_ref[j]), head_ref, live_ref, exponent_ref)
            finish(j, log_of_sum(highest, exponent_ref))
            return carry

        lax.fori_loop(0, coefs_ref.shape[0], again, 0)


def weighted_tails(logs, log_count_ref, tails_ref, weight_ref):
    log_count = log_count_ref[...]
    valid = log_count > NEGATIVE / 2
    free = jnp.where(valid, logs * -LOG2E, 4 * NEGATIVE)
    highest = jnp.max(jnp.max(free, axis=0, keepdims=True), axis=1, keepdims=True)
    free = jnp.where(valid, free - highest, 0.0)
    weight = log_count + free
    weight_ref[...] = weight
    for j in range(tails_ref.shape[0]):
        tails_ref[j] = tail_rows(tile_row(weight, j))
    return highest, jnp.min(free)


def first_kernel(
    meta_ref, mine_ref, other_ref, place_ref, digits_ref, head_ref, points_ref, dead_ref,
    logs_ref, log_count_ref, coefs_ref, anchored_ref, base_ref,
    tails_ref, packed_ref, energy_ref, live_ref, exponent_ref, low_ref, rows_ref,
):
    groups = mine_ref.shape[0]
    packed_ref[...] = jnp.zeros(packed_ref.shape, F32)
    for t in range(groups):
        chosen = jnp.where(iota((2 * LANES, LANES), 0) == place_ref[t : t + 1, :], 1.0, 0.0).astype(BF16)
        moved = dot_nt(jnp.concatenate([mine_ref[t], other_ref[t], digits_ref[t]], 0), chosen)
        at = meta_ref[t]
        packed_ref[at] += moved[:, :LANES]
        packed_ref[at + 1] += moved[:, LANES:]
    for h in range(log_count_ref.shape[0]):
        digits = [packed_ref[h, COMP + k : COMP + k + 1, :] for k in range(3)]
        counts = digits[0] * 16384.0 + digits[1] * 128.0 + digits[2]
        log_count_ref[h : h + 1, :] = jnp.where(counts > 0, jnp.log2(jnp.maximum(counts, 1.0)), NEGATIVE)
    log_count = log_count_ref[...]
    for j in range(coefs_ref.shape[0]):
        coefs_ref[j] = jnp.concatenate([packed_ref[2 * j, 0:COMP, :], packed_ref[2 * j + 1, 0:COMP, :]], 1).astype(BF16)
        tails_ref[j] = tail_rows(tile_row(log_count, j))

    def denominators(c):
        logden = exact_denominators(c, head_ref, points_ref, coefs_ref, tails_ref, energy_ref)
        base_ref[chunk(c), :] = logden
        anchored_ref[chunk(c), :] = with_shift(points_ref[chunk(c), :].astype(F32), -logden).astype(BF16)
        put_live(c, points_ref, logden, live_ref, dead_ref)

    each_chunk(points_ref.shape[0], denominators)
    counted_log_sums(
        log_count_ref, coefs_ref, tails_ref, head_ref, live_ref, exponent_ref, rows_ref, low_ref
    )
    logs_ref[...] = jnp.broadcast_to(rows_ref[...][None], logs_ref.shape)


def new_denominators(least, base_ref, head_ref, anchored_ref, points_ref, coefs_ref, tails_ref, energy_ref, put):
    rows = points_ref.shape[0]
    near = least > -SPREAD

    @pl.when(near)
    def _():
        each_chunk(
            rows,
            lambda c: put(c, near_denominators(c, base_ref, head_ref, anchored_ref, coefs_ref, tails_ref)),
        )

    @pl.when(jnp.logical_not(near))
    def _():
        each_chunk(
            rows, lambda c: put(c, exact_denominators(c, head_ref, points_ref, coefs_ref, tails_ref, energy_ref))
        )


def places(slot_rows):
    if slot_rows == SMALL_ROWS:
        return (slot_rows - 1, slot_rows - 2), LANES - 1
    return (slot_rows, slot_rows + 1), 0


def put_message(logs, slot_rows, message_ref):
    (own_row, zero_row), zero_lane = places(slot_rows)
    rows = message_ref.shape[1]
    common = logs[0:slot_rows, :]
    if rows > slot_rows:
        common = jnp.concatenate([common, jnp.zeros((rows - slot_rows, LANES), F32)], 0)
    row, lane = iota(common.shape, 0), iota(common.shape, 1)
    common = jnp.where((row == zero_row) & (lane == zero_lane), logs[slot_rows : slot_rows + 1, 0:1], common)
    for t in range(message_ref.shape[0]):
        own = logs[slot_rows + t : slot_rows + t + 1, :]
        message_ref[t] = jnp.where(row == own_row, own, common)


def second_kernel(
    logs_in_ref, mine_ref, other_ref, log_count_ref, coefs_ref, head_ref, points_ref, dead_ref, anchored_ref,
    base_ref,
    message_ref,
    tails_ref, weight_ref, energy_ref, live_ref, exponent_ref, low_ref, rows_ref,
):
    groups = mine_ref.shape[0]
    slot_rows = weight_ref.shape[0]
    logs = log_sum_pieces(logs_in_ref)
    _, least = weighted_tails(logs, log_count_ref, tails_ref, weight_ref)
    new_denominators(
        least, base_ref, head_ref, anchored_ref, points_ref, coefs_ref, tails_ref, energy_ref,
        lambda c, logden: put_live(c, points_ref, logden, live_ref, dead_ref),
    )
    counted_log_sums(
        weight_ref, coefs_ref, tails_ref, head_ref, live_ref, exponent_ref, rows_ref, low_ref
    )
    tail = tail_rows(None)
    last = groups * LANES // TILE - 1

    def every_tile(t):
        parts = [jnp.concatenate([mine_ref[2 * t + k], other_ref[2 * t + k]], 0) for k in range(2)]
        return whole_tile(jnp.concatenate(parts, 1), tail)

    def step(t, highest):
        tile = every_tile(jnp.minimum(t + 1, last))
        totals = jnp.zeros((8, TILE), F32)
        tops = []
        for c in range(live_ref.shape[0] // CHUNK):
            grown = jnp.exp2(exponent_ref[chunk(c), :] - highest)
            totals = totals + jnp.sum(grown.reshape(CHUNK // 8, 8, TILE), axis=0)
            exponents = against(head_ref, live_ref, c, tile)
            exponent_ref[chunk(c), :] = exponents
            tops.append(jnp.max(exponents.reshape(CHUNK // 8, 8, TILE), axis=0))
        logs = highest + jnp.log2(jnp.sum(totals, axis=0, keepdims=True))
        put_rows(rows_ref, slot_rows + 2 * t, logs)
        return jnp.max(functools.reduce(jnp.maximum, tops), axis=0, keepdims=True)

    start = exponents_and_highest(every_tile(0), head_ref, live_ref, exponent_ref)
    lax.fori_loop(0, last + 1, step, start, unroll=4)
    put_message(rows_ref[...], slot_rows, message_ref)


def third_kernel(
    logs_in_ref, log_count_ref, coefs_ref, head_ref, points_ref, anchored_ref, base_ref,
    free_ref, logden_ref,
    tails_ref, weight_ref, energy_ref, totals_ref,
):
    slot_rows = weight_ref.shape[0]
    logs = log_sum_pieces(logs_in_ref)
    (own_row, zero_row), zero_lane = places(slot_rows)
    zero = logs[zero_row : zero_row + 1, zero_lane : zero_lane + 1]
    free_ref[...] = zero - logs[own_row : own_row + 1, :]
    highest, least = weighted_tails(logs[:slot_rows], log_count_ref, tails_ref, weight_ref)

    def put(c, logden):
        totals_ref[chunk(c), :] = logden

    new_denominators(
        least, base_ref, head_ref, anchored_ref, points_ref, coefs_ref, tails_ref, energy_ref, put
    )
    turned = [totals_ref[pl.ds(b * LANES, LANES), :].T[0:1, :] for b in range(points_ref.shape[0] // LANES)]
    logden = (jnp.concatenate(turned, 0) + highest) * LN2 + zero
    logden_ref[...] = jnp.broadcast_to(logden[None], logden_ref.shape)


def iterated(slot_rows, meta, mine, other, place, digits, head, points, dead):
    samps = lax.axis_size(SAMP)
    groups = mine.shape[0]
    rows = points.shape[0]
    tile_count = slot_rows * LANES // TILE
    shape = jax.ShapeDtypeStruct
    vmem = pl.BlockSpec(memory_space=pltpu.VMEM)
    smem = pl.BlockSpec(memory_space=pltpu.SMEM)
    params = pltpu.CompilerParams(vmem_limit_bytes=24 << 20)
    tails_work = pltpu.VMEM((tile_count, LANES - COMP, TILE), BF16)
    weight_work = pltpu.VMEM((slot_rows, LANES), F32)
    energy_work = pltpu.VMEM((tile_count, CHUNK, TILE), F32)
    live_work = pltpu.VMEM((rows, LANES), BF16)
    exponent_work = pltpu.VMEM((rows, TILE), F32)
    low_work = pltpu.VMEM((8, TILE), F32)
    logs, log_count, coefs, anchored, base = pl.pallas_call(
        first_kernel,
        out_shape=(
            shape((samps, slot_rows, LANES), F32), shape((slot_rows, LANES), F32), shape((tile_count, COMP, TILE), BF16), shape((rows, LANES), BF16),
            shape((rows, LANES), F32),
        ),
        in_specs=[smem] + [vmem] * 7, out_specs=(vmem,) * 5,
        scratch_shapes=[
            tails_work, pltpu.VMEM((slot_rows + 2, COMP + TAIL, LANES), F32), energy_work, live_work, exponent_work, low_work,
            weight_work,
        ],
        compiler_params=params, name="first",
    )(meta, mine, other, place, digits, head, points, dead)
    logs = log_sum(exchanged(logs, SAMP))
    logs = copies_of_each(logs, STATE)
    logs = pl.pallas_call(
        second_kernel,
        out_shape=shape((groups, slot_rows if slot_rows == SMALL_ROWS else slot_rows + 8, LANES), F32),
        in_specs=[vmem] * 10, out_specs=vmem,
        scratch_shapes=[
            tails_work, weight_work, energy_work, live_work, exponent_work,
            low_work, pltpu.VMEM((slot_rows + groups, LANES), F32),
        ],
        compiler_params=params, name="second",
    )(logs, mine, other, log_count, coefs, head, points, dead, anchored, base)
    logs = copies_of_each(log_sum(exchanged(logs, STATE)), SAMP)
    return pl.pallas_call(
        third_kernel,
        out_shape=(shape((1, LANES), F32), shape((groups, rows // LANES, LANES), F32)),
        in_specs=[vmem] * 7, out_specs=(vmem, vmem),
        scratch_shapes=[tails_work, weight_work, energy_work, pltpu.VMEM((rows, LANES), F32)],
        compiler_params=params, name="third",
    )(logs, log_count, coefs, head, points, anchored, base)


def shards(components, coefficients, block_window, block_fill):
    groups = lax.axis_size(STATE)
    samps = lax.axis_size(SAMP)
    position = lax.axis_index(STATE)
    core = lax.axis_index(SAMP[1])
    rows = components.shape[1] // groups
    slot_rows = min(samps * block_window.shape[0] // LANES, groups)
    shape = jax.ShapeDtypeStruct
    vmem = pl.BlockSpec(memory_space=pltpu.VMEM)
    params = pltpu.CompilerParams(vmem_limit_bytes=24 << 20)
    spot = jnp.stack([position, core]).astype(jnp.int32)

    half = COMP // 2
    mine = copies_of_each(lax.dynamic_slice_in_dim(coefficients, core * half, half, 0), STATE)
    pair = jnp.stack([block_window, block_fill])[None]
    blocks = jnp.concatenate([pair, lax.ppermute(pair, SAMP[1], [(0, 1), (1, 0)])], 0)
    along = lax.axis_size(SAMP[0])
    turns = [[(i, (i + k) % along) for i in range(along)] for k in range(1, along)]
    pieces = [blocks] + [lax.ppermute(blocks, SAMP[0], turn) for turn in turns]
    head, points, dead = pl.pallas_call(
        points_kernel,
        out_shape=(shape((rows, LANES), BF16), shape((rows, LANES), BF16), shape((rows, LANES), F32)),
        grid_spec=pltpu.PrefetchScalarGridSpec(
            num_scalar_prefetch=1, grid=(1,),
            in_specs=[
                pl.BlockSpec(pair.shape, lambda i, at: (0, 0, 0)), pl.BlockSpec((COMP, rows), lambda i, at: (0, at[0])),
            ],
            out_specs=(pl.BlockSpec((rows, LANES), lambda i, at: (0, 0)),) * 3,
        ),
        compiler_params=pltpu.CompilerParams(vmem_limit_bytes=60 << 20), name="points",
    )(spot, pair, components)
    other = lax.ppermute(mine, SAMP[1], [(0, 1), (1, 0)])
    place, meta, digits = pl.pallas_call(
        count_kernel,
        out_shape=(
            shape((groups, LANES), jnp.int32), shape((groups + 8, LANES), jnp.int32),
            shape((groups, TAIL, LANES), BF16),
        ),
        in_specs=[vmem] * len(pieces), out_specs=(vmem, vmem, vmem), compiler_params=params, name="count",
    )(*pieces)
    total = meta[groups, 0]
    meta = meta[:groups, 0]
    free, logden = lax.cond(
        total <= SMALL,
        functools.partial(iterated, SMALL_ROWS), functools.partial(iterated, slot_rows),
        meta, mine, other, place, digits, head, points, dead,
    )
    return free.reshape(-1), exchanged(logden, STATE).reshape(-1)


def solution(mesh):
    torus = Mesh(mesh.devices.reshape(4, 2, 8, 4), ("samp_0", "samp_1", "state_0", "state_1"))
    placed = (P(None, SAMP), P(None, STATE), P(SAMP), P(SAMP))
    return jax.shard_map(
        shards, mesh=torus, in_specs=placed, out_specs=(P(STATE), P(SAMP)), check_vma=False
    )
```

```python
import functools

import jax
import jax.numpy as jnp
from jax import lax
from jax.experimental import pallas as pl
from jax.experimental.pallas import tpu as pltpu
from jax.sharding import Mesh
from jax.sharding import PartitionSpec as P


BLOCK = 128
LANES = 128
COMP = 64
TILE = 256
PARTS = 3
LOG2E = 1.4426950408889634
LN2 = 0.6931471805599453
CHUNK = 512
TAIL = 16
LEAST = 1e-25
SPREAD = 72.0
SMALL_ROWS = 8
SMALL = (SMALL_ROWS - 1) * LANES - 1
STATE = ("state_0", "state_1")
SAMP = ("samp_0", "samp_1")
NEGATIVE = -1e30
BF16 = jnp.bfloat16
F32 = jnp.float32


def exchanged(copies, axes):
    return lax.all_to_all(copies, axes, split_axis=0, concat_axis=0, tiled=True)


def copies_of_each(x, axes):
    return exchanged(jnp.broadcast_to(x, (lax.axis_size(axes), *x.shape)), axes)


def iota(shape, dim):
    return lax.broadcasted_iota(jnp.int32, shape, dim)


def dot_nt(a, b):
    return lax.dot_general(a, b, (((1,), (1,)), ((), ())), preferred_element_type=F32)


def dot(a, b):
    return jnp.dot(a, b, preferred_element_type=F32)


def three_parts(x):
    high = x.astype(BF16).astype(F32)
    rest = x - high
    middle = rest.astype(BF16).astype(F32)
    return high, middle, rest - middle


def log_sum(logs):
    highest = jnp.max(logs, axis=0)
    return highest + jnp.log(jnp.sum(jnp.exp(logs - highest[None]), axis=0))


def log_sum_pieces(logs_ref):
    pieces = logs_ref.shape[0]
    highest = functools.reduce(jnp.maximum, [logs_ref[p] for p in range(pieces)])
    totals = functools.reduce(jnp.add, [jnp.exp(logs_ref[p] - highest) for p in range(pieces)])
    return highest + jnp.log(totals)


def chunk(c):
    return pl.ds(c * CHUNK if isinstance(c, int) else pl.multiple_of(c * CHUNK, CHUNK), CHUNK)


def halves(combine, x):
    return x if x.shape[1] == LANES else combine(x[:, :LANES], x[:, LANES:])


def used_tile(coefs_ref, tails_ref, j):
    width = LANES if isinstance(j, int) and j == SMALL_ROWS * LANES // TILE - 1 else TILE
    return whole_tile(coefs_ref[j], tails_ref[j])[:, :width]


def points_kernel(spot_ref, own_ref, block_ref, head_ref, points_ref, dead_ref):
    rows = points_ref.shape[0]
    half = COMP // 2
    own = pl.multiple_of(spot_ref[1] * half, half)
    lane = iota((LANES, LANES - COMP), 1)
    ones = jnp.where((lane >= 3) & (lane < 6), 1.0, 0.0)
    for b in range(rows // LANES):
        at = slice(b * LANES, (b + 1) * LANES)
        mine = block_ref[pl.ds(own, half), at].astype(F32)
        other = block_ref[pl.ds(pl.multiple_of(half - own, half), half), at].astype(F32)
        high, middle, low = three_parts(jnp.concatenate([mine, other], 0).T * -LOG2E)
        head_ref[at, :] = jnp.concatenate([high, middle], 1).astype(BF16)
        points_ref[at, :] = jnp.concatenate([low, ones], 1).astype(BF16)
        fills = own_ref[0, 1:2, :]
        chosen = iota(fills.shape, 1) == spot_ref[0] * (rows // BLOCK) + b
        fill = jnp.sum(jnp.where(chosen, fills.astype(F32), 0.0), axis=1, keepdims=True)
        dead_ref[at, :] = jnp.where(iota((BLOCK, LANES), 0).astype(F32) < fill, 0.0, NEGATIVE)


def count_kernel(*refs):
    blocks_refs, (place_ref, meta_ref, digits_ref) = refs[:-3], refs[-3:]
    groups = place_ref.shape[0]
    width = blocks_refs[0].shape[2]
    counts = jnp.zeros((groups, LANES), F32)
    for blocks_ref, s in [(r, s) for r in blocks_refs for s in range(r.shape[0])]:
        window = blocks_ref[s, 0:1, :]
        fill = blocks_ref[s, 1:2, :]
        of_group = jnp.where(iota((groups, width), 0) == window >> 7, fill, 0).astype(F32).astype(BF16)
        of_lane = jnp.where(iota((LANES, width), 0) == (window & 127), 1.0, 0.0).astype(BF16)
        counts = counts + dot_nt(of_group, of_lane)
    counted = counts > 0
    packed = jnp.where(counted, 1.0, 0.0).astype(BF16)
    before = jnp.where(iota((LANES, LANES), 0) < iota((LANES, LANES), 1), 1.0, 0.0).astype(BF16)
    within = dot(packed, before)
    total = dot(packed, jnp.ones((LANES, LANES), BF16))
    earlier = jnp.where(iota((groups, groups), 1) < iota((groups, groups), 0), 1.0, 0.0).astype(BF16)
    offset_int = dot(earlier, total.astype(BF16)).astype(jnp.int32)
    within_int = within.astype(jnp.int32)
    place_ref[...] = jnp.where(counted, (offset_int & 127) + within_int, -1)
    meta_ref[0:groups, :] = offset_int >> 7
    everything = jnp.sum(total, axis=0, keepdims=True).astype(jnp.int32)
    meta_ref[groups : groups + 8, :] = jnp.broadcast_to(everything, (8, LANES))
    counts_int = counts.astype(jnp.int32)
    digits = [d.astype(F32) for d in (counts_int >> 14, (counts_int >> 7) & 127, counts_int & 127)]
    row = iota((TAIL, LANES), 0)
    for t in range(groups):
        rows = jnp.zeros((TAIL, LANES), F32)
        for k, digit in enumerate(digits):
            rows = jnp.where(row == k, digit[t : t + 1, :], rows)
        digits_ref[t] = rows.astype(BF16)


def tail_rows(weight):
    row = iota((TAIL, TILE), 0)
    rows = jnp.where(row < 3, 1.0, 0.0)
    if weight is not None:
        for k, part in enumerate(three_parts(weight)):
            rows = jnp.where(row == 3 + k, part, rows)
    return jnp.concatenate([rows.astype(BF16), jnp.zeros((LANES - COMP - TAIL, TILE), BF16)], 0)


def whole_tile(coefs, tail):
    return jnp.concatenate([coefs] * PARTS + [tail], 0)


def against(head_ref, points_ref, c, tile):
    return dot(jnp.concatenate([head_ref[chunk(c), :], points_ref[chunk(c), :]], 1), tile)


def with_shift(points, shift):
    lane = iota(points.shape, 1)
    for k, part in enumerate(three_parts(shift)):
        points = jnp.where(lane == COMP + k, part, points)
    return points


def tile_row(rows, j):
    return jnp.concatenate([rows[2 * j : 2 * j + 1, :], rows[2 * j + 1 : 2 * j + 2, :]], 1)


def over_tiles(tile_count, body, carry):
    if tile_count * TILE == SMALL_ROWS * LANES:
        for j in range(tile_count):
            carry = body(j, carry)
        return carry
    return lax.fori_loop(0, tile_count, body, carry)


def exact_denominators(c, head_ref, points_ref, coefs_ref, tails_ref, energy_ref):
    def find(j, top):
        exponents = against(head_ref, points_ref, c, used_tile(coefs_ref, tails_ref, j))
        energy_ref[j, :, : exponents.shape[1]] = exponents
        return jnp.maximum(top, halves(jnp.maximum, exponents))

    tile_count = coefs_ref.shape[0]
    top = over_tiles(tile_count, find, jnp.full((CHUNK, LANES), 4 * NEGATIVE, F32))
    top = jnp.max(top, axis=1, keepdims=True)

    def add(j, sums):
        width = used_tile(coefs_ref, tails_ref, j).shape[1]
        return sums + halves(jnp.add, jnp.exp2(energy_ref[j, :, :width] - top))

    sums = over_tiles(tile_count, add, jnp.zeros((CHUNK, LANES), F32))
    return jnp.broadcast_to(top + jnp.log2(jnp.sum(sums, axis=1, keepdims=True)), (CHUNK, LANES))


def near_denominators(c, base_ref, head_ref, anchored_ref, coefs_ref, tails_ref):
    def add(j, sums):
        tile = used_tile(coefs_ref, tails_ref, j)
        return sums + halves(jnp.add, jnp.exp2(against(head_ref, anchored_ref, c, tile)))

    sums = over_tiles(coefs_ref.shape[0], add, jnp.zeros((CHUNK, LANES), F32))
    return base_ref[chunk(c), :] + jnp.log2(jnp.sum(sums, axis=1, keepdims=True))


def put_live(c, points_ref, logden, live_ref, dead_ref):
    shift = dead_ref[chunk(c), :] - logden
    live_ref[chunk(c), :] = with_shift(points_ref[chunk(c), :].astype(F32), shift).astype(BF16)


def each_chunk(rows, body):
    def one(c, carry):
        body(c)
        return carry

    lax.fori_loop(0, rows // CHUNK, one, 0)


def exponents_and_highest(tile, head_ref, live_ref, exponent_ref):
    highest = None
    for c in range(live_ref.shape[0] // CHUNK):
        exponents = against(head_ref, live_ref, c, tile)
        exponent_ref[chunk(c), :] = exponents
        top = jnp.max(exponents.reshape(CHUNK // 8, 8, TILE), axis=0)
        highest = top if highest is None else jnp.maximum(highest, top)
    return jnp.max(highest, axis=0, keepdims=True)


def log_of_sum(highest, exponent_ref):
    totals = jnp.zeros((8, TILE), F32)
    for c in range(exponent_ref.shape[0] // CHUNK):
        grown = jnp.exp2(exponent_ref[chunk(c), :] - highest)
        totals = totals + jnp.sum(grown.reshape(CHUNK // 8, 8, TILE), axis=0)
    return highest + jnp.log2(jnp.sum(totals, axis=0, keepdims=True))


def put_rows(logs_ref, first, logs):
    logs = logs * LN2
    logs_ref[pl.ds(first, 1), :] = logs[:, :LANES]
    logs_ref[pl.ds(first + 1, 1), :] = logs[:, LANES:]


def counted_log_sums(weight_ref, coefs_ref, tails_ref, head_ref, live_ref, exponent_ref, logs_ref, low_ref):
    low_ref[...] = jnp.zeros(low_ref.shape, F32)
    logs_ref[0 : weight_ref.shape[0], :] = jnp.zeros(weight_ref.shape, F32)

    def finish(j, logs):
        weight = jnp.concatenate([weight_ref[pl.ds(2 * j, 1), :], weight_ref[pl.ds(2 * j + 1, 1), :]], 1)
        valid = weight > NEGATIVE / 2
        put_rows(logs_ref, 2 * j, jnp.where(valid, logs - weight, 0.0))
        return valid

    def one(i, carry):
        for k in range(2):
            j = 2 * i + k
            totals = jnp.zeros((8, TILE), F32)
            tile = whole_tile(coefs_ref[j], tails_ref[j])
            for c in range(live_ref.shape[0] // CHUNK):
                grown = jnp.exp2(against(head_ref, live_ref, c, tile))
                totals = totals + jnp.sum(grown.reshape(CHUNK // 8, 8, TILE), axis=0)
            totals = jnp.sum(totals, axis=0, keepdims=True)
            valid = finish(j, jnp.log2(totals))
            low_ref[0:1, :] = jnp.maximum(low_ref[0:1, :], jnp.where(valid & (totals < LEAST), 1.0, 0.0))
        return carry

    lax.fori_loop(0, coefs_ref.shape[0] // 2, one, 0)

    @pl.when(jnp.max(low_ref[...]) > 0)
    def _():
        def again(j, carry):
            highest = exponents_and_highest(whole_tile(coefs_ref[j], tails_ref[j]), head_ref, live_ref, exponent_ref)
            finish(j, log_of_sum(highest, exponent_ref))
            return carry

        lax.fori_loop(0, coefs_ref.shape[0], again, 0)


def weighted_tails(logs, log_count_ref, tails_ref, weight_ref):
    log_count = log_count_ref[...]
    valid = log_count > NEGATIVE / 2
    free = jnp.where(valid, logs * -LOG2E, 4 * NEGATIVE)
    highest = jnp.max(jnp.max(free, axis=0, keepdims=True), axis=1, keepdims=True)
    free = jnp.where(valid, free - highest, 0.0)
    weight = log_count + free
    weight_ref[...] = weight
    for j in range(tails_ref.shape[0]):
        tails_ref[j] = tail_rows(tile_row(weight, j))
    return highest, jnp.min(free)


def first_kernel(
    meta_ref, mine_ref, other_ref, place_ref, digits_ref, head_ref, points_ref, dead_ref,
    logs_ref, log_count_ref, coefs_ref, anchored_ref, base_ref,
    tails_ref, packed_ref, energy_ref, live_ref, exponent_ref, low_ref, rows_ref,
):
    groups = mine_ref.shape[0]
    packed_ref[...] = jnp.zeros(packed_ref.shape, F32)
    for t in range(groups):
        chosen = jnp.where(iota((2 * LANES, LANES), 0) == place_ref[t : t + 1, :], 1.0, 0.0).astype(BF16)
        moved = dot_nt(jnp.concatenate([mine_ref[t], other_ref[t], digits_ref[t]], 0), chosen)
        at = meta_ref[t]
        packed_ref[at] += moved[:, :LANES]
        packed_ref[at + 1] += moved[:, LANES:]
    for h in range(log_count_ref.shape[0]):
        digits = [packed_ref[h, COMP + k : COMP + k + 1, :] for k in range(3)]
        counts = digits[0] * 16384.0 + digits[1] * 128.0 + digits[2]
        log_count_ref[h : h + 1, :] = jnp.where(counts > 0, jnp.log2(jnp.maximum(counts, 1.0)), NEGATIVE)
    log_count = log_count_ref[...]
    for j in range(coefs_ref.shape[0]):
        coefs_ref[j] = jnp.concatenate([packed_ref[2 * j, 0:COMP, :], packed_ref[2 * j + 1, 0:COMP, :]], 1).astype(BF16)
        tails_ref[j] = tail_rows(tile_row(log_count, j))

    def denominators(c):
        logden = exact_denominators(c, head_ref, points_ref, coefs_ref, tails_ref, energy_ref)
        base_ref[chunk(c), :] = logden
        anchored_ref[chunk(c), :] = with_shift(points_ref[chunk(c), :].astype(F32), -logden).astype(BF16)
        put_live(c, points_ref, logden, live_ref, dead_ref)

    each_chunk(points_ref.shape[0], denominators)
    counted_log_sums(
        log_count_ref, coefs_ref, tails_ref, head_ref, live_ref, exponent_ref, rows_ref, low_ref
    )
    logs_ref[...] = jnp.broadcast_to(rows_ref[...][None], logs_ref.shape)


def new_denominators(least, base_ref, head_ref, anchored_ref, points_ref, coefs_ref, tails_ref, energy_ref, put):
    rows = points_ref.shape[0]
    near = least > -SPREAD

    @pl.when(near)
    def _():
        each_chunk(
            rows,
            lambda c: put(c, near_denominators(c, base_ref, head_ref, anchored_ref, coefs_ref, tails_ref)),
        )

    @pl.when(jnp.logical_not(near))
    def _():
        each_chunk(
            rows, lambda c: put(c, exact_denominators(c, head_ref, points_ref, coefs_ref, tails_ref, energy_ref))
        )


def places(slot_rows):
    if slot_rows == SMALL_ROWS:
        return (slot_rows - 1, slot_rows - 2), LANES - 1
    return (slot_rows, slot_rows + 1), 0


def put_message(logs, slot_rows, message_ref):
    (own_row, zero_row), zero_lane = places(slot_rows)
    rows = message_ref.shape[1]
    common = logs[0:slot_rows, :]
    if rows > slot_rows:
        common = jnp.concatenate([common, jnp.zeros((rows - slot_rows, LANES), F32)], 0)
    row, lane = iota(common.shape, 0), iota(common.shape, 1)
    common = jnp.where((row == zero_row) & (lane == zero_lane), logs[slot_rows : slot_rows + 1, 0:1], common)
    for t in range(message_ref.shape[0]):
        own = logs[slot_rows + t : slot_rows + t + 1, :]
        message_ref[t] = jnp.where(row == own_row, own, common)


def second_kernel(
    logs_in_ref, mine_ref, other_ref, log_count_ref, coefs_ref, head_ref, points_ref, dead_ref, anchored_ref,
    base_ref,
    message_ref,
    tails_ref, weight_ref, energy_ref, live_ref, exponent_ref, low_ref, rows_ref,
):
    groups = mine_ref.shape[0]
    slot_rows = weight_ref.shape[0]
    logs = log_sum_pieces(logs_in_ref)
    _, least = weighted_tails(logs, log_count_ref, tails_ref, weight_ref)
    new_denominators(
        least, base_ref, head_ref, anchored_ref, points_ref, coefs_ref, tails_ref, energy_ref,
        lambda c, logden: put_live(c, points_ref, logden, live_ref, dead_ref),
    )
    counted_log_sums(
        weight_ref, coefs_ref, tails_ref, head_ref, live_ref, exponent_ref, rows_ref, low_ref
    )
    tail = tail_rows(None)
    last = groups * LANES // TILE - 1

    def every_tile(t):
        parts = [jnp.concatenate([mine_ref[2 * t + k], other_ref[2 * t + k]], 0) for k in range(2)]
        return whole_tile(jnp.concatenate(parts, 1), tail)

    def step(t, highest):
        tile = every_tile(jnp.minimum(t + 1, last))
        totals = jnp.zeros((8, TILE), F32)
        tops = []
        for c in range(live_ref.shape[0] // CHUNK):
            grown = jnp.exp2(exponent_ref[chunk(c), :] - highest)
            totals = totals + jnp.sum(grown.reshape(CHUNK // 8, 8, TILE), axis=0)
            exponents = against(head_ref, live_ref, c, tile)
            exponent_ref[chunk(c), :] = exponents
            tops.append(jnp.max(exponents.reshape(CHUNK // 8, 8, TILE), axis=0))
        logs = highest + jnp.log2(jnp.sum(totals, axis=0, keepdims=True))
        put_rows(rows_ref, slot_rows + 2 * t, logs)
        return jnp.max(functools.reduce(jnp.maximum, tops), axis=0, keepdims=True)

    start = exponents_and_highest(every_tile(0), head_ref, live_ref, exponent_ref)
    lax.fori_loop(0, last + 1, step, start, unroll=4)
    put_message(rows_ref[...], slot_rows, message_ref)


def third_kernel(
    logs_in_ref, log_count_ref, coefs_ref, head_ref, points_ref, anchored_ref, base_ref,
    free_ref, logden_ref,
    tails_ref, weight_ref, energy_ref, totals_ref,
):
    slot_rows = weight_ref.shape[0]
    logs = log_sum_pieces(logs_in_ref)
    (own_row, zero_row), zero_lane = places(slot_rows)
    zero = logs[zero_row : zero_row + 1, zero_lane : zero_lane + 1]
    free_ref[...] = zero - logs[own_row : own_row + 1, :]
    highest, least = weighted_tails(logs[:slot_rows], log_count_ref, tails_ref, weight_ref)

    def put(c, logden):
        totals_ref[chunk(c), :] = logden

    new_denominators(
        least, base_ref, head_ref, anchored_ref, points_ref, coefs_ref, tails_ref, energy_ref, put
    )
    turned = [totals_ref[pl.ds(b * LANES, LANES), :].T[0:1, :] for b in range(points_ref.shape[0] // LANES)]
    logden = (jnp.concatenate(turned, 0) + highest) * LN2 + zero
    logden_ref[...] = jnp.broadcast_to(logden[None], logden_ref.shape)


def iterated(slot_rows, meta, mine, other, place, digits, head, points, dead):
    samps = lax.axis_size(SAMP)
    groups = mine.shape[0]
    rows = points.shape[0]
    tile_count = slot_rows * LANES // TILE
    shape = jax.ShapeDtypeStruct
    vmem = pl.BlockSpec(memory_space=pltpu.VMEM)
    smem = pl.BlockSpec(memory_space=pltpu.SMEM)
    params = pltpu.CompilerParams(vmem_limit_bytes=24 << 20)
    tails_work = pltpu.VMEM((tile_count, LANES - COMP, TILE), BF16)
    weight_work = pltpu.VMEM((slot_rows, LANES), F32)
    energy_work = pltpu.VMEM((tile_count, CHUNK, TILE), F32)
    live_work = pltpu.VMEM((rows, LANES), BF16)
    exponent_work = pltpu.VMEM((rows, TILE), F32)
    low_work = pltpu.VMEM((8, TILE), F32)
    logs, log_count, coefs, anchored, base = pl.pallas_call(
        first_kernel,
        out_shape=(
            shape((samps, slot_rows, LANES), F32), shape((slot_rows, LANES), F32), shape((tile_count, COMP, TILE), BF16), shape((rows, LANES), BF16),
            shape((rows, LANES), F32),
        ),
        in_specs=[smem] + [vmem] * 7, out_specs=(vmem,) * 5,
        scratch_shapes=[
            tails_work, pltpu.VMEM((slot_rows + 2, COMP + TAIL, LANES), F32), energy_work, live_work, exponent_work, low_work,
            weight_work,
        ],
        compiler_params=params, name="first",
    )(meta, mine, other, place, digits, head, points, dead)
    logs = log_sum(exchanged(logs, SAMP))
    logs = copies_of_each(logs, STATE)
    logs = pl.pallas_call(
        second_kernel,
        out_shape=shape((groups, slot_rows if slot_rows == SMALL_ROWS else slot_rows + 8, LANES), F32),
        in_specs=[vmem] * 10, out_specs=vmem,
        scratch_shapes=[
            tails_work, weight_work, energy_work, live_work, exponent_work,
            low_work, pltpu.VMEM((slot_rows + groups, LANES), F32),
        ],
        compiler_params=params, name="second",
    )(logs, mine, other, log_count, coefs, head, points, dead, anchored, base)
    logs = copies_of_each(log_sum(exchanged(logs, STATE)), SAMP)
    return pl.pallas_call(
        third_kernel,
        out_shape=(shape((1, LANES), F32), shape((groups, rows // LANES, LANES), F32)),
        in_specs=[vmem] * 7, out_specs=(vmem, vmem),
        scratch_shapes=[tails_work, weight_work, energy_work, pltpu.VMEM((rows, LANES), F32)],
        compiler_params=params, name="third",
    )(logs, log_count, coefs, head, points, anchored, base)


def shards(components, coefficients, block_window, block_fill):
    groups = lax.axis_size(STATE)
    samps = lax.axis_size(SAMP)
    position = lax.axis_index(STATE)
    core = lax.axis_index(SAMP[1])
    rows = components.shape[1] // groups
    slot_rows = min(samps * block_window.shape[0] // LANES, groups)
    shape = jax.ShapeDtypeStruct
    vmem = pl.BlockSpec(memory_space=pltpu.VMEM)
    smem = pl.BlockSpec(memory_space=pltpu.SMEM)
    params = pltpu.CompilerParams(vmem_limit_bytes=24 << 20)
    spot = jnp.stack([position, core]).astype(jnp.int32)

    half = COMP // 2
    mine = copies_of_each(lax.dynamic_slice_in_dim(coefficients, core * half, half, 0), STATE)
    pair = jnp.stack([block_window, block_fill])[None]
    blocks = jnp.concatenate([pair, lax.ppermute(pair, SAMP[1], [(0, 1), (1, 0)])], 0)
    along = lax.axis_size(SAMP[0])
    turns = [[(i, (i + k) % along) for i in range(along)] for k in range(1, along)]
    pieces = [blocks] + [lax.ppermute(blocks, SAMP[0], turn) for turn in turns]
    head, points, dead = pl.pallas_call(
        points_kernel,
        out_shape=(shape((rows, LANES), BF16), shape((rows, LANES), BF16), shape((rows, LANES), F32)),
        in_specs=[smem, vmem, vmem], out_specs=(vmem, vmem, vmem),
        compiler_params=params, name="points",
    )(spot, pair, lax.dynamic_slice_in_dim(components, position * rows, rows, 1))
    other = lax.ppermute(mine, SAMP[1], [(0, 1), (1, 0)])
    place, meta, digits = pl.pallas_call(
        count_kernel,
        out_shape=(
            shape((groups, LANES), jnp.int32), shape((groups + 8, LANES), jnp.int32),
            shape((groups, TAIL, LANES), BF16),
        ),
        in_specs=[vmem] * len(pieces), out_specs=(vmem, vmem, vmem), compiler_params=params, name="count",
    )(*pieces)
    total = meta[groups, 0]
    meta = meta[:groups, 0]
    free, logden = lax.cond(
        total <= SMALL,
        functools.partial(iterated, SMALL_ROWS), functools.partial(iterated, slot_rows),
        meta, mine, other, place, digits, head, points, dead,
    )
    return free.reshape(-1), exchanged(logden, STATE).reshape(-1)


def solution(mesh):
    torus = Mesh(mesh.devices.reshape(4, 2, 8, 4), ("samp_0", "samp_1", "state_0", "state_1"))
    placed = (P(None, SAMP), P(None, STATE), P(SAMP), P(SAMP))
    return jax.shard_map(
        shards, mesh=torus, in_specs=placed, out_specs=(P(STATE), P(SAMP)), check_vma=False
    )
```

```python
import functools

import jax
import jax.numpy as jnp
from jax import lax
from jax.experimental import pallas as pl
from jax.experimental.pallas import tpu as pltpu
from jax.sharding import Mesh
from jax.sharding import PartitionSpec as P


BLOCK = 128
LANES = 128
COMP = 64
TILE = 256
PARTS = 3
LOG2E = 1.4426950408889634
LN2 = 0.6931471805599453
CHUNK = 512
TAIL = 16
LEAST = 1e-25
SPREAD = 72.0
SMALL_ROWS = 8
SMALL = (SMALL_ROWS - 1) * LANES - 1
STATE = ("state_0", "state_1")
SAMP = ("samp_0", "samp_1")
NEGATIVE = -1e30
BF16 = jnp.bfloat16
F32 = jnp.float32


def exchanged(copies, axes):
    return lax.all_to_all(copies, axes, split_axis=0, concat_axis=0, tiled=True)


def copies_of_each(x, axes):
    return exchanged(jnp.broadcast_to(x, (lax.axis_size(axes), *x.shape)), axes)


def iota(shape, dim):
    return lax.broadcasted_iota(jnp.int32, shape, dim)


def dot_nt(a, b):
    return lax.dot_general(a, b, (((1,), (1,)), ((), ())), preferred_element_type=F32)


def dot(a, b):
    return jnp.dot(a, b, preferred_element_type=F32)


def three_parts(x):
    high = x.astype(BF16).astype(F32)
    rest = x - high
    middle = rest.astype(BF16).astype(F32)
    return high, middle, rest - middle


def log_sum_pieces(logs_ref):
    pieces = logs_ref.shape[0]
    highest = functools.reduce(jnp.maximum, [logs_ref[p] for p in range(pieces)])
    totals = functools.reduce(jnp.add, [jnp.exp(logs_ref[p] - highest) for p in range(pieces)])
    return highest + jnp.log(totals)


def chunk(c):
    return pl.ds(c * CHUNK if isinstance(c, int) else pl.multiple_of(c * CHUNK, CHUNK), CHUNK)


def halves(combine, x):
    return x if x.shape[1] == LANES else combine(x[:, :LANES], x[:, LANES:])


def used_tile(coefs_ref, tails_ref, j):
    width = LANES if isinstance(j, int) and j == SMALL_ROWS * LANES // TILE - 1 else TILE
    return whole_tile(coefs_ref[j], tails_ref[j])[:, :width]


def points_kernel(spot_ref, own_ref, block_ref, head_ref, points_ref, dead_ref):
    rows = points_ref.shape[0]
    half = COMP // 2
    own = pl.multiple_of(spot_ref[1] * half, half)
    lane = iota((LANES, LANES - COMP), 1)
    ones = jnp.where((lane >= 3) & (lane < 6), 1.0, 0.0)
    for b in range(rows // LANES):
        at = slice(b * LANES, (b + 1) * LANES)
        mine = block_ref[pl.ds(own, half), at].astype(F32)
        other = block_ref[pl.ds(pl.multiple_of(half - own, half), half), at].astype(F32)
        high, middle, low = three_parts(jnp.concatenate([mine, other], 0).T * -LOG2E)
        head_ref[at, :] = jnp.concatenate([high, middle], 1).astype(BF16)
        points_ref[at, :] = jnp.concatenate([low, ones], 1).astype(BF16)
        fills = own_ref[0, 1:2, :]
        chosen = iota(fills.shape, 1) == spot_ref[0] * (rows // BLOCK) + b
        fill = jnp.sum(jnp.where(chosen, fills.astype(F32), 0.0), axis=1, keepdims=True)
        dead_ref[at, :] = jnp.where(iota((BLOCK, LANES), 0).astype(F32) < fill, 0.0, NEGATIVE)


def count_kernel(*refs):
    blocks_refs, (place_ref, meta_ref, digits_ref) = refs[:-3], refs[-3:]
    groups = place_ref.shape[0]
    width = blocks_refs[0].shape[2]
    counts = jnp.zeros((groups, LANES), F32)
    for blocks_ref, s in [(r, s) for r in blocks_refs for s in range(r.shape[0])]:
        window = blocks_ref[s, 0:1, :]
        fill = blocks_ref[s, 1:2, :]
        of_group = jnp.where(iota((groups, width), 0) == window >> 7, fill, 0).astype(F32).astype(BF16)
        of_lane = jnp.where(iota((LANES, width), 0) == (window & 127), 1.0, 0.0).astype(BF16)
        counts = counts + dot_nt(of_group, of_lane)
    counted = counts > 0
    packed = jnp.where(counted, 1.0, 0.0).astype(BF16)
    before = jnp.where(iota((LANES, LANES), 0) < iota((LANES, LANES), 1), 1.0, 0.0).astype(BF16)
    within = dot(packed, before)
    total = dot(packed, jnp.ones((LANES, LANES), BF16))
    earlier = jnp.where(iota((groups, groups), 1) < iota((groups, groups), 0), 1.0, 0.0).astype(BF16)
    offset_int = dot(earlier, total.astype(BF16)).astype(jnp.int32)
    within_int = within.astype(jnp.int32)
    place_ref[...] = jnp.where(counted, (offset_int & 127) + within_int, -1)
    meta_ref[0:groups, :] = offset_int >> 7
    everything = jnp.sum(total, axis=0, keepdims=True).astype(jnp.int32)
    meta_ref[groups : groups + 8, :] = jnp.broadcast_to(everything, (8, LANES))
    counts_int = counts.astype(jnp.int32)
    digits = [d.astype(F32) for d in (counts_int >> 14, (counts_int >> 7) & 127, counts_int & 127)]
    row = iota((TAIL, LANES), 0)
    for t in range(groups):
        rows = jnp.zeros((TAIL, LANES), F32)
        for k, digit in enumerate(digits):
            rows = jnp.where(row == k, digit[t : t + 1, :], rows)
        digits_ref[t] = rows.astype(BF16)


def tail_rows(weight):
    row = iota((TAIL, TILE), 0)
    rows = jnp.where(row < 3, 1.0, 0.0)
    if weight is not None:
        for k, part in enumerate(three_parts(weight)):
            rows = jnp.where(row == 3 + k, part, rows)
    return jnp.concatenate([rows.astype(BF16), jnp.zeros((LANES - COMP - TAIL, TILE), BF16)], 0)


def whole_tile(coefs, tail):
    return jnp.concatenate([coefs] * PARTS + [tail], 0)


def against(head_ref, points_ref, c, tile):
    return dot(jnp.concatenate([head_ref[chunk(c), :], points_ref[chunk(c), :]], 1), tile)


def with_shift(points, shift):
    lane = iota(points.shape, 1)
    for k, part in enumerate(three_parts(shift)):
        points = jnp.where(lane == COMP + k, part, points)
    return points


def tile_row(rows, j):
    return jnp.concatenate([rows[2 * j : 2 * j + 1, :], rows[2 * j + 1 : 2 * j + 2, :]], 1)


def over_tiles(tile_count, body, carry):
    if tile_count * TILE == SMALL_ROWS * LANES:
        for j in range(tile_count):
            carry = body(j, carry)
        return carry
    return lax.fori_loop(0, tile_count, body, carry)


def exact_denominators(c, head_ref, points_ref, coefs_ref, tails_ref, energy_ref):
    def find(j, top):
        exponents = against(head_ref, points_ref, c, used_tile(coefs_ref, tails_ref, j))
        energy_ref[j, :, : exponents.shape[1]] = exponents
        return jnp.maximum(top, halves(jnp.maximum, exponents))

    tile_count = coefs_ref.shape[0]
    top = over_tiles(tile_count, find, jnp.full((CHUNK, LANES), 4 * NEGATIVE, F32))
    top = jnp.max(top, axis=1, keepdims=True)

    def add(j, sums):
        width = used_tile(coefs_ref, tails_ref, j).shape[1]
        return sums + halves(jnp.add, jnp.exp2(energy_ref[j, :, :width] - top))

    sums = over_tiles(tile_count, add, jnp.zeros((CHUNK, LANES), F32))
    return jnp.broadcast_to(top + jnp.log2(jnp.sum(sums, axis=1, keepdims=True)), (CHUNK, LANES))


def near_denominators(c, base_ref, head_ref, anchored_ref, coefs_ref, tails_ref):
    def add(j, sums):
        tile = used_tile(coefs_ref, tails_ref, j)
        return sums + halves(jnp.add, jnp.exp2(against(head_ref, anchored_ref, c, tile)))

    sums = over_tiles(coefs_ref.shape[0], add, jnp.zeros((CHUNK, LANES), F32))
    return base_ref[chunk(c), :] + jnp.log2(jnp.sum(sums, axis=1, keepdims=True))


def put_live(c, points_ref, logden, live_ref, dead_ref):
    shift = dead_ref[chunk(c), :] - logden
    live_ref[chunk(c), :] = with_shift(points_ref[chunk(c), :].astype(F32), shift).astype(BF16)


def each_chunk(rows, body):
    def one(c, carry):
        body(c)
        return carry

    lax.fori_loop(0, rows // CHUNK, one, 0)


def exponents_and_highest(tile, head_ref, live_ref, exponent_ref):
    highest = None
    for c in range(live_ref.shape[0] // CHUNK):
        exponents = against(head_ref, live_ref, c, tile)
        exponent_ref[chunk(c), :] = exponents
        top = jnp.max(exponents.reshape(CHUNK // 8, 8, TILE), axis=0)
        highest = top if highest is None else jnp.maximum(highest, top)
    return jnp.max(highest, axis=0, keepdims=True)


def log_of_sum(highest, exponent_ref):
    totals = jnp.zeros((8, TILE), F32)
    for c in range(exponent_ref.shape[0] // CHUNK):
        grown = jnp.exp2(exponent_ref[chunk(c), :] - highest)
        totals = totals + jnp.sum(grown.reshape(CHUNK // 8, 8, TILE), axis=0)
    return highest + jnp.log2(jnp.sum(totals, axis=0, keepdims=True))


def put_rows(logs_ref, first, logs):
    logs = logs * LN2
    logs_ref[pl.ds(first, 1), :] = logs[:, :LANES]
    logs_ref[pl.ds(first + 1, 1), :] = logs[:, LANES:]


def counted_log_sums(weight_ref, coefs_ref, tails_ref, head_ref, live_ref, exponent_ref, logs_ref, low_ref):
    low_ref[...] = jnp.zeros(low_ref.shape, F32)
    logs_ref[0 : weight_ref.shape[0], :] = jnp.zeros(weight_ref.shape, F32)

    def finish(j, logs):
        weight = jnp.concatenate([weight_ref[pl.ds(2 * j, 1), :], weight_ref[pl.ds(2 * j + 1, 1), :]], 1)
        valid = weight > NEGATIVE / 2
        put_rows(logs_ref, 2 * j, jnp.where(valid, logs - weight, 0.0))
        return valid

    def one(i, carry):
        for k in range(2):
            j = 2 * i + k
            totals = jnp.zeros((8, TILE), F32)
            tile = whole_tile(coefs_ref[j], tails_ref[j])
            for c in range(live_ref.shape[0] // CHUNK):
                grown = jnp.exp2(against(head_ref, live_ref, c, tile))
                totals = totals + jnp.sum(grown.reshape(CHUNK // 8, 8, TILE), axis=0)
            totals = jnp.sum(totals, axis=0, keepdims=True)
            valid = finish(j, jnp.log2(totals))
            low_ref[0:1, :] = jnp.maximum(low_ref[0:1, :], jnp.where(valid & (totals < LEAST), 1.0, 0.0))
        return carry

    lax.fori_loop(0, coefs_ref.shape[0] // 2, one, 0)

    @pl.when(jnp.max(low_ref[...]) > 0)
    def _():
        def again(j, carry):
            highest = exponents_and_highest(whole_tile(coefs_ref[j], tails_ref[j]), head_ref, live_ref, exponent_ref)
            finish(j, log_of_sum(highest, exponent_ref))
            return carry

        lax.fori_loop(0, coefs_ref.shape[0], again, 0)


def weighted_tails(logs, log_count_ref, tails_ref, weight_ref):
    log_count = log_count_ref[...]
    valid = log_count > NEGATIVE / 2
    free = jnp.where(valid, logs * -LOG2E, 4 * NEGATIVE)
    highest = jnp.max(jnp.max(free, axis=0, keepdims=True), axis=1, keepdims=True)
    free = jnp.where(valid, free - highest, 0.0)
    weight = log_count + free
    weight_ref[...] = weight
    for j in range(tails_ref.shape[0]):
        tails_ref[j] = tail_rows(tile_row(weight, j))
    return highest, jnp.min(free)


def first_kernel(
    meta_ref, mine_ref, other_ref, place_ref, digits_ref, head_ref, points_ref, dead_ref,
    logs_ref, log_count_ref, coefs_ref, anchored_ref, base_ref,
    tails_ref, packed_ref, energy_ref, live_ref, exponent_ref, low_ref, rows_ref,
):
    groups = mine_ref.shape[0]
    packed_ref[...] = jnp.zeros(packed_ref.shape, F32)
    for t in range(groups):
        chosen = jnp.where(iota((2 * LANES, LANES), 0) == place_ref[t : t + 1, :], 1.0, 0.0).astype(BF16)
        moved = dot_nt(jnp.concatenate([mine_ref[t], other_ref[t], digits_ref[t]], 0), chosen)
        at = meta_ref[t]
        packed_ref[at] += moved[:, :LANES]
        packed_ref[at + 1] += moved[:, LANES:]
    for h in range(log_count_ref.shape[0]):
        digits = [packed_ref[h, COMP + k : COMP + k + 1, :] for k in range(3)]
        counts = digits[0] * 16384.0 + digits[1] * 128.0 + digits[2]
        log_count_ref[h : h + 1, :] = jnp.where(counts > 0, jnp.log2(jnp.maximum(counts, 1.0)), NEGATIVE)
    log_count = log_count_ref[...]
    for j in range(coefs_ref.shape[0]):
        coefs_ref[j] = jnp.concatenate([packed_ref[2 * j, 0:COMP, :], packed_ref[2 * j + 1, 0:COMP, :]], 1).astype(BF16)
        tails_ref[j] = tail_rows(tile_row(log_count, j))

    def denominators(c):
        logden = exact_denominators(c, head_ref, points_ref, coefs_ref, tails_ref, energy_ref)
        base_ref[chunk(c), :] = logden
        anchored_ref[chunk(c), :] = with_shift(points_ref[chunk(c), :].astype(F32), -logden).astype(BF16)
        put_live(c, points_ref, logden, live_ref, dead_ref)

    each_chunk(points_ref.shape[0], denominators)
    counted_log_sums(
        log_count_ref, coefs_ref, tails_ref, head_ref, live_ref, exponent_ref, rows_ref, low_ref
    )
    logs_ref[...] = jnp.broadcast_to(rows_ref[...][None], logs_ref.shape)


def new_denominators(least, base_ref, head_ref, anchored_ref, points_ref, coefs_ref, tails_ref, energy_ref, put):
    rows = points_ref.shape[0]
    near = least > -SPREAD

    @pl.when(near)
    def _():
        each_chunk(
            rows,
            lambda c: put(c, near_denominators(c, base_ref, head_ref, anchored_ref, coefs_ref, tails_ref)),
        )

    @pl.when(jnp.logical_not(near))
    def _():
        each_chunk(
            rows, lambda c: put(c, exact_denominators(c, head_ref, points_ref, coefs_ref, tails_ref, energy_ref))
        )


def merge_kernel(logs_ref, copies_ref):
    copies_ref[...] = jnp.broadcast_to(log_sum_pieces(logs_ref)[None], copies_ref.shape)


def merged(logs, axes):
    vmem = pl.BlockSpec(memory_space=pltpu.VMEM)
    return pl.pallas_call(
        merge_kernel, out_shape=jax.ShapeDtypeStruct((lax.axis_size(axes), *logs.shape[1:]), F32),
        in_specs=[vmem], out_specs=vmem,
        compiler_params=pltpu.CompilerParams(vmem_limit_bytes=24 << 20), name="merge",
    )(logs)


def places(slot_rows):
    if slot_rows == SMALL_ROWS:
        return (slot_rows - 1, slot_rows - 2), LANES - 1
    return (slot_rows, slot_rows + 1), 0


def put_message(logs, slot_rows, message_ref):
    (own_row, zero_row), zero_lane = places(slot_rows)
    rows = message_ref.shape[1]
    common = logs[0:slot_rows, :]
    if rows > slot_rows:
        common = jnp.concatenate([common, jnp.zeros((rows - slot_rows, LANES), F32)], 0)
    row, lane = iota(common.shape, 0), iota(common.shape, 1)
    common = jnp.where((row == zero_row) & (lane == zero_lane), logs[slot_rows : slot_rows + 1, 0:1], common)
    for t in range(message_ref.shape[0]):
        own = logs[slot_rows + t : slot_rows + t + 1, :]
        message_ref[t] = jnp.where(row == own_row, own, common)


def second_kernel(
    logs_in_ref, mine_ref, other_ref, log_count_ref, coefs_ref, head_ref, points_ref, dead_ref, anchored_ref,
    base_ref,
    message_ref,
    tails_ref, weight_ref, energy_ref, live_ref, exponent_ref, low_ref, rows_ref,
):
    groups = mine_ref.shape[0]
    slot_rows = weight_ref.shape[0]
    logs = log_sum_pieces(logs_in_ref)
    _, least = weighted_tails(logs, log_count_ref, tails_ref, weight_ref)
    new_denominators(
        least, base_ref, head_ref, anchored_ref, points_ref, coefs_ref, tails_ref, energy_ref,
        lambda c, logden: put_live(c, points_ref, logden, live_ref, dead_ref),
    )
    counted_log_sums(
        weight_ref, coefs_ref, tails_ref, head_ref, live_ref, exponent_ref, rows_ref, low_ref
    )
    tail = tail_rows(None)
    last = groups * LANES // TILE - 1

    def every_tile(t):
        parts = [jnp.concatenate([mine_ref[2 * t + k], other_ref[2 * t + k]], 0) for k in range(2)]
        return whole_tile(jnp.concatenate(parts, 1), tail)

    def step(t, highest):
        tile = every_tile(jnp.minimum(t + 1, last))
        totals = jnp.zeros((8, TILE), F32)
        tops = []
        for c in range(live_ref.shape[0] // CHUNK):
            grown = jnp.exp2(exponent_ref[chunk(c), :] - highest)
            totals = totals + jnp.sum(grown.reshape(CHUNK // 8, 8, TILE), axis=0)
            exponents = against(head_ref, live_ref, c, tile)
            exponent_ref[chunk(c), :] = exponents
            tops.append(jnp.max(exponents.reshape(CHUNK // 8, 8, TILE), axis=0))
        logs = highest + jnp.log2(jnp.sum(totals, axis=0, keepdims=True))
        put_rows(rows_ref, slot_rows + 2 * t, logs)
        return jnp.max(functools.reduce(jnp.maximum, tops), axis=0, keepdims=True)

    start = exponents_and_highest(every_tile(0), head_ref, live_ref, exponent_ref)
    lax.fori_loop(0, last + 1, step, start, unroll=4)
    put_message(rows_ref[...], slot_rows, message_ref)


def third_kernel(
    logs_in_ref, log_count_ref, coefs_ref, head_ref, points_ref, anchored_ref, base_ref,
    free_ref, logden_ref,
    tails_ref, weight_ref, energy_ref, totals_ref,
):
    slot_rows = weight_ref.shape[0]
    logs = log_sum_pieces(logs_in_ref)
    (own_row, zero_row), zero_lane = places(slot_rows)
    zero = logs[zero_row : zero_row + 1, zero_lane : zero_lane + 1]
    free_ref[...] = zero - logs[own_row : own_row + 1, :]
    highest, least = weighted_tails(logs[:slot_rows], log_count_ref, tails_ref, weight_ref)

    def put(c, logden):
        totals_ref[chunk(c), :] = logden

    new_denominators(
        least, base_ref, head_ref, anchored_ref, points_ref, coefs_ref, tails_ref, energy_ref, put
    )
    turned = [totals_ref[pl.ds(b * LANES, LANES), :].T[0:1, :] for b in range(points_ref.shape[0] // LANES)]
    logden = (jnp.concatenate(turned, 0) + highest) * LN2 + zero
    logden_ref[...] = jnp.broadcast_to(logden[None], logden_ref.shape)


def iterated(slot_rows, meta, mine, other, place, digits, head, points, dead):
    samps = lax.axis_size(SAMP)
    groups = mine.shape[0]
    rows = points.shape[0]
    tile_count = slot_rows * LANES // TILE
    shape = jax.ShapeDtypeStruct
    vmem = pl.BlockSpec(memory_space=pltpu.VMEM)
    smem = pl.BlockSpec(memory_space=pltpu.SMEM)
    params = pltpu.CompilerParams(vmem_limit_bytes=24 << 20)
    tails_work = pltpu.VMEM((tile_count, LANES - COMP, TILE), BF16)
    weight_work = pltpu.VMEM((slot_rows, LANES), F32)
    energy_work = pltpu.VMEM((tile_count, CHUNK, TILE), F32)
    live_work = pltpu.VMEM((rows, LANES), BF16)
    exponent_work = pltpu.VMEM((rows, TILE), F32)
    low_work = pltpu.VMEM((8, TILE), F32)
    logs, log_count, coefs, anchored, base = pl.pallas_call(
        first_kernel,
        out_shape=(
            shape((samps, slot_rows, LANES), F32), shape((slot_rows, LANES), F32), shape((tile_count, COMP, TILE), BF16), shape((rows, LANES), BF16),
            shape((rows, LANES), F32),
        ),
        in_specs=[smem] + [vmem] * 7, out_specs=(vmem,) * 5,
        scratch_shapes=[
            tails_work, pltpu.VMEM((slot_rows + 2, COMP + TAIL, LANES), F32), energy_work, live_work, exponent_work, low_work,
            weight_work,
        ],
        compiler_params=params, name="first",
    )(meta, mine, other, place, digits, head, points, dead)
    logs = exchanged(merged(exchanged(logs, SAMP), STATE), STATE)
    logs = pl.pallas_call(
        second_kernel,
        out_shape=shape((groups, slot_rows if slot_rows == SMALL_ROWS else slot_rows + 8, LANES), F32),
        in_specs=[vmem] * 10, out_specs=vmem,
        scratch_shapes=[
            tails_work, weight_work, energy_work, live_work, exponent_work,
            low_work, pltpu.VMEM((slot_rows + groups, LANES), F32),
        ],
        compiler_params=params, name="second",
    )(logs, mine, other, log_count, coefs, head, points, dead, anchored, base)
    logs = exchanged(merged(exchanged(logs, STATE), SAMP), SAMP)
    return pl.pallas_call(
        third_kernel,
        out_shape=(shape((1, LANES), F32), shape((groups, rows // LANES, LANES), F32)),
        in_specs=[vmem] * 7, out_specs=(vmem, vmem),
        scratch_shapes=[tails_work, weight_work, energy_work, pltpu.VMEM((rows, LANES), F32)],
        compiler_params=params, name="third",
    )(logs, log_count, coefs, head, points, anchored, base)


def shards(components, coefficients, block_window, block_fill):
    groups = lax.axis_size(STATE)
    samps = lax.axis_size(SAMP)
    position = lax.axis_index(STATE)
    core = lax.axis_index(SAMP[1])
    rows = components.shape[1] // groups
    slot_rows = min(samps * block_window.shape[0] // LANES, groups)
    shape = jax.ShapeDtypeStruct
    vmem = pl.BlockSpec(memory_space=pltpu.VMEM)
    smem = pl.BlockSpec(memory_space=pltpu.SMEM)
    params = pltpu.CompilerParams(vmem_limit_bytes=24 << 20)
    spot = jnp.stack([position, core]).astype(jnp.int32)

    half = COMP // 2
    mine = copies_of_each(lax.dynamic_slice_in_dim(coefficients, core * half, half, 0), STATE)
    pair = jnp.stack([block_window, block_fill])[None]
    blocks = jnp.concatenate([pair, lax.ppermute(pair, SAMP[1], [(0, 1), (1, 0)])], 0)
    along = lax.axis_size(SAMP[0])
    turns = [[(i, (i + k) % along) for i in range(along)] for k in range(1, along)]
    pieces = [blocks] + [lax.ppermute(blocks, SAMP[0], turn) for turn in turns]
    head, points, dead = pl.pallas_call(
        points_kernel,
        out_shape=(shape((rows, LANES), BF16), shape((rows, LANES), BF16), shape((rows, LANES), F32)),
        in_specs=[smem, vmem, vmem], out_specs=(vmem, vmem, vmem),
        compiler_params=params, name="points",
    )(spot, pair, lax.dynamic_slice_in_dim(components, position * rows, rows, 1))
    other = lax.ppermute(mine, SAMP[1], [(0, 1), (1, 0)])
    place, meta, digits = pl.pallas_call(
        count_kernel,
        out_shape=(
            shape((groups, LANES), jnp.int32), shape((groups + 8, LANES), jnp.int32),
            shape((groups, TAIL, LANES), BF16),
        ),
        in_specs=[vmem] * len(pieces), out_specs=(vmem, vmem, vmem), compiler_params=params, name="count",
    )(*pieces)
    total = meta[groups, 0]
    meta = meta[:groups, 0]
    free, logden = lax.cond(
        total <= SMALL,
        functools.partial(iterated, SMALL_ROWS), functools.partial(iterated, slot_rows),
        meta, mine, other, place, digits, head, points, dead,
    )
    return free.reshape(-1), exchanged(logden, STATE).reshape(-1)


def solution(mesh):
    torus = Mesh(mesh.devices.reshape(4, 2, 8, 4), ("samp_0", "samp_1", "state_0", "state_1"))
    placed = (P(None, SAMP), P(None, STATE), P(SAMP), P(SAMP))
    return jax.shard_map(
        shards, mesh=torus, in_specs=placed, out_specs=(P(STATE), P(SAMP)), check_vma=False
    )
```
